32 devices in a mesh: lat: 16 (over z, x, core), freq: 2 (over y).
Axes of the slice: x: 2, y: 2, z: 4, core: 2. Of those that a mesh axis runs over, the one named last changes fastest.
Arguments:
- wavefield: float32 [4, 2, 8, 32768], P(None, 'freq', None, 'lat'), may hold values from -6 to 6
- propagator_table: bfloat16 [2, 4, 2112, 128], P('freq'), may hold values from -0.125 to 0.125
- table_index: int32 [3, 256], P(None, 'lat'), may hold values from 0 to 3
- slowness: float32 [3, 32768], P(None, 'lat'), may hold values from -1 to 1
- frequency_scale: float32 [2], P('freq'), may hold values from 1 to 8
Outputs:
- image: float32 [3, 8, 32768], P(None, 'freq', 'lat')
The draws below stay inside these ranges and needn't reach their ends.
All inputs are finite; a program needn't handle non-finite values.
Results may differ from the reference program's by a relative error of at most 0.024.
Values may be sent and summed in bfloat16 or wider, within the bound.
No kernel may reach another device: no remote copies, remote signals or barrier semaphores. Data moves between devices by JAX's collectives and lax.ppermute only.
A program may use at most 64 MiB of HBM per device.

```python
import functools
import math
import jax
import jax.numpy as jnp
from jax import lax

WINDOW = 128
COEFS = 64
REACH = 16
MARGIN = 64
WIN_DEV = 16
SOURCES = 8
TABLES = 4
STEPS = 3
NWIN = 256
NX = 32768
FREQS = 2


def touch_ends(drawn, rng, least, largest):
    spot = [jax.random.randint(jax.random.fold_in(rng, axis), (), 0, length) for axis, length in enumerate(drawn.shape)]
    main_axis = drawn.shape.index(max(drawn.shape))
    beside = spot[:main_axis] + [(spot[main_axis] + 1) % drawn.shape[main_axis]] + spot[main_axis + 1:]
    return drawn.at[tuple(spot)].set(least).at[tuple(beside)].set(largest)


def steps_of(stream_key, extent, shards, smallest, largest):
    gain, own = 1.0, jax.random.fold_in(stream_key, 6)
    for dim, parts in shards:
        draws = jnp.exp(jax.random.uniform(jax.random.fold_in(own, dim), (parts,), jnp.float32, smallest / len(shards), largest / len(shards)))
        gain = gain * jnp.repeat(draws, extent[dim] // parts).reshape([-1 if axis == dim else 1 for axis in range(len(extent))])
    return gain


def noise(own_key, extent, spread, limit, cuts=(), kind=jnp.bfloat16):
    entries = spread * jax.random.normal(own_key, extent, jnp.float32)
    if cuts:
        entries = entries * steps_of(own_key, extent, cuts, -0.22, 0.18)
    return jnp.clip(entries, -limit, limit).astype(kind)


def setup_inputs(seed: int = 0) -> dict:
    keys = jax.random.split(jax.random.key(seed), 6)
    wavefield = noise(keys[0], (4, FREQS, SOURCES, NX), 1.0, 6.0, ((1, 2), (3, 16)), jnp.float32)
    propagator_table = noise(keys[1], (FREQS, TABLES, (2 * REACH + 1) * COEFS, 2 * COEFS), ((2 * REACH + 1) * COEFS) ** -0.5, 0.125, ((0, 2),))
    table_index = touch_ends(jax.random.randint(keys[2], (STEPS, NWIN), 0, TABLES), jax.random.fold_in(keys[2], 1), 0, TABLES - 1).astype(jnp.int32)
    slowness = jnp.clip(jax.random.uniform(keys[3], (STEPS, NX), jnp.float32, -1.0, 1.0) * steps_of(keys[3], (STEPS, NX), ((1, 16),), -0.4, 0.0), -1.0, 1.0)
    frequency_scale = jnp.clip(jnp.exp(math.log(8.0) - 2.0794415 * jax.random.uniform(keys[4], (FREQS,), jnp.float32) ** steps_of(keys[4], (FREQS,), ((0, 2),), -0.2, 0.2)), 1.0, 8.0)
    return {"wavefield": wavefield, "propagator_table": propagator_table, "table_index": table_index, "slowness": slowness, "frequency_scale": frequency_scale}


def basis_table():
    points = jnp.arange(2 * WINDOW, dtype=jnp.float32)[:, None]
    orders = jnp.arange(COEFS, dtype=jnp.float32)[None, :]
    bell_taper = jnp.sin(math.pi * (points + 0.5) / (2 * WINDOW))
    cosine = jnp.cos(math.pi * (orders + 0.5) * (points - MARGIN + 0.5) / WINDOW)
    return (bell_taper * math.sqrt(2.0 / WINDOW) * cosine).astype(jnp.bfloat16)

def rounded(values):
    return lax.optimization_barrier(values.astype(jnp.bfloat16)).astype(jnp.float32)

def one_frequency(table_index, slowness, inputs):
    field, table, scale = inputs
    basis = basis_table().astype(jnp.float32)
    band = 2 * REACH + 1
    images = []
    for step in range(STEPS):
        samples = rounded(field)
        padded = jnp.pad(samples, ((0, 0), (0, 0), (MARGIN, MARGIN)))
        blocks = padded.reshape(4, SOURCES, NWIN + 1, WINDOW)
        coefs = jnp.einsum('asbl,lk->bask', blocks[:, :, :NWIN], basis[:WINDOW])
        coefs = coefs + jnp.einsum('asbl,lk->bask', blocks[:, :, 1:], basis[WINDOW:])
        coefs = rounded(coefs).reshape(NWIN, 4 * SOURCES, COEFS)
        extended = jnp.pad(coefs, ((REACH, REACH), (0, 0), (0, 0)))
        chosen_rows = table_index[step].reshape(NWIN // WIN_DEV, WIN_DEV)
        starts = jnp.arange(NWIN // WIN_DEV, dtype=jnp.int32) * WIN_DEV

        def propagate_block(block):
            begin, chosen = block
            local = lax.dynamic_slice_in_dim(extended, begin, WIN_DEV + 2 * REACH, 0)
            unfolded = jnp.stack([local[offset:offset + WIN_DEV] for offset in range(band)], axis=2)
            unfolded = unfolded.reshape(WIN_DEV, 4 * SOURCES, band * COEFS)
            operators = jnp.take(table, chosen, axis=0).astype(jnp.float32)
            return jnp.einsum('wrk,wkc->wrc', unfolded, operators)
        products = lax.map(propagate_block, (starts, chosen_rows))
        products = products.reshape(NWIN, 4, SOURCES, 2 * COEFS)
        real_part = products[..., :COEFS]
        imag_part = products[..., COEFS:]
        propagated = jnp.stack([real_part[:, 0] - imag_part[:, 1], real_part[:, 1] + imag_part[:, 0], real_part[:, 2] + imag_part[:, 3], real_part[:, 3] - imag_part[:, 2]], axis=1)
        propagated = rounded(propagated)
        segments = jnp.einsum('wask,tk->aswt', propagated, basis)
        zero_block = jnp.zeros((4, SOURCES, 1, WINDOW), jnp.float32)
        summed = jnp.concatenate([segments[..., :WINDOW], zero_block], 2) + jnp.concatenate([zero_block, segments[..., WINDOW:]], 2)
        back = summed.reshape(4, SOURCES, (NWIN + 1) * WINDOW)[:, :, MARGIN:MARGIN + NX]
        phase = scale * slowness[step]
        cosines = jnp.cos(phase)
        sines = jnp.sin(phase)
        field = jnp.stack([back[0] * cosines - back[1] * sines, back[0] * sines + back[1] * cosines, back[2] * cosines + back[3] * sines, back[3] * cosines - back[2] * sines])
        images.append(field[0] * field[2] + field[1] * field[3])
    return jnp.stack(images)

def reference(wavefield, propagator_table, table_index, slowness, frequency_scale):
    worker = functools.partial(one_frequency, table_index, slowness)
    images = lax.map(worker, (jnp.moveaxis(wavefield, 1, 0), propagator_table, frequency_scale))
    return lax.optimization_barrier(jnp.sum(images, axis=0))
```

```python
import math

import jax
import jax.numpy as jnp
import numpy as np
from jax import lax
from jax.experimental import pallas as pl
from jax.experimental.pallas import tpu as pltpu
from jax.sharding import PartitionSpec as P

WINDOW = 128
COEFS = 64
REACH = 16
STEPS = 3
HALF = WINDOW // 2
F32 = jnp.float32
BF16 = jnp.bfloat16
LANES = 2 * COEFS


def basis_table():
    t = np.arange(2 * WINDOW, dtype=np.float32)[:, None]
    k = np.arange(COEFS, dtype=np.float32)[None, :]
    taper = np.sin(np.float32(math.pi) * (t + np.float32(0.5)) / np.float32(2 * WINDOW))
    wave = np.cos(
        np.float32(math.pi)
        * (k + np.float32(0.5))
        * (t - np.float32(HALF) + np.float32(0.5))
        / np.float32(WINDOW)
    )
    return (taper * np.float32(math.sqrt(2.0 / WINDOW)) * wave).astype(np.float32)


def pair_matrices():
    b = basis_table()
    first = np.zeros((4 * WINDOW, LANES), np.float32)
    first[HALF : HALF + 2 * WINDOW, :COEFS] = b
    first[HALF + WINDOW : HALF + 3 * WINDOW, COEFS:] = b
    forward = np.zeros((3 * WINDOW, LANES), np.float32)
    forward[: 2 * WINDOW, :COEFS] = b
    forward[WINDOW:, COEFS:] = b
    inverse = np.zeros((4 * COEFS, 2 * WINDOW), np.float32)
    inverse[COEFS : 2 * COEFS, :WINDOW] = b[WINDOW:].T
    inverse[2 * COEFS : 3 * COEFS, :WINDOW] = b[:WINDOW].T
    inverse[2 * COEFS : 3 * COEFS, WINDOW:] = b[WINDOW:].T
    inverse[3 * COEFS :, WINDOW:] = b[:WINDOW].T
    return first, forward, inverse


def sin_cos(theta):
    turns = jnp.floor(theta * np.float32(2.0 / math.pi) + np.float32(0.5))
    r = theta - turns * np.float32(1.5703125)
    r = r - turns * np.float32(4.837512969970703e-4)
    r = r - turns * np.float32(7.549789948768648e-8)
    r2 = r * r
    s = r + r * r2 * (
        np.float32(-1.6666654611e-1)
        + r2 * (np.float32(8.3321608736e-3) + r2 * np.float32(-1.9515295891e-4))
    )
    c = 1.0 - 0.5 * r2 + r2 * r2 * (
        np.float32(4.166664568298827e-2)
        + r2 * (np.float32(-1.388731625493765e-3) + r2 * np.float32(2.443315711809948e-5))
    )
    quarter = turns - 4.0 * jnp.floor(turns * 0.25)
    odd = (quarter == 1.0) | (quarter == 3.0)
    sin_v = jnp.where(odd, c, s)
    cos_v = jnp.where(odd, s, c)
    sin_v = jnp.where(quarter >= 2.0, -sin_v, sin_v)
    cos_v = jnp.where((quarter == 1.0) | (quarter == 2.0), -cos_v, cos_v)
    return sin_v, cos_v


def lane_swap(v):
    return pltpu.roll(v, LANES // 2, v.ndim - 1)


def low_lanes(shape):
    return lax.broadcasted_iota(jnp.int32, shape, len(shape) - 1) < LANES // 2


def prep_kernel(wave_ref, slow_ref, index_ref, first_ref, keep_ref, send_ref, both_ref, rows_ref):
    core = lax.rem(lax.axis_index("lat"), 2)
    blocks = wave_ref.shape[-1] // WINDOW
    pairs = blocks // 2
    upper = lax.broadcasted_iota(jnp.int32, (8, wave_ref.shape[-1]), 0) < 4
    for side in range(2):
        halves = []
        for low in range(2):
            near, far = wave_ref[low, 0], wave_ref[low + 2, 0]
            if side == 0:
                halves.append(jnp.where(upper, near, pltpu.roll(far, 4, 0)))
            else:
                halves.append(jnp.where(upper, pltpu.roll(near, 4, 0), far))
        samples = jnp.concatenate(halves, axis=0).astype(BF16)
        zero = jnp.zeros((16, WINDOW), BF16)
        padded = [zero] * 3
        padded += [samples[:, WINDOW * g : WINDOW * (g + 1)] for g in range(blocks)]
        padded += [zero] * 3
        parts = [
            jnp.concatenate([padded[2 * i + j] for i in range(pairs + 2)], axis=0)
            for j in range(4)
        ]
        coefs = jnp.dot(
            jnp.concatenate(parts, axis=1), first_ref[...], preferred_element_type=F32
        )
        both_ref[side] = coefs.reshape(pairs + 2, 16, LANES).astype(BF16)
    keep_ref[...] = both_ref[core]
    send_ref[0 : pairs + 2] = both_ref[1 - core]
    slow = slow_ref[...]
    high = slow.astype(BF16).astype(F32)
    rest = slow - high
    lanes = low_lanes((1, LANES))
    rows_ref[...] = jnp.zeros(rows_ref.shape, F32)
    for n in range(STEPS):
        for g in range(blocks):
            cut = slice(WINDOW * g, WINDOW * (g + 1))
            rows_ref[(2 * n) * blocks + g : (2 * n) * blocks + g + 1, :] = high[n : n + 1, cut]
            rows_ref[(2 * n + 1) * blocks + g : (2 * n + 1) * blocks + g + 1, :] = rest[n : n + 1, cut]
        for q in range(pairs):
            at = 2 * STEPS * blocks + n * pairs + q
            rows_ref[at : at + 1, :] = jnp.where(
                lanes,
                jnp.full((1, LANES), index_ref[n, 2 * q], jnp.int32),
                jnp.full((1, LANES), index_ref[n, 2 * q + 1], jnp.int32),
            ).astype(F32)
    send_ref[pairs + 2 :] = rows_ref[...].reshape(-1, 16, LANES).astype(BF16)


def unit_kernel(keep_ref, sent_ref, got_ref, near_ref, far_a_ref, far_b_ref, last_ref):
    place = lax.axis_index("lat")
    second = lax.rem(place, 2) == 1
    n = keep_ref.shape[0]
    own_c, own_i = keep_ref[...].astype(F32), sent_ref[n:].astype(F32)
    got_c, got_i = got_ref[:n].astype(F32), got_ref[n:].astype(F32)
    b0 = jnp.where(second, got_c, own_c)
    b1 = jnp.where(second, own_c, got_c)
    i0 = jnp.where(second, got_i, own_i)
    i1 = jnp.where(second, own_i, got_i)
    unit = jnp.concatenate([b0[: n - 2], b0[n - 2 :] + b1[:2], b1[2:]], axis=0)
    near_ref[0 : 2 * n - 2] = unit.astype(BF16)
    at = 2 * n - 2
    for step in range(2):
        for part in range(2):
            near_ref[at] = i0[2 * step + part].astype(BF16)
            near_ref[at + 1] = i1[2 * step + part].astype(BF16)
            at += 2
    near_ref[at] = jnp.concatenate([i0[6, :8], i1[6, :8]], axis=0).astype(BF16)
    near_ref[at + 1] = jnp.concatenate([i0[6, 8:], i1[6, 8:]], axis=0).astype(BF16)
    near_ref[at + 2] = jnp.concatenate([i0[7, :8], i1[7, :8]], axis=0).astype(BF16)
    for part in range(2):
        last_ref[2 * part] = i0[4 + part].astype(BF16)
        last_ref[2 * part + 1] = i1[4 + part].astype(BF16)
    even_quad = lax.rem(lax.div(place, 4), 2) == 0
    count = far_a_ref.shape[0] - 3
    base = 2 * n - 2
    for ref, right in ((far_a_ref, even_quad), (far_b_ref, jnp.logical_not(even_quad))):
        start = jnp.where(right, base - count, 0)
        pick = jnp.where(right, 1, 0)
        ref[0:count] = near_ref[pl.ds(start, count)]
        ref[count] = near_ref[base + pick]
        ref[count + 1] = near_ref[base + 2 + pick]
        ref[count + 2] = near_ref[base + 8]


def main_kernel(
    units,
    near_ref,
    last_ref,
    a1_ref,
    b1_ref,
    a2_ref,
    b2_ref,
    table_ref,
    forward_ref,
    inverse_ref,
    scale_ref,
    keep_ref,
    send_ref,
    c_ref,
    p_ref,
    ve_ref,
    vo_ref,
    xe_ref,
    xo_ref,
    slow_ref,
    cos_ref,
    sin_ref,
    pick_ref,
    image_ref,
):
    place = lax.axis_index("lat")
    unit = lax.div(place, 2)
    second = lax.rem(place, 2)
    odd_unit = lax.rem(unit, 2) == 1
    odd_quad = lax.rem(lax.div(place, 4), 2) == 1
    has_l1, has_l2 = unit >= 1, unit >= 2
    has_r1, has_r2 = unit + 1 < units, unit + 2 < units
    pairs = 16
    coef_n = pairs + 2
    far_n = a2_ref.shape[0] - 3
    tables = table_ref.shape[0]

    def valid(flag, v):
        return jnp.where(flag, v, jnp.zeros_like(v))

    def choose(flag, x_ref, y_ref, lo, hi):
        return jnp.where(flag, x_ref[lo:hi], y_ref[lo:hi]).astype(F32)

    base = 26
    own = near_ref[0:coef_n].astype(F32)
    left = valid(has_l1, choose(odd_unit, a1_ref, b1_ref, 0, coef_n))
    right = valid(has_r1, choose(odd_unit, b1_ref, a1_ref, 0, coef_n))
    left2 = valid(has_l2, choose(odd_quad, a2_ref, b2_ref, 0, far_n))
    right2 = valid(has_r2, choose(odd_quad, b2_ref, a2_ref, 0, far_n))
    c_ref[0 : far_n - 2] = left2[: far_n - 2].astype(BF16)
    c_ref[base - 17 : base - 15] = (left2[far_n - 2 :] + jnp.concatenate(
        [valid(has_l2, left[0:1]), left[1:2]], axis=0)).astype(BF16)
    c_ref[base - 15 : base - 1] = left[2 : coef_n - 2].astype(BF16)
    c_ref[base - 1 : base + 1] = (left[coef_n - 2 :] + jnp.concatenate(
        [valid(has_l1, own[0:1]), own[1:2]], axis=0)).astype(BF16)
    c_ref[base + 1 : base + 15] = own[2 : coef_n - 2].astype(BF16)
    c_ref[base + 15 : base + 17] = (right[:2] + jnp.concatenate(
        [own[coef_n - 2 : coef_n - 1], valid(has_r1, own[coef_n - 1 :])], axis=0)).astype(BF16)
    c_ref[base + 17 : base + 31] = right[2 : coef_n - 2].astype(BF16)
    c_ref[base + 31 : base + 33] = (right2[:2] + jnp.concatenate(
        [right[coef_n - 2 : coef_n - 1], valid(has_r2, right[coef_n - 1 :])], axis=0)).astype(BF16)
    c_ref[base + 33 : base + 31 + far_n] = right2[2:].astype(BF16)

    at = coef_n
    far_rows = 48
    for step in range(2):
        lo = at + 4 * step
        for ref_rows, flag, pos in ((0, odd_unit, -32), (1, jnp.logical_not(odd_unit), 32)):
            hi_v = choose(flag, a1_ref, b1_ref, lo, lo + 2)
            lo_v = choose(flag, a1_ref, b1_ref, lo + 2, lo + 4)
            slow_ref[step, far_rows + pos : far_rows + pos + 32] = (hi_v + lo_v).reshape(32, LANES)
        slow_ref[step, far_rows : far_rows + 32] = (
            near_ref[lo : lo + 2].astype(F32) + near_ref[lo + 2 : lo + 4].astype(F32)
        ).reshape(32, LANES)
    for flag, pos in ((odd_quad, -48), (jnp.logical_not(odd_quad), 64)):
        rows = choose(flag, a2_ref, b2_ref, far_n, far_n + 1) + choose(
            flag, a2_ref, b2_ref, far_n + 1, far_n + 2
        )
        slow_ref[0, far_rows + pos : far_rows + pos + 16] = rows[0]
    slow_ref[2, far_rows : far_rows + 32] = (
        last_ref[0:2].astype(F32) + last_ref[2:4].astype(F32)
    ).reshape(32, LANES)

    for step in range(STEPS):
        pos = coef_n + 8 + step
        pick_ref[step, 32:48] = near_ref[pos].astype(F32)
        pick_ref[step, 16:32] = jnp.where(
            has_l1, choose(odd_unit, a1_ref, b1_ref, pos, pos + 1)[0], -1.0)
        pick_ref[step, 48:64] = jnp.where(
            has_r1, choose(odd_unit, b1_ref, a1_ref, pos, pos + 1)[0], -1.0)
    pick_ref[0, 0:16] = jnp.where(
        has_l2, choose(odd_quad, a2_ref, b2_ref, far_n + 2, far_n + 3)[0], -1.0)
    pick_ref[0, 64:80] = jnp.where(
        has_r2, choose(odd_quad, b2_ref, a2_ref, far_n + 2, far_n + 3)[0], -1.0)

    scale = scale_ref[0]
    row8 = lax.broadcasted_iota(jnp.int32, (1, 8, LANES), 1)
    sign = jnp.where(row8 < 4, 1.0, -1.0).astype(F32)
    lane3 = low_lanes((1, 1, LANES))
    lane2 = low_lanes((1, LANES))

    def table_rows(parity):
        zero = jnp.zeros((COEFS, tables * LANES), BF16)
        full = jnp.concatenate([table_ref[t] for t in range(tables)], axis=1)
        return jnp.concatenate([full, zero] if parity == 0 else [zero, full], axis=0)

    plan = (
        dict(lo=-18, hi=34, base=26, first=-17),
        dict(lo=-9, hi=25, base=17, first=-9),
        dict(lo=-1, hi=17, base=9, first=0),
    )
    for step, item in enumerate(plan):
        lo, hi = item["lo"], item["hi"]
        count = hi - lo
        off = item["base"] + lo - 8
        rows = pick_ref[step, lo + 32 : hi + 32]
        swapped = lane_swap(rows)
        for parity, v_ref in ((0, ve_ref), (1, vo_ref)):
            lhs = jnp.concatenate(
                [c_ref[off + k : off + k + count].reshape(count * 16, LANES) for k in range(17)],
                axis=1,
            )
            out = jnp.dot(lhs, table_rows(parity), preferred_element_type=F32)
            pick = jnp.where(lane2, rows, swapped) if parity == 0 else jnp.where(lane2, swapped, rows)
            pick = pick.reshape(count, 1, LANES)
            v = jnp.zeros((count, 16, LANES), F32)
            for t in range(tables):
                v = jnp.where(
                    pick == float(t), out[:, LANES * t : LANES * (t + 1)].reshape(count, 16, LANES), v
                )
            v_ref[0:count] = v
        ve, vo = ve_ref[0:count], vo_ref[0:count]
        x = jnp.where(lane3, ve, lane_swap(vo))
        y = jnp.where(lane3, lane_swap(ve), vo)
        prop = jnp.concatenate(
            [x[:, :8] - sign * y[:, 8:], x[:, 8:] + sign * y[:, :8]], axis=1
        )
        p_ref[0] = jnp.zeros((16, LANES), BF16)
        p_ref[1 : count + 1] = prop.astype(BF16)
        first = item["first"]
        n = hi - first
        o = first - lo
        lhs = jnp.concatenate(
            [p_ref[o : o + n].reshape(n * 16, LANES), p_ref[o + 1 : o + 1 + n].reshape(n * 16, LANES)],
            axis=1,
        )
        back = jnp.dot(lhs, inverse_ref[...], preferred_element_type=F32)
        g0 = 2 * first + far_rows
        before = slow_ref[step, g0 - 1 : g0 - 1 + 2 * n]
        after = slow_ref[step, g0 : g0 + 2 * n]
        if step < 2:
            number = lax.broadcasted_iota(jnp.int32, (2 * n, 1), 0) + 2 * first
            def exists(block):
                inside = (block >= 0) & (block < 32)
                l1 = (block < 0) & (block >= -32) & has_l1
                r1 = (block >= 32) & (block < 64) & has_r1
                l2 = (block < -32) & has_l2
                r2 = (block >= 64) & has_r2
                return inside | l1 | r1 | l2 | r2
            ok = jnp.where(lane2, exists(number - 1).astype(jnp.int32), exists(number).astype(jnp.int32)) > 0
        theta = scale * jnp.where(lane2, lane_swap(before), lane_swap(after))
        sin_v, cos_v = sin_cos(theta)
        if step < 2:
            sin_v = jnp.where(ok, sin_v, 0.0)
            cos_v = jnp.where(ok, cos_v, 0.0)
        cos_ref[0 : 2 * n] = cos_v
        sin_ref[0 : 2 * n] = sin_v
        images = []
        for parity, x_ref in ((0, xe_ref), (1, xo_ref)):
            b = back[:, LANES * parity : LANES * (parity + 1)].reshape(n, 16, LANES)
            c = cos_ref[pl.ds(parity, n, stride=2)].reshape(n, 1, LANES)
            s = sin_ref[pl.ds(parity, n, stride=2)].reshape(n, 1, LANES) * sign
            f0 = c * b[:, :8] - s * b[:, 8:]
            f1 = c * b[:, 8:] + s * b[:, :8]
            if step < 2:
                x_ref[0:n] = jnp.concatenate([f0, f1], axis=1).astype(BF16)
            m = 17 - parity
            f0, f1 = f0[-first : -first + m], f1[-first : -first + m]
            images.append(lane_swap(f0 * pltpu.roll(f0, 4, 1) + f1 * pltpu.roll(f1, 4, 1)))
        even, odd = images
        image_ref[step, 0] = jnp.where(lane3, even[:16], odd)
        image_ref[step, 1] = jnp.where(lane3, odd, even[1:])
        if step < 2:
            if step == 1:
                xe_ref[n] = jnp.zeros((16, LANES), BF16)
                m = n
            else:
                m = n - 1
            lhs = jnp.concatenate(
                [
                    xe_ref[0:m].reshape(m * 16, LANES),
                    xo_ref[0:m].reshape(m * 16, LANES),
                    xe_ref[1 : m + 1].reshape(m * 16, LANES),
                ],
                axis=1,
            )
            coefs = jnp.dot(lhs, forward_ref[...], preferred_element_type=F32).reshape(m, 16, LANES)
            number = lax.broadcasted_iota(jnp.int32, (m, 1, 1), 0) + first
            ok = (
                ((number >= 0) & (number < 16))
                | ((number < 0) & (number >= -16) & has_l1)
                | ((number >= 16) & (number < 32) & has_r1)
                | ((number < -16) & has_l2)
                | ((number >= 32) & has_r2)
            )
            c_ref[0:m] = jnp.where(ok, coefs, 0.0).astype(BF16)
    row3 = row8 < 4
    for ref, half in ((keep_ref, second), (send_ref, 1 - second)):
        for parity in range(2):
            span = pl.ds(8 * half, 8)
            top = jnp.where(row3, image_ref[0, parity, span], image_ref[1, parity, span])
            ref[parity] = jnp.concatenate([top, image_ref[2, parity, span]], axis=1).astype(BF16)


def final_kernel(a_ref, b_ref, out_ref):
    total = a_ref[...].astype(F32) + b_ref[...].astype(F32)
    for parity in range(2):
        for q in range(8):
            cut = slice(WINDOW * (2 * q + parity), WINDOW * (2 * q + parity + 1))
            for n in range(STEPS):
                out_ref[n, :, cut] = total[parity, q, 4 * n : 4 * n + 4]


def matching(size, by, odd):
    pairs = []
    for i in range(size):
        right = (i // by) % 2 == odd
        j = i + by if right else i - by
        pairs.append((i, j if 0 <= j < size else i))
    return pairs


def on_device(wavefield, propagator_table, table_index, slowness, frequency_scale):
    sources = wavefield.shape[2]
    points = wavefield.shape[3]
    lat = lax.axis_size("lat")
    freqs = lax.axis_size("freq")
    pairs = points // (2 * WINDOW)
    first, forward, inverse = (jnp.asarray(m, BF16) for m in pair_matrices())
    vmem = pl.BlockSpec(memory_space=pltpu.VMEM)
    smem = pl.BlockSpec(memory_space=pltpu.SMEM)

    def tiles(n):
        return jax.ShapeDtypeStruct((n, 16, LANES), BF16)

    info = 8
    keep, send = pl.pallas_call(
        prep_kernel,
        out_shape=(tiles(pairs + 2), tiles(pairs + 2 + info)),
        in_specs=[vmem, vmem, smem, vmem],
        out_specs=(vmem, vmem),
        scratch_shapes=[
            pltpu.VMEM((2, pairs + 2, 16, LANES), BF16),
            pltpu.VMEM((info * 16, LANES), F32),
        ],
        name="prep",
    )(wavefield, slowness, table_index, first)
    partner = [(i, i ^ 1) for i in range(lat)]
    got = lax.ppermute(send, "lat", partner)
    near_n = 2 * (pairs + 2) - 2 + 8 + STEPS
    far_n = 11 + 3
    near, far_a, far_b, last = pl.pallas_call(
        unit_kernel,
        out_shape=(tiles(near_n), tiles(far_n), tiles(far_n), tiles(4)),
        in_specs=[vmem] * 3,
        out_specs=(vmem,) * 4,
        name="unit",
    )(keep, send, got)
    a1 = lax.ppermute(near, "lat", matching(lat, 2, 0))
    b1 = lax.ppermute(near, "lat", matching(lat, 2, 1))
    a2 = lax.ppermute(far_a, "lat", matching(lat, 4, 0))
    b2 = lax.ppermute(far_b, "lat", matching(lat, 4, 1))
    image = jax.ShapeDtypeStruct((2, pairs, 16, LANES), BF16)
    own, other = pl.pallas_call(
        lambda *refs: main_kernel(lat // 2, *refs),
        out_shape=(image, image),
        in_specs=[vmem] * 9 + [smem],
        out_specs=(vmem, vmem),
        scratch_shapes=[
            pltpu.VMEM((68, 16, LANES), BF16),
            pltpu.VMEM((53, 16, LANES), BF16),
            pltpu.VMEM((52, 16, LANES), F32),
            pltpu.VMEM((52, 16, LANES), F32),
            pltpu.VMEM((52, 16, LANES), BF16),
            pltpu.VMEM((52, 16, LANES), BF16),
            pltpu.VMEM((STEPS, 128, LANES), F32),
            pltpu.VMEM((104, LANES), F32),
            pltpu.VMEM((104, LANES), F32),
            pltpu.VMEM((STEPS, 80, LANES), F32),
            pltpu.VMEM((STEPS, 2, 16, 8, LANES), F32),
        ],
        name="steps",
    )(near, last, a1, b1, a2, b2, propagator_table[0], forward, inverse, frequency_scale)
    swapped = lax.ppermute(other, "lat", partner)
    core = lax.rem(lax.axis_index("lat"), 2)
    if freqs == 2:
        mine = core == lax.axis_index("freq")
        stay = jnp.where(mine, own, swapped)
        leave = jnp.where(mine, swapped, own)
        come = lax.ppermute(leave, "freq", [(0, 1), (1, 0)])
        return pl.pallas_call(
            final_kernel,
            out_shape=jax.ShapeDtypeStruct((STEPS, sources // 2, points), F32),
            in_specs=[vmem, vmem],
            out_specs=vmem,
            name="total",
        )(stay, come)
    low = jnp.where(core == 0, own, swapped)
    high = jnp.where(core == 0, swapped, own)
    whole = jnp.stack([low, high])[:, :, :, : 4 * STEPS]
    whole = whole.reshape(2, 2, pairs, STEPS, 4, LANES)
    whole = jnp.transpose(whole, (3, 0, 4, 2, 1, 5)).reshape(STEPS, sources, points)
    return lax.psum_scatter(whole, "freq", scatter_dimension=1, tiled=True).astype(F32)


def solution(mesh):
    placed = (
        P(None, "freq", None, "lat"),
        P("freq", None, None, None),
        P(None, "lat"),
        P(None, "lat"),
        P("freq"),
    )
    return jax.shard_map(
        on_device, mesh=mesh, in_specs=placed, out_specs=P(None, "freq", "lat"), check_vma=False
    )
```

```python
import math

import jax
import jax.numpy as jnp
import numpy as np
from jax import lax
from jax.experimental import pallas as pl
from jax.experimental.pallas import tpu as pltpu
from jax.sharding import PartitionSpec as P

WINDOW = 128
COEFS = 64
REACH = 16
STEPS = 3
HALF = WINDOW // 2
F32 = jnp.float32
BF16 = jnp.bfloat16
LANES = 2 * COEFS


def basis_table():
    t = np.arange(2 * WINDOW, dtype=np.float32)[:, None]
    k = np.arange(COEFS, dtype=np.float32)[None, :]
    taper = np.sin(np.float32(math.pi) * (t + np.float32(0.5)) / np.float32(2 * WINDOW))
    wave = np.cos(
        np.float32(math.pi)
        * (k + np.float32(0.5))
        * (t - np.float32(HALF) + np.float32(0.5))
        / np.float32(WINDOW)
    )
    return (taper * np.float32(math.sqrt(2.0 / WINDOW)) * wave).astype(np.float32)


def pair_matrices():
    b = basis_table()
    first = np.zeros((4 * WINDOW, LANES), np.float32)
    first[HALF : HALF + 2 * WINDOW, :COEFS] = b
    first[HALF + WINDOW : HALF + 3 * WINDOW, COEFS:] = b
    forward = np.zeros((3 * WINDOW, LANES), np.float32)
    forward[: 2 * WINDOW, :COEFS] = b
    forward[WINDOW:, COEFS:] = b
    inverse = np.zeros((4 * COEFS, 2 * WINDOW), np.float32)
    inverse[COEFS : 2 * COEFS, :WINDOW] = b[WINDOW:].T
    inverse[2 * COEFS : 3 * COEFS, :WINDOW] = b[:WINDOW].T
    inverse[2 * COEFS : 3 * COEFS, WINDOW:] = b[WINDOW:].T
    inverse[3 * COEFS :, WINDOW:] = b[:WINDOW].T
    return first, forward, inverse


def sin_cos(theta):
    turns = jnp.floor(theta * np.float32(2.0 / math.pi) + np.float32(0.5))
    r = theta - turns * np.float32(1.5703125)
    r = r - turns * np.float32(4.837512969970703e-4)
    r = r - turns * np.float32(7.549789948768648e-8)
    r2 = r * r
    s = r + r * r2 * (
        np.float32(-1.6666654611e-1)
        + r2 * (np.float32(8.3321608736e-3) + r2 * np.float32(-1.9515295891e-4))
    )
    c = 1.0 - 0.5 * r2 + r2 * r2 * (
        np.float32(4.166664568298827e-2)
        + r2 * (np.float32(-1.388731625493765e-3) + r2 * np.float32(2.443315711809948e-5))
    )
    quarter = turns - 4.0 * jnp.floor(turns * 0.25)
    odd = (quarter == 1.0) | (quarter == 3.0)
    sin_v = jnp.where(odd, c, s)
    cos_v = jnp.where(odd, s, c)
    sin_v = jnp.where(quarter >= 2.0, -sin_v, sin_v)
    cos_v = jnp.where((quarter == 1.0) | (quarter == 2.0), -cos_v, cos_v)
    return sin_v, cos_v


def lane_swap(v):
    return pltpu.roll(v, LANES // 2, v.ndim - 1)


def low_lanes(shape):
    return lax.broadcasted_iota(jnp.int32, shape, len(shape) - 1) < LANES // 2


def prep_kernel(wave_ref, slow_ref, index_ref, first_ref, keep_ref, send_ref, both_ref, rows_ref):
    core = lax.rem(lax.axis_index("lat"), 2)
    blocks = wave_ref.shape[-1] // WINDOW
    pairs = blocks // 2
    upper = lax.broadcasted_iota(jnp.int32, (8, wave_ref.shape[-1]), 0) < 4
    for side in range(2):
        halves = []
        for low in range(2):
            near, far = wave_ref[low, 0], wave_ref[low + 2, 0]
            if side == 0:
                halves.append(jnp.where(upper, near, pltpu.roll(far, 4, 0)))
            else:
                halves.append(jnp.where(upper, pltpu.roll(near, 4, 0), far))
        samples = jnp.concatenate(halves, axis=0).astype(BF16)
        zero = jnp.zeros((16, WINDOW), BF16)
        padded = [zero] * 3
        padded += [samples[:, WINDOW * g : WINDOW * (g + 1)] for g in range(blocks)]
        padded += [zero] * 3
        parts = [
            jnp.concatenate([padded[2 * i + j] for i in range(pairs + 2)], axis=0)
            for j in range(4)
        ]
        coefs = jnp.dot(
            jnp.concatenate(parts, axis=1), first_ref[...], preferred_element_type=F32
        )
        both_ref[side] = coefs.reshape(pairs + 2, 16, LANES).astype(BF16)
    keep_ref[...] = both_ref[core]
    send_ref[0 : pairs + 2] = both_ref[1 - core]
    slow = slow_ref[...]
    high = slow.astype(BF16).astype(F32)
    rest = slow - high
    lanes = low_lanes((1, LANES))
    rows_ref[...] = jnp.zeros(rows_ref.shape, F32)
    for n in range(STEPS):
        for g in range(blocks):
            cut = slice(WINDOW * g, WINDOW * (g + 1))
            rows_ref[(2 * n) * blocks + g : (2 * n) * blocks + g + 1, :] = high[n : n + 1, cut]
            rows_ref[(2 * n + 1) * blocks + g : (2 * n + 1) * blocks + g + 1, :] = rest[n : n + 1, cut]
        for q in range(pairs):
            at = 2 * STEPS * blocks + n * pairs + q
            rows_ref[at : at + 1, :] = jnp.where(
                lanes,
                jnp.full((1, LANES), index_ref[n, 2 * q], jnp.int32),
                jnp.full((1, LANES), index_ref[n, 2 * q + 1], jnp.int32),
            ).astype(F32)
    send_ref[pairs + 2 :] = rows_ref[...].reshape(-1, 16, LANES).astype(BF16)


def unit_kernel(keep_ref, sent_ref, got_ref, near_ref, far_a_ref, far_b_ref, last_ref):
    place = lax.axis_index("lat")
    second = lax.rem(place, 2) == 1
    n = keep_ref.shape[0]
    own_c, own_i = keep_ref[...].astype(F32), sent_ref[n:].astype(F32)
    got_c, got_i = got_ref[:n].astype(F32), got_ref[n:].astype(F32)
    b0 = jnp.where(second, got_c, own_c)
    b1 = jnp.where(second, own_c, got_c)
    i0 = jnp.where(second, got_i, own_i)
    i1 = jnp.where(second, own_i, got_i)
    unit = jnp.concatenate([b0[: n - 2], b0[n - 2 :] + b1[:2], b1[2:]], axis=0)
    near_ref[0 : 2 * n - 2] = unit.astype(BF16)
    at = 2 * n - 2
    for step in range(2):
        for part in range(2):
            near_ref[at] = i0[2 * step + part].astype(BF16)
            near_ref[at + 1] = i1[2 * step + part].astype(BF16)
            at += 2
    near_ref[at] = jnp.concatenate([i0[6, :8], i1[6, :8]], axis=0).astype(BF16)
    near_ref[at + 1] = jnp.concatenate([i0[6, 8:], i1[6, 8:]], axis=0).astype(BF16)
    near_ref[at + 2] = jnp.concatenate([i0[7, :8], i1[7, :8]], axis=0).astype(BF16)
    for part in range(2):
        last_ref[2 * part] = i0[4 + part].astype(BF16)
        last_ref[2 * part + 1] = i1[4 + part].astype(BF16)
    even_quad = lax.rem(lax.div(place, 4), 2) == 0
    count = far_a_ref.shape[0] - 3
    base = 2 * n - 2
    for ref, right in ((far_a_ref, even_quad), (far_b_ref, jnp.logical_not(even_quad))):
        start = jnp.where(right, base - count, 0)
        pick = jnp.where(right, 1, 0)
        ref[0:count] = near_ref[pl.ds(start, count)]
        ref[count] = near_ref[base + pick]
        ref[count + 1] = near_ref[base + 2 + pick]
        ref[count + 2] = near_ref[base + 8]


def main_kernel(
    units,
    near_ref,
    last_ref,
    a1_ref,
    b1_ref,
    a2_ref,
    b2_ref,
    table_ref,
    forward_ref,
    inverse_ref,
    scale_ref,
    keep_ref,
    send_ref,
    c_ref,
    p_ref,
    ve_ref,
    vo_ref,
    xe_ref,
    xo_ref,
    slow_ref,
    cos_ref,
    sin_ref,
    pick_ref,
    image_ref,
):
    place = lax.axis_index("lat")
    unit = lax.div(place, 2)
    second = lax.rem(place, 2)
    odd_unit = lax.rem(unit, 2) == 1
    odd_quad = lax.rem(lax.div(place, 4), 2) == 1
    has_l1, has_l2 = unit >= 1, unit >= 2
    has_r1, has_r2 = unit + 1 < units, unit + 2 < units
    pairs = 16
    coef_n = pairs + 2
    far_n = a2_ref.shape[0] - 3
    tables = table_ref.shape[0]

    def valid(flag, v):
        return jnp.where(flag, v, jnp.zeros_like(v))

    def choose(flag, x_ref, y_ref, lo, hi):
        return jnp.where(flag, x_ref[lo:hi], y_ref[lo:hi]).astype(F32)

    base = 26
    own = near_ref[0:coef_n].astype(F32)
    left = valid(has_l1, choose(odd_unit, a1_ref, b1_ref, 0, coef_n))
    right = valid(has_r1, choose(odd_unit, b1_ref, a1_ref, 0, coef_n))
    left2 = valid(has_l2, choose(odd_quad, a2_ref, b2_ref, 0, far_n))
    right2 = valid(has_r2, choose(odd_quad, b2_ref, a2_ref, 0, far_n))
    c_ref[0 : far_n - 2] = left2[: far_n - 2].astype(BF16)
    c_ref[base - 17 : base - 15] = (left2[far_n - 2 :] + jnp.concatenate(
        [valid(has_l2, left[0:1]), left[1:2]], axis=0)).astype(BF16)
    c_ref[base - 15 : base - 1] = left[2 : coef_n - 2].astype(BF16)
    c_ref[base - 1 : base + 1] = (left[coef_n - 2 :] + jnp.concatenate(
        [valid(has_l1, own[0:1]), own[1:2]], axis=0)).astype(BF16)
    c_ref[base + 1 : base + 15] = own[2 : coef_n - 2].astype(BF16)
    c_ref[base + 15 : base + 17] = (right[:2] + jnp.concatenate(
        [own[coef_n - 2 : coef_n - 1], valid(has_r1, own[coef_n - 1 :])], axis=0)).astype(BF16)
    c_ref[base + 17 : base + 31] = right[2 : coef_n - 2].astype(BF16)
    c_ref[base + 31 : base + 33] = (right2[:2] + jnp.concatenate(
        [right[coef_n - 2 : coef_n - 1], valid(has_r2, right[coef_n - 1 :])], axis=0)).astype(BF16)
    c_ref[base + 33 : base + 31 + far_n] = right2[2:].astype(BF16)

    at = coef_n
    far_rows = 48
    for step in range(2):
        lo = at + 4 * step
        for ref_rows, flag, pos in ((0, odd_unit, -32), (1, jnp.logical_not(odd_unit), 32)):
            hi_v = choose(flag, a1_ref, b1_ref, lo, lo + 2)
            lo_v = choose(flag, a1_ref, b1_ref, lo + 2, lo + 4)
            slow_ref[step, far_rows + pos : far_rows + pos + 32] = (hi_v + lo_v).reshape(32, LANES)
        slow_ref[step, far_rows : far_rows + 32] = (
            near_ref[lo : lo + 2].astype(F32) + near_ref[lo + 2 : lo + 4].astype(F32)
        ).reshape(32, LANES)
    for flag, pos in ((odd_quad, -48), (jnp.logical_not(odd_quad), 64)):
        rows = choose(flag, a2_ref, b2_ref, far_n, far_n + 1) + choose(
            flag, a2_ref, b2_ref, far_n + 1, far_n + 2
        )
        slow_ref[0, far_rows + pos : far_rows + pos + 16] = rows[0]
    slow_ref[2, far_rows : far_rows + 32] = (
        last_ref[0:2].astype(F32) + last_ref[2:4].astype(F32)
    ).reshape(32, LANES)

    for step in range(STEPS):
        pos = coef_n + 8 + step
        pick_ref[step, 32:48] = near_ref[pos].astype(F32)
        pick_ref[step, 16:32] = jnp.where(
            has_l1, choose(odd_unit, a1_ref, b1_ref, pos, pos + 1)[0], -1.0)
        pick_ref[step, 48:64] = jnp.where(
            has_r1, choose(odd_unit, b1_ref, a1_ref, pos, pos + 1)[0], -1.0)
    pick_ref[0, 0:16] = jnp.where(
        has_l2, choose(odd_quad, a2_ref, b2_ref, far_n + 2, far_n + 3)[0], -1.0)
    pick_ref[0, 64:80] = jnp.where(
        has_r2, choose(odd_quad, b2_ref, a2_ref, far_n + 2, far_n + 3)[0], -1.0)

    scale = scale_ref[0]
    row8 = lax.broadcasted_iota(jnp.int32, (1, 8, LANES), 1)
    sign = jnp.where(row8 < 4, 1.0, -1.0).astype(F32)
    lane3 = low_lanes((1, 1, LANES))
    lane2 = low_lanes((1, LANES))

    def table_rows(parity):
        zero = jnp.zeros((COEFS, tables * LANES), BF16)
        full = jnp.concatenate([table_ref[t] for t in range(tables)], axis=1)
        return jnp.concatenate([full, zero] if parity == 0 else [zero, full], axis=0)

    plan = (
        dict(lo=-18, hi=34, base=26, first=-17),
        dict(lo=-9, hi=25, base=17, first=-9),
        dict(lo=-1, hi=17, base=9, first=0),
    )
    for step, item in enumerate(plan):
        lo, hi = item["lo"], item["hi"]
        count = hi - lo
        off = item["base"] + lo - 8
        rows = pick_ref[step, lo + 32 : hi + 32]
        swapped = lane_swap(rows)
        for parity, v_ref in ((0, ve_ref), (1, vo_ref)):
            lhs = jnp.concatenate(
                [c_ref[off + k : off + k + count].reshape(count * 16, LANES) for k in range(17)],
                axis=1,
            )
            out = jnp.dot(lhs, table_rows(parity), preferred_element_type=F32)
            pick = jnp.where(lane2, rows, swapped) if parity == 0 else jnp.where(lane2, swapped, rows)
            pick = pick.reshape(count, 1, LANES)
            v = jnp.zeros((count, 16, LANES), F32)
            for t in range(tables):
                v = jnp.where(
                    pick == float(t), out[:, LANES * t : LANES * (t + 1)].reshape(count, 16, LANES), v
                )
            v_ref[0:count] = v
        ve, vo = ve_ref[0:count], vo_ref[0:count]
        x = jnp.where(lane3, ve, lane_swap(vo))
        y = jnp.where(lane3, lane_swap(ve), vo)
        prop = jnp.concatenate(
            [x[:, :8] - sign * y[:, 8:], x[:, 8:] + sign * y[:, :8]], axis=1
        )
        p_ref[0] = jnp.zeros((16, LANES), BF16)
        p_ref[1 : count + 1] = prop.astype(BF16)
        first = item["first"]
        n = hi - first
        o = first - lo
        lhs = jnp.concatenate(
            [p_ref[o : o + n].reshape(n * 16, LANES), p_ref[o + 1 : o + 1 + n].reshape(n * 16, LANES)],
            axis=1,
        )
        back = jnp.dot(lhs, inverse_ref[...], preferred_element_type=F32)
        g0 = 2 * first + far_rows
        before = slow_ref[step, g0 - 1 : g0 - 1 + 2 * n]
        after = slow_ref[step, g0 : g0 + 2 * n]
        if step < 2:
            number = lax.broadcasted_iota(jnp.int32, (2 * n, 1), 0) + 2 * first
            def exists(block):
                inside = (block >= 0) & (block < 32)
                l1 = (block < 0) & (block >= -32) & has_l1
                r1 = (block >= 32) & (block < 64) & has_r1
                l2 = (block < -32) & has_l2
                r2 = (block >= 64) & has_r2
                return inside | l1 | r1 | l2 | r2
            ok = jnp.where(lane2, exists(number - 1).astype(jnp.int32), exists(number).astype(jnp.int32)) > 0
        theta = scale * jnp.where(lane2, lane_swap(before), lane_swap(after))
        sin_v, cos_v = sin_cos(theta)
        if step < 2:
            sin_v = jnp.where(ok, sin_v, 0.0)
            cos_v = jnp.where(ok, cos_v, 0.0)
        cos_ref[0 : 2 * n] = cos_v
        sin_ref[0 : 2 * n] = sin_v
        images = []
        for parity, x_ref in ((0, xe_ref), (1, xo_ref)):
            b = back[:, LANES * parity : LANES * (parity + 1)].reshape(n, 16, LANES)
            c = cos_ref[pl.ds(parity, n, stride=2)].reshape(n, 1, LANES)
            s = sin_ref[pl.ds(parity, n, stride=2)].reshape(n, 1, LANES) * sign
            f0 = c * b[:, :8] - s * b[:, 8:]
            f1 = c * b[:, 8:] + s * b[:, :8]
            if step < 2:
                x_ref[0:n] = jnp.concatenate([f0, f1], axis=1).astype(BF16)
            m = 17 - parity
            f0, f1 = f0[-first : -first + m], f1[-first : -first + m]
            images.append(lane_swap(f0 * pltpu.roll(f0, 4, 1) + f1 * pltpu.roll(f1, 4, 1)))
        even, odd = images
        image_ref[step, 0] = jnp.where(lane3, even[:16], odd)
        image_ref[step, 1] = jnp.where(lane3, odd, even[1:])
        if step < 2:
            if step == 1:
                xe_ref[n] = jnp.zeros((16, LANES), BF16)
                m = n
            else:
                m = n - 1
            lhs = jnp.concatenate(
                [
                    xe_ref[0:m].reshape(m * 16, LANES),
                    xo_ref[0:m].reshape(m * 16, LANES),
                    xe_ref[1 : m + 1].reshape(m * 16, LANES),
                ],
                axis=1,
            )
            coefs = jnp.dot(lhs, forward_ref[...], preferred_element_type=F32).reshape(m, 16, LANES)
            number = lax.broadcasted_iota(jnp.int32, (m, 1, 1), 0) + first
            ok = (
                ((number >= 0) & (number < 16))
                | ((number < 0) & (number >= -16) & has_l1)
                | ((number >= 16) & (number < 32) & has_r1)
                | ((number < -16) & has_l2)
                | ((number >= 32) & has_r2)
            )
            c_ref[0:m] = jnp.where(ok, coefs, 0.0).astype(BF16)
    row3 = row8 < 4
    for ref, half in ((keep_ref, second), (send_ref, 1 - second)):
        for parity in range(2):
            span = pl.ds(8 * half, 8)
            top = jnp.where(row3, image_ref[0, parity, span], image_ref[1, parity, span])
            ref[parity] = jnp.concatenate([top, image_ref[2, parity, span]], axis=1).astype(BF16)


def final_kernel(a_ref, b_ref, out_ref):
    total = a_ref[...].astype(F32) + b_ref[...].astype(F32)
    for parity in range(2):
        for q in range(8):
            cut = slice(WINDOW * (2 * q + parity), WINDOW * (2 * q + parity + 1))
            for n in range(STEPS):
                out_ref[n, :, cut] = total[parity, q, 4 * n : 4 * n + 4]


def matching(size, by, odd):
    pairs = []
    for i in range(size):
        right = (i // by) % 2 == odd
        j = i + by if right else i - by
        pairs.append((i, j if 0 <= j < size else i))
    return pairs


def on_device(wavefield, propagator_table, table_index, slowness, frequency_scale):
    sources = wavefield.shape[2]
    points = wavefield.shape[3]
    lat = lax.axis_size("lat")
    freqs = lax.axis_size("freq")
    pairs = points // (2 * WINDOW)
    first, forward, inverse = (jnp.asarray(m, BF16) for m in pair_matrices())
    vmem = pl.BlockSpec(memory_space=pltpu.VMEM)
    smem = pl.BlockSpec(memory_space=pltpu.SMEM)

    def tiles(n):
        return jax.ShapeDtypeStruct((n, 16, LANES), BF16)

    info = 8
    keep, send = pl.pallas_call(
        prep_kernel,
        out_shape=(tiles(pairs + 2), tiles(pairs + 2 + info)),
        in_specs=[vmem, vmem, smem, vmem],
        out_specs=(vmem, vmem),
        scratch_shapes=[
            pltpu.VMEM((2, pairs + 2, 16, LANES), BF16),
            pltpu.VMEM((info * 16, LANES), F32),
        ],
        compiler_params=pltpu.CompilerParams(vmem_limit_bytes=8 << 20),
        name="prep",
    )(wavefield, slowness, table_index, first)
    partner = [(i, i ^ 1) for i in range(lat)]
    got = lax.ppermute(send, "lat", partner)
    near_n = 2 * (pairs + 2) - 2 + 8 + STEPS
    far_n = 11 + 3
    near, far_a, far_b, last = pl.pallas_call(
        unit_kernel,
        out_shape=(tiles(near_n), tiles(far_n), tiles(far_n), tiles(4)),
        in_specs=[vmem] * 3,
        out_specs=(vmem,) * 4,
        compiler_params=pltpu.CompilerParams(vmem_limit_bytes=4 << 20),
        name="unit",
    )(keep, send, got)
    a1 = lax.ppermute(near, "lat", matching(lat, 2, 0))
    b1 = lax.ppermute(near, "lat", matching(lat, 2, 1))
    a2 = lax.ppermute(far_a, "lat", matching(lat, 4, 0))
    b2 = lax.ppermute(far_b, "lat", matching(lat, 4, 1))
    image = jax.ShapeDtypeStruct((2, pairs, 16, LANES), BF16)
    own, other = pl.pallas_call(
        lambda *refs: main_kernel(lat // 2, *refs),
        out_shape=(image, image),
        in_specs=[vmem] * 9 + [smem],
        out_specs=(vmem, vmem),
        scratch_shapes=[
            pltpu.VMEM((68, 16, LANES), BF16),
            pltpu.VMEM((53, 16, LANES), BF16),
            pltpu.VMEM((52, 16, LANES), F32),
            pltpu.VMEM((52, 16, LANES), F32),
            pltpu.VMEM((52, 16, LANES), BF16),
            pltpu.VMEM((52, 16, LANES), BF16),
            pltpu.VMEM((STEPS, 128, LANES), F32),
            pltpu.VMEM((104, LANES), F32),
            pltpu.VMEM((104, LANES), F32),
            pltpu.VMEM((STEPS, 80, LANES), F32),
            pltpu.VMEM((STEPS, 2, 16, 8, LANES), F32),
        ],
        compiler_params=pltpu.CompilerParams(vmem_limit_bytes=32 << 20),
        name="steps",
    )(near, last, a1, b1, a2, b2, propagator_table[0], forward, inverse, frequency_scale)
    swapped = lax.ppermute(other, "lat", partner)
    core = lax.rem(lax.axis_index("lat"), 2)
    if freqs == 2:
        mine = core == lax.axis_index("freq")
        stay = jnp.where(mine, own, swapped)
        leave = jnp.where(mine, swapped, own)
        come = lax.ppermute(leave, "freq", [(0, 1), (1, 0)])
        return pl.pallas_call(
            final_kernel,
            out_shape=jax.ShapeDtypeStruct((STEPS, sources // 2, points), F32),
            in_specs=[vmem, vmem],
            out_specs=vmem,
            compiler_params=pltpu.CompilerParams(vmem_limit_bytes=4 << 20),
            name="total",
        )(stay, come)
    low = jnp.where(core == 0, own, swapped)
    high = jnp.where(core == 0, swapped, own)
    whole = jnp.stack([low, high])[:, :, :, : 4 * STEPS]
    whole = whole.reshape(2, 2, pairs, STEPS, 4, LANES)
    whole = jnp.transpose(whole, (3, 0, 4, 2, 1, 5)).reshape(STEPS, sources, points)
    return lax.psum_scatter(whole, "freq", scatter_dimension=1, tiled=True).astype(F32)


def solution(mesh):
    placed = (
        P(None, "freq", None, "lat"),
        P("freq", None, None, None),
        P(None, "lat"),
        P(None, "lat"),
        P("freq"),
    )
    return jax.shard_map(
        on_device, mesh=mesh, in_specs=placed, out_specs=P(None, "freq", "lat"), check_vma=False
    )
```

```python
import math

import jax
import jax.numpy as jnp
import numpy as np
from jax import lax
from jax.experimental import pallas as pl
from jax.experimental.pallas import tpu as pltpu
from jax.sharding import PartitionSpec as P

WINDOW = 128
COEFS = 64
REACH = 16
STEPS = 3
HALF = WINDOW // 2
F32 = jnp.float32
BF16 = jnp.bfloat16
LANES = 2 * COEFS


def basis_table():
    t = np.arange(2 * WINDOW, dtype=np.float32)[:, None]
    k = np.arange(COEFS, dtype=np.float32)[None, :]
    taper = np.sin(np.float32(math.pi) * (t + np.float32(0.5)) / np.float32(2 * WINDOW))
    wave = np.cos(
        np.float32(math.pi)
        * (k + np.float32(0.5))
        * (t - np.float32(HALF) + np.float32(0.5))
        / np.float32(WINDOW)
    )
    return (taper * np.float32(math.sqrt(2.0 / WINDOW)) * wave).astype(np.float32)


def pair_matrices():
    b = basis_table()
    first = np.zeros((4 * WINDOW, LANES), np.float32)
    first[HALF : HALF + 2 * WINDOW, :COEFS] = b
    first[HALF + WINDOW : HALF + 3 * WINDOW, COEFS:] = b
    forward = np.zeros((3 * WINDOW, LANES), np.float32)
    forward[: 2 * WINDOW, :COEFS] = b
    forward[WINDOW:, COEFS:] = b
    inverse = np.zeros((4 * COEFS, 2 * WINDOW), np.float32)
    inverse[COEFS : 2 * COEFS, :WINDOW] = b[WINDOW:].T
    inverse[2 * COEFS : 3 * COEFS, :WINDOW] = b[:WINDOW].T
    inverse[2 * COEFS : 3 * COEFS, WINDOW:] = b[WINDOW:].T
    inverse[3 * COEFS :, WINDOW:] = b[:WINDOW].T
    return first, forward, inverse


def sin_cos(theta):
    turns = jnp.floor(theta * np.float32(2.0 / math.pi) + np.float32(0.5))
    r = theta - turns * np.float32(1.5703125)
    r = r - turns * np.float32(4.837512969970703e-4)
    r = r - turns * np.float32(7.549789948768648e-8)
    r2 = r * r
    s = r + r * r2 * (
        np.float32(-1.6666654611e-1)
        + r2 * (np.float32(8.3321608736e-3) + r2 * np.float32(-1.9515295891e-4))
    )
    c = 1.0 - 0.5 * r2 + r2 * r2 * (
        np.float32(4.166664568298827e-2)
        + r2 * (np.float32(-1.388731625493765e-3) + r2 * np.float32(2.443315711809948e-5))
    )
    quarter = turns - 4.0 * jnp.floor(turns * 0.25)
    odd = (quarter == 1.0) | (quarter == 3.0)
    sin_v = jnp.where(odd, c, s)
    cos_v = jnp.where(odd, s, c)
    sin_v = jnp.where(quarter >= 2.0, -sin_v, sin_v)
    cos_v = jnp.where((quarter == 1.0) | (quarter == 2.0), -cos_v, cos_v)
    return sin_v, cos_v


def lane_swap(v):
    return pltpu.roll(v, LANES // 2, v.ndim - 1)


def low_lanes(shape):
    return lax.broadcasted_iota(jnp.int32, shape, len(shape) - 1) < LANES // 2


def prep_kernel(
    wave_hbm,
    slow_hbm,
    index_hbm,
    first_hbm,
    keep_ref,
    send_ref,
    wave_ref,
    slow_ref,
    index_ref,
    first_ref,
    both_ref,
    rows_ref,
    sems,
):
    copies = [
        pltpu.make_async_copy(source, target, sems.at[i])
        for i, (source, target) in enumerate(
            (
                (wave_hbm, wave_ref),
                (first_hbm, first_ref),
                (slow_hbm, slow_ref),
                (index_hbm, index_ref),
            )
        )
    ]
    for copy in copies:
        copy.start()
    core = lax.rem(lax.axis_index("lat"), 2)
    copies[2].wait()
    copies[3].wait()
    blocks = wave_ref.shape[-1] // WINDOW
    pairs = blocks // 2
    slow = slow_ref[...]
    high = slow.astype(BF16).astype(F32)
    rest = slow - high
    lanes = low_lanes((1, LANES))
    rows_ref[...] = jnp.zeros(rows_ref.shape, F32)
    for n in range(STEPS):
        for g in range(blocks):
            cut = slice(WINDOW * g, WINDOW * (g + 1))
            rows_ref[(2 * n) * blocks + g : (2 * n) * blocks + g + 1, :] = high[n : n + 1, cut]
            rows_ref[(2 * n + 1) * blocks + g : (2 * n + 1) * blocks + g + 1, :] = rest[n : n + 1, cut]
        for q in range(pairs):
            at = 2 * STEPS * blocks + n * pairs + q
            rows_ref[at : at + 1, :] = jnp.where(
                lanes,
                jnp.full((1, LANES), index_ref[n, 2 * q], jnp.int32),
                jnp.full((1, LANES), index_ref[n, 2 * q + 1], jnp.int32),
            ).astype(F32)
    send_ref[pairs + 2 :] = rows_ref[...].reshape(-1, 16, LANES).astype(BF16)
    copies[0].wait()
    copies[1].wait()
    upper = lax.broadcasted_iota(jnp.int32, (8, wave_ref.shape[-1]), 0) < 4
    for side in range(2):
        halves = []
        for low in range(2):
            near, far = wave_ref[low, 0], wave_ref[low + 2, 0]
            if side == 0:
                halves.append(jnp.where(upper, near, pltpu.roll(far, 4, 0)))
            else:
                halves.append(jnp.where(upper, pltpu.roll(near, 4, 0), far))
        samples = jnp.concatenate(halves, axis=0).astype(BF16)
        zero = jnp.zeros((16, WINDOW), BF16)
        padded = [zero] * 3
        padded += [samples[:, WINDOW * g : WINDOW * (g + 1)] for g in range(blocks)]
        padded += [zero] * 3
        parts = [
            jnp.concatenate([padded[2 * i + j] for i in range(pairs + 2)], axis=0)
            for j in range(4)
        ]
        coefs = jnp.dot(
            jnp.concatenate(parts, axis=1), first_ref[...], preferred_element_type=F32
        )
        both_ref[side] = coefs.reshape(pairs + 2, 16, LANES).astype(BF16)
    keep_ref[...] = both_ref[core]
    send_ref[0 : pairs + 2] = both_ref[1 - core]


def unit_kernel(keep_ref, sent_ref, got_ref, near_ref, far_a_ref, far_b_ref, last_ref):
    place = lax.axis_index("lat")
    second = lax.rem(place, 2) == 1
    n = keep_ref.shape[0]
    own_c, own_i = keep_ref[...].astype(F32), sent_ref[n:].astype(F32)
    got_c, got_i = got_ref[:n].astype(F32), got_ref[n:].astype(F32)
    b0 = jnp.where(second, got_c, own_c)
    b1 = jnp.where(second, own_c, got_c)
    i0 = jnp.where(second, got_i, own_i)
    i1 = jnp.where(second, own_i, got_i)
    unit = jnp.concatenate([b0[: n - 2], b0[n - 2 :] + b1[:2], b1[2:]], axis=0)
    near_ref[0 : 2 * n - 2] = unit.astype(BF16)
    at = 2 * n - 2
    for step in range(2):
        for part in range(2):
            near_ref[at] = i0[2 * step + part].astype(BF16)
            near_ref[at + 1] = i1[2 * step + part].astype(BF16)
            at += 2
    near_ref[at] = jnp.concatenate([i0[6, :8], i1[6, :8]], axis=0).astype(BF16)
    near_ref[at + 1] = jnp.concatenate([i0[6, 8:], i1[6, 8:]], axis=0).astype(BF16)
    near_ref[at + 2] = jnp.concatenate([i0[7, :8], i1[7, :8]], axis=0).astype(BF16)
    for part in range(2):
        last_ref[2 * part] = i0[4 + part].astype(BF16)
        last_ref[2 * part + 1] = i1[4 + part].astype(BF16)
    even_quad = lax.rem(lax.div(place, 4), 2) == 0
    count = far_a_ref.shape[0] - 3
    base = 2 * n - 2
    for ref, right in ((far_a_ref, even_quad), (far_b_ref, jnp.logical_not(even_quad))):
        start = jnp.where(right, base - count, 0)
        pick = jnp.where(right, 1, 0)
        ref[0:count] = near_ref[pl.ds(start, count)]
        ref[count] = near_ref[base + pick]
        ref[count + 1] = near_ref[base + 2 + pick]
        ref[count + 2] = near_ref[base + 8]


def main_kernel(
    units,
    near_ref,
    last_ref,
    a1_ref,
    b1_ref,
    a2_ref,
    b2_ref,
    table_ref,
    forward_ref,
    inverse_ref,
    scale_ref,
    keep_ref,
    send_ref,
    c_ref,
    p_ref,
    ve_ref,
    vo_ref,
    xe_ref,
    xo_ref,
    slow_ref,
    cos_ref,
    sin_ref,
    pick_ref,
    image_ref,
):
    place = lax.axis_index("lat")
    unit = lax.div(place, 2)
    second = lax.rem(place, 2)
    odd_unit = lax.rem(unit, 2) == 1
    odd_quad = lax.rem(lax.div(place, 4), 2) == 1
    has_l1, has_l2 = unit >= 1, unit >= 2
    has_r1, has_r2 = unit + 1 < units, unit + 2 < units
    pairs = 16
    coef_n = pairs + 2
    far_n = a2_ref.shape[0] - 3
    tables = table_ref.shape[0]

    def valid(flag, v):
        return jnp.where(flag, v, jnp.zeros_like(v))

    def choose(flag, x_ref, y_ref, lo, hi):
        return jnp.where(flag, x_ref[lo:hi], y_ref[lo:hi]).astype(F32)

    base = 26
    own = near_ref[0:coef_n].astype(F32)
    left = valid(has_l1, choose(odd_unit, a1_ref, b1_ref, 0, coef_n))
    right = valid(has_r1, choose(odd_unit, b1_ref, a1_ref, 0, coef_n))
    left2 = valid(has_l2, choose(odd_quad, a2_ref, b2_ref, 0, far_n))
    right2 = valid(has_r2, choose(odd_quad, b2_ref, a2_ref, 0, far_n))
    c_ref[0 : far_n - 2] = left2[: far_n - 2].astype(BF16)
    c_ref[base - 17 : base - 15] = (left2[far_n - 2 :] + jnp.concatenate(
        [valid(has_l2, left[0:1]), left[1:2]], axis=0)).astype(BF16)
    c_ref[base - 15 : base - 1] = left[2 : coef_n - 2].astype(BF16)
    c_ref[base - 1 : base + 1] = (left[coef_n - 2 :] + jnp.concatenate(
        [valid(has_l1, own[0:1]), own[1:2]], axis=0)).astype(BF16)
    c_ref[base + 1 : base + 15] = own[2 : coef_n - 2].astype(BF16)
    c_ref[base + 15 : base + 17] = (right[:2] + jnp.concatenate(
        [own[coef_n - 2 : coef_n - 1], valid(has_r1, own[coef_n - 1 :])], axis=0)).astype(BF16)
    c_ref[base + 17 : base + 31] = right[2 : coef_n - 2].astype(BF16)
    c_ref[base + 31 : base + 33] = (right2[:2] + jnp.concatenate(
        [right[coef_n - 2 : coef_n - 1], valid(has_r2, right[coef_n - 1 :])], axis=0)).astype(BF16)
    c_ref[base + 33 : base + 31 + far_n] = right2[2:].astype(BF16)

    at = coef_n
    far_rows = 48
    for step in range(2):
        lo = at + 4 * step
        for ref_rows, flag, pos in ((0, odd_unit, -32), (1, jnp.logical_not(odd_unit), 32)):
            hi_v = choose(flag, a1_ref, b1_ref, lo, lo + 2)
            lo_v = choose(flag, a1_ref, b1_ref, lo + 2, lo + 4)
            slow_ref[step, far_rows + pos : far_rows + pos + 32] = (hi_v + lo_v).reshape(32, LANES)
        slow_ref[step, far_rows : far_rows + 32] = (
            near_ref[lo : lo + 2].astype(F32) + near_ref[lo + 2 : lo + 4].astype(F32)
        ).reshape(32, LANES)
    for flag, pos in ((odd_quad, -48), (jnp.logical_not(odd_quad), 64)):
        rows = choose(flag, a2_ref, b2_ref, far_n, far_n + 1) + choose(
            flag, a2_ref, b2_ref, far_n + 1, far_n + 2
        )
        slow_ref[0, far_rows + pos : far_rows + pos + 16] = rows[0]
    slow_ref[2, far_rows : far_rows + 32] = (
        last_ref[0:2].astype(F32) + last_ref[2:4].astype(F32)
    ).reshape(32, LANES)

    for step in range(STEPS):
        pos = coef_n + 8 + step
        pick_ref[step, 32:48] = near_ref[pos].astype(F32)
        pick_ref[step, 16:32] = jnp.where(
            has_l1, choose(odd_unit, a1_ref, b1_ref, pos, pos + 1)[0], -1.0)
        pick_ref[step, 48:64] = jnp.where(
            has_r1, choose(odd_unit, b1_ref, a1_ref, pos, pos + 1)[0], -1.0)
    pick_ref[0, 0:16] = jnp.where(
        has_l2, choose(odd_quad, a2_ref, b2_ref, far_n + 2, far_n + 3)[0], -1.0)
    pick_ref[0, 64:80] = jnp.where(
        has_r2, choose(odd_quad, b2_ref, a2_ref, far_n + 2, far_n + 3)[0], -1.0)

    scale = scale_ref[0]
    row8 = lax.broadcasted_iota(jnp.int32, (1, 8, LANES), 1)
    sign = jnp.where(row8 < 4, 1.0, -1.0).astype(F32)
    lane3 = low_lanes((1, 1, LANES))
    lane2 = low_lanes((1, LANES))

    def table_rows(parity):
        zero = jnp.zeros((COEFS, tables * LANES), BF16)
        full = jnp.concatenate([table_ref[t] for t in range(tables)], axis=1)
        return jnp.concatenate([full, zero] if parity == 0 else [zero, full], axis=0)

    plan = (
        dict(lo=-18, hi=34, base=26, first=-17),
        dict(lo=-9, hi=25, base=17, first=-9),
        dict(lo=-1, hi=17, base=9, first=0),
    )
    for step, item in enumerate(plan):
        lo, hi = item["lo"], item["hi"]
        count = hi - lo
        off = item["base"] + lo - 8
        rows = pick_ref[step, lo + 32 : hi + 32]
        swapped = lane_swap(rows)
        for parity, v_ref in ((0, ve_ref), (1, vo_ref)):
            lhs = jnp.concatenate(
                [c_ref[off + k : off + k + count].reshape(count * 16, LANES) for k in range(17)],
                axis=1,
            )
            out = jnp.dot(lhs, table_rows(parity), preferred_element_type=F32)
            pick = jnp.where(lane2, rows, swapped) if parity == 0 else jnp.where(lane2, swapped, rows)
            pick = pick.reshape(count, 1, LANES)
            v = jnp.zeros((count, 16, LANES), F32)
            for t in range(tables):
                v = jnp.where(
                    pick == float(t), out[:, LANES * t : LANES * (t + 1)].reshape(count, 16, LANES), v
                )
            v_ref[0:count] = v
        ve, vo = ve_ref[0:count], vo_ref[0:count]
        x = jnp.where(lane3, ve, lane_swap(vo))
        y = jnp.where(lane3, lane_swap(ve), vo)
        prop = jnp.concatenate(
            [x[:, :8] - sign * y[:, 8:], x[:, 8:] + sign * y[:, :8]], axis=1
        )
        p_ref[0] = jnp.zeros((16, LANES), BF16)
        p_ref[1 : count + 1] = prop.astype(BF16)
        first = item["first"]
        n = hi - first
        o = first - lo
        lhs = jnp.concatenate(
            [p_ref[o : o + n].reshape(n * 16, LANES), p_ref[o + 1 : o + 1 + n].reshape(n * 16, LANES)],
            axis=1,
        )
        back = jnp.dot(lhs, inverse_ref[...], preferred_element_type=F32)
        g0 = 2 * first + far_rows
        before = slow_ref[step, g0 - 1 : g0 - 1 + 2 * n]
        after = slow_ref[step, g0 : g0 + 2 * n]
        if step < 2:
            number = lax.broadcasted_iota(jnp.int32, (2 * n, 1), 0) + 2 * first
            def exists(block):
                inside = (block >= 0) & (block < 32)
                l1 = (block < 0) & (block >= -32) & has_l1
                r1 = (block >= 32) & (block < 64) & has_r1
                l2 = (block < -32) & has_l2
                r2 = (block >= 64) & has_r2
                return inside | l1 | r1 | l2 | r2
            ok = jnp.where(lane2, exists(number - 1).astype(jnp.int32), exists(number).astype(jnp.int32)) > 0
        theta = scale * jnp.where(lane2, lane_swap(before), lane_swap(after))
        sin_v, cos_v = sin_cos(theta)
        if step < 2:
            sin_v = jnp.where(ok, sin_v, 0.0)
            cos_v = jnp.where(ok, cos_v, 0.0)
        cos_ref[0 : 2 * n] = cos_v
        sin_ref[0 : 2 * n] = sin_v
        images = []
        for parity, x_ref in ((0, xe_ref), (1, xo_ref)):
            b = back[:, LANES * parity : LANES * (parity + 1)].reshape(n, 16, LANES)
            c = cos_ref[pl.ds(parity, n, stride=2)].reshape(n, 1, LANES)
            s = sin_ref[pl.ds(parity, n, stride=2)].reshape(n, 1, LANES) * sign
            f0 = c * b[:, :8] - s * b[:, 8:]
            f1 = c * b[:, 8:] + s * b[:, :8]
            if step < 2:
                x_ref[0:n] = jnp.concatenate([f0, f1], axis=1).astype(BF16)
            m = 17 - parity
            f0, f1 = f0[-first : -first + m], f1[-first : -first + m]
            images.append(lane_swap(f0 * pltpu.roll(f0, 4, 1) + f1 * pltpu.roll(f1, 4, 1)))
        even, odd = images
        image_ref[step, 0] = jnp.where(lane3, even[:16], odd)
        image_ref[step, 1] = jnp.where(lane3, odd, even[1:])
        if step < 2:
            if step == 1:
                xe_ref[n] = jnp.zeros((16, LANES), BF16)
                m = n
            else:
                m = n - 1
            lhs = jnp.concatenate(
                [
                    xe_ref[0:m].reshape(m * 16, LANES),
                    xo_ref[0:m].reshape(m * 16, LANES),
                    xe_ref[1 : m + 1].reshape(m * 16, LANES),
                ],
                axis=1,
            )
            coefs = jnp.dot(lhs, forward_ref[...], preferred_element_type=F32).reshape(m, 16, LANES)
            number = lax.broadcasted_iota(jnp.int32, (m, 1, 1), 0) + first
            ok = (
                ((number >= 0) & (number < 16))
                | ((number < 0) & (number >= -16) & has_l1)
                | ((number >= 16) & (number < 32) & has_r1)
                | ((number < -16) & has_l2)
                | ((number >= 32) & has_r2)
            )
            c_ref[0:m] = jnp.where(ok, coefs, 0.0).astype(BF16)
    row3 = row8 < 4
    for ref, half in ((keep_ref, second), (send_ref, 1 - second)):
        for parity in range(2):
            span = pl.ds(8 * half, 8)
            top = jnp.where(row3, image_ref[0, parity, span], image_ref[1, parity, span])
            ref[parity] = jnp.concatenate([top, image_ref[2, parity, span]], axis=1).astype(BF16)


def final_kernel(a_ref, b_ref, out_ref):
    total = a_ref[...].astype(F32) + b_ref[...].astype(F32)
    for parity in range(2):
        for q in range(8):
            cut = slice(WINDOW * (2 * q + parity), WINDOW * (2 * q + parity + 1))
            for n in range(STEPS):
                out_ref[n, :, cut] = total[parity, q, 4 * n : 4 * n + 4]


def matching(size, by, odd):
    pairs = []
    for i in range(size):
        right = (i // by) % 2 == odd
        j = i + by if right else i - by
        pairs.append((i, j if 0 <= j < size else i))
    return pairs


def on_device(wavefield, propagator_table, table_index, slowness, frequency_scale):
    sources = wavefield.shape[2]
    points = wavefield.shape[3]
    lat = lax.axis_size("lat")
    freqs = lax.axis_size("freq")
    pairs = points // (2 * WINDOW)
    first, forward, inverse = (jnp.asarray(m, BF16) for m in pair_matrices())
    vmem = pl.BlockSpec(memory_space=pltpu.VMEM)
    smem = pl.BlockSpec(memory_space=pltpu.SMEM)
    hbm = pl.BlockSpec(memory_space=pltpu.HBM)

    def tiles(n):
        return jax.ShapeDtypeStruct((n, 16, LANES), BF16)

    info = 8
    keep, send = pl.pallas_call(
        prep_kernel,
        out_shape=(tiles(pairs + 2), tiles(pairs + 2 + info)),
        in_specs=[hbm] * 4,
        out_specs=(vmem, vmem),
        scratch_shapes=[
            pltpu.VMEM(wavefield.shape, F32),
            pltpu.VMEM(slowness.shape, F32),
            pltpu.SMEM(table_index.shape, jnp.int32),
            pltpu.VMEM(first.shape, BF16),
            pltpu.VMEM((2, pairs + 2, 16, LANES), BF16),
            pltpu.VMEM((info * 16, LANES), F32),
            pltpu.SemaphoreType.DMA((4,)),
        ],
        compiler_params=pltpu.CompilerParams(vmem_limit_bytes=8 << 20),
        cost_estimate=pl.CostEstimate(flops=10**9, bytes_accessed=10**7, transcendentals=0),
        name="prep",
    )(
        *(
            pltpu.with_memory_space_constraint(x, pltpu.HBM)
            for x in (wavefield, slowness, table_index, first)
        )
    )
    partner = [(i, i ^ 1) for i in range(lat)]
    got = lax.ppermute(send, "lat", partner)
    near_n = 2 * (pairs + 2) - 2 + 8 + STEPS
    far_n = 11 + 3
    near, far_a, far_b, last = pl.pallas_call(
        unit_kernel,
        out_shape=(tiles(near_n), tiles(far_n), tiles(far_n), tiles(4)),
        in_specs=[vmem] * 3,
        out_specs=(vmem,) * 4,
        compiler_params=pltpu.CompilerParams(vmem_limit_bytes=4 << 20),
        name="unit",
    )(keep, send, got)
    a1 = lax.ppermute(near, "lat", matching(lat, 2, 0))
    b1 = lax.ppermute(near, "lat", matching(lat, 2, 1))
    a2 = lax.ppermute(far_a, "lat", matching(lat, 4, 0))
    b2 = lax.ppermute(far_b, "lat", matching(lat, 4, 1))
    image = jax.ShapeDtypeStruct((2, pairs, 16, LANES), BF16)
    own, other = pl.pallas_call(
        lambda *refs: main_kernel(lat // 2, *refs),
        out_shape=(image, image),
        in_specs=[vmem] * 9 + [smem],
        out_specs=(vmem, vmem),
        scratch_shapes=[
            pltpu.VMEM((68, 16, LANES), BF16),
            pltpu.VMEM((53, 16, LANES), BF16),
            pltpu.VMEM((52, 16, LANES), F32),
            pltpu.VMEM((52, 16, LANES), F32),
            pltpu.VMEM((52, 16, LANES), BF16),
            pltpu.VMEM((52, 16, LANES), BF16),
            pltpu.VMEM((STEPS, 128, LANES), F32),
            pltpu.VMEM((104, LANES), F32),
            pltpu.VMEM((104, LANES), F32),
            pltpu.VMEM((STEPS, 80, LANES), F32),
            pltpu.VMEM((STEPS, 2, 16, 8, LANES), F32),
        ],
        compiler_params=pltpu.CompilerParams(vmem_limit_bytes=32 << 20),
        name="steps",
    )(near, last, a1, b1, a2, b2, propagator_table[0], forward, inverse, frequency_scale)
    swapped = lax.ppermute(other, "lat", partner)
    core = lax.rem(lax.axis_index("lat"), 2)
    if freqs == 2:
        mine = core == lax.axis_index("freq")
        stay = jnp.where(mine, own, swapped)
        leave = jnp.where(mine, swapped, own)
        come = lax.ppermute(leave, "freq", [(0, 1), (1, 0)])
        return pl.pallas_call(
            final_kernel,
            out_shape=jax.ShapeDtypeStruct((STEPS, sources // 2, points), F32),
            in_specs=[vmem, vmem],
            out_specs=vmem,
            compiler_params=pltpu.CompilerParams(vmem_limit_bytes=4 << 20),
            name="total",
        )(stay, come)
    low = jnp.where(core == 0, own, swapped)
    high = jnp.where(core == 0, swapped, own)
    whole = jnp.stack([low, high])[:, :, :, : 4 * STEPS]
    whole = whole.reshape(2, 2, pairs, STEPS, 4, LANES)
    whole = jnp.transpose(whole, (3, 0, 4, 2, 1, 5)).reshape(STEPS, sources, points)
    return lax.psum_scatter(whole, "freq", scatter_dimension=1, tiled=True).astype(F32)


def solution(mesh):
    placed = (
        P(None, "freq", None, "lat"),
        P("freq", None, None, None),
        P(None, "lat"),
        P(None, "lat"),
        P("freq"),
    )
    return jax.shard_map(
        on_device, mesh=mesh, in_specs=placed, out_specs=P(None, "freq", "lat"), check_vma=False
    )
```

```python
import math

import jax
import jax.numpy as jnp
import numpy as np
from jax import lax
from jax.experimental import pallas as pl
from jax.experimental.pallas import tpu as pltpu
from jax.sharding import PartitionSpec as P

WINDOW = 128
COEFS = 64
REACH = 16
STEPS = 3
HALF = WINDOW // 2
F32 = jnp.float32
BF16 = jnp.bfloat16
LANES = 2 * COEFS


def basis_table():
    t = np.arange(2 * WINDOW, dtype=np.float32)[:, None]
    k = np.arange(COEFS, dtype=np.float32)[None, :]
    taper = np.sin(np.float32(math.pi) * (t + np.float32(0.5)) / np.float32(2 * WINDOW))
    wave = np.cos(
        np.float32(math.pi)
        * (k + np.float32(0.5))
        * (t - np.float32(HALF) + np.float32(0.5))
        / np.float32(WINDOW)
    )
    return (taper * np.float32(math.sqrt(2.0 / WINDOW)) * wave).astype(np.float32)


def pair_matrices():
    b = basis_table()
    first = np.zeros((4 * WINDOW, LANES), np.float32)
    first[HALF : HALF + 2 * WINDOW, :COEFS] = b
    first[HALF + WINDOW : HALF + 3 * WINDOW, COEFS:] = b
    forward = np.zeros((3 * WINDOW, LANES), np.float32)
    forward[: 2 * WINDOW, :COEFS] = b
    forward[WINDOW:, COEFS:] = b
    inverse = np.zeros((4 * COEFS, 2 * WINDOW), np.float32)
    inverse[COEFS : 2 * COEFS, :WINDOW] = b[WINDOW:].T
    inverse[2 * COEFS : 3 * COEFS, :WINDOW] = b[:WINDOW].T
    inverse[2 * COEFS : 3 * COEFS, WINDOW:] = b[WINDOW:].T
    inverse[3 * COEFS :, WINDOW:] = b[:WINDOW].T
    return first, forward, inverse


def sin_cos(theta):
    turns = jnp.floor(theta * np.float32(2.0 / math.pi) + np.float32(0.5))
    r = theta - turns * np.float32(1.5703125)
    r = r - turns * np.float32(4.837512969970703e-4)
    r = r - turns * np.float32(7.549789948768648e-8)
    r2 = r * r
    s = r + r * r2 * (
        np.float32(-1.6666654611e-1)
        + r2 * (np.float32(8.3321608736e-3) + r2 * np.float32(-1.9515295891e-4))
    )
    c = 1.0 - 0.5 * r2 + r2 * r2 * (
        np.float32(4.166664568298827e-2)
        + r2 * (np.float32(-1.388731625493765e-3) + r2 * np.float32(2.443315711809948e-5))
    )
    quarter = turns - 4.0 * jnp.floor(turns * 0.25)
    odd = (quarter == 1.0) | (quarter == 3.0)
    sin_v = jnp.where(odd, c, s)
    cos_v = jnp.where(odd, s, c)
    sin_v = jnp.where(quarter >= 2.0, -sin_v, sin_v)
    cos_v = jnp.where((quarter == 1.0) | (quarter == 2.0), -cos_v, cos_v)
    return sin_v, cos_v


def lane_swap(v):
    return pltpu.roll(v, LANES // 2, v.ndim - 1)


def low_lanes(shape):
    return lax.broadcasted_iota(jnp.int32, shape, len(shape) - 1) < LANES // 2


def prep_kernel(
    wave_hbm,
    slow_hbm,
    index_hbm,
    first_hbm,
    keep_ref,
    send_ref,
    wave_ref,
    slow_ref,
    index_ref,
    first_ref,
    both_ref,
    rows_ref,
    sems,
):
    copies = [
        pltpu.make_async_copy(source, target, sems.at[i])
        for i, (source, target) in enumerate(
            (
                (wave_hbm, wave_ref),
                (first_hbm, first_ref),
                (slow_hbm, slow_ref),
                (index_hbm, index_ref),
            )
        )
    ]
    for copy in copies:
        copy.start()
    core = lax.rem(lax.axis_index("lat"), 2)
    copies[2].wait()
    copies[3].wait()
    blocks = wave_ref.shape[-1] // WINDOW
    pairs = blocks // 2
    slow = slow_ref[...]
    high = slow.astype(BF16).astype(F32)
    rest = slow - high
    lanes = low_lanes((1, LANES))
    rows_ref[...] = jnp.zeros(rows_ref.shape, F32)
    for n in range(STEPS):
        for g in range(blocks):
            cut = slice(WINDOW * g, WINDOW * (g + 1))
            rows_ref[(2 * n) * blocks + g : (2 * n) * blocks + g + 1, :] = high[n : n + 1, cut]
            rows_ref[(2 * n + 1) * blocks + g : (2 * n + 1) * blocks + g + 1, :] = rest[n : n + 1, cut]
        for q in range(pairs):
            at = 2 * STEPS * blocks + n * pairs + q
            rows_ref[at : at + 1, :] = jnp.where(
                lanes,
                jnp.full((1, LANES), index_ref[n, 2 * q], jnp.int32),
                jnp.full((1, LANES), index_ref[n, 2 * q + 1], jnp.int32),
            ).astype(F32)
    send_ref[pairs + 2 :] = rows_ref[...].reshape(-1, 16, LANES).astype(BF16)
    copies[0].wait()
    copies[1].wait()
    upper = lax.broadcasted_iota(jnp.int32, (8, wave_ref.shape[-1]), 0) < 4
    for side in range(2):
        halves = []
        for low in range(2):
            near, far = wave_ref[low, 0], wave_ref[low + 2, 0]
            if side == 0:
                halves.append(jnp.where(upper, near, pltpu.roll(far, 4, 0)))
            else:
                halves.append(jnp.where(upper, pltpu.roll(near, 4, 0), far))
        samples = jnp.concatenate(halves, axis=0).astype(BF16)
        zero = jnp.zeros((16, WINDOW), BF16)
        padded = [zero] * 3
        padded += [samples[:, WINDOW * g : WINDOW * (g + 1)] for g in range(blocks)]
        padded += [zero] * 3
        parts = [
            jnp.concatenate([padded[2 * i + j] for i in range(pairs + 2)], axis=0)
            for j in range(4)
        ]
        coefs = jnp.dot(
            jnp.concatenate(parts, axis=1), first_ref[...], preferred_element_type=F32
        )
        both_ref[side] = coefs.reshape(pairs + 2, 16, LANES).astype(BF16)
    keep_ref[...] = both_ref[core]
    send_ref[0 : pairs + 2] = both_ref[1 - core]


def unit_kernel(keep_ref, sent_ref, got_ref, scale_ref, near_ref, far_a_ref, far_b_ref, last_ref):
    place = lax.axis_index("lat")
    second = lax.rem(place, 2) == 1
    n = keep_ref.shape[0]
    own_c, own_i = keep_ref[...].astype(F32), sent_ref[n:].astype(F32)
    got_c, got_i = got_ref[:n].astype(F32), got_ref[n:].astype(F32)
    b0 = jnp.where(second, got_c, own_c)
    b1 = jnp.where(second, own_c, got_c)
    i0 = jnp.where(second, got_i, own_i)
    i1 = jnp.where(second, own_i, got_i)
    unit = jnp.concatenate([b0[: n - 2], b0[n - 2 :] + b1[:2], b1[2:]], axis=0)
    near_ref[0 : 2 * n - 2] = unit.astype(BF16)
    at = 2 * n - 2
    for step in range(STEPS):
        ref, to = (near_ref, at) if step < 2 else (last_ref, 0)
        for block, info in enumerate((i0, i1)):
            theta = scale_ref[0] * (info[2 * step] + info[2 * step + 1])
            high = theta.astype(BF16)
            ref[to + block] = high
            ref[to + 2 + block] = (theta - high.astype(F32)).astype(BF16)
        if step < 2:
            at += 4
    near_ref[at] = jnp.concatenate([i0[6, :8], i1[6, :8]], axis=0).astype(BF16)
    near_ref[at + 1] = jnp.concatenate([i0[6, 8:], i1[6, 8:]], axis=0).astype(BF16)
    near_ref[at + 2] = jnp.concatenate([i0[7, :8], i1[7, :8]], axis=0).astype(BF16)
    even_quad = lax.rem(lax.div(place, 4), 2) == 0
    count = far_a_ref.shape[0] - 3
    base = 2 * n - 2
    for ref, right in ((far_a_ref, even_quad), (far_b_ref, jnp.logical_not(even_quad))):
        start = jnp.where(right, base - count, 0)
        pick = jnp.where(right, 1, 0)
        ref[0:count] = near_ref[pl.ds(start, count)]
        ref[count] = near_ref[base + pick]
        ref[count + 1] = near_ref[base + 2 + pick]
        ref[count + 2] = near_ref[base + 8]


def sign_rows():
    row = lax.broadcasted_iota(jnp.int32, (1, 8, LANES), 1)
    return jnp.where(row < 4, 1.0, -1.0).astype(F32)


def valid(flag, v):
    return jnp.where(flag, v, jnp.zeros_like(v))


def choose(flag, x_ref, y_ref, lo, hi):
    return jnp.where(flag, x_ref[lo:hi], y_ref[lo:hi]).astype(F32)


def middle_coefs(c_ref, at, near_ref, left, right, has_l1, has_r1, coef_n):
    own = near_ref[0:coef_n].astype(F32)
    c_ref[at - 15 : at - 1] = left[2 : coef_n - 2].astype(BF16)
    c_ref[at - 1 : at + 1] = (
        left[coef_n - 2 :] + jnp.concatenate([valid(has_l1, own[0:1]), own[1:2]], axis=0)
    ).astype(BF16)
    c_ref[at + 1 : at + 15] = own[2 : coef_n - 2].astype(BF16)
    c_ref[at + 15 : at + 17] = (
        right[:2]
        + jnp.concatenate([own[coef_n - 2 : coef_n - 1], valid(has_r1, own[coef_n - 1 :])], axis=0)
    ).astype(BF16)
    c_ref[at + 17 : at + 31] = right[2 : coef_n - 2].astype(BF16)


def band_product(c_ref, parts, rows, table_ref, ve_ref, vo_ref):
    tables = table_ref.shape[0]
    count = sum(n for _, n in parts)
    lane2, lane3 = low_lanes((1, LANES)), low_lanes((1, 1, LANES))
    sign = sign_rows()
    swapped = lane_swap(rows)
    zero = jnp.zeros((COEFS, tables * LANES), BF16)
    for parity, v_ref in ((0, ve_ref), (1, vo_ref)):
        lhs = jnp.concatenate(
            [
                jnp.concatenate([c_ref[o + k : o + k + n] for o, n in parts], axis=0).reshape(
                    count * 16, LANES
                )
                for k in range(REACH + 1)
            ],
            axis=1,
        )
        full = jnp.concatenate([table_ref[t] for t in range(tables)], axis=1)
        rhs = jnp.concatenate([full, zero] if parity == 0 else [zero, full], axis=0)
        out = jnp.dot(lhs, rhs, preferred_element_type=F32)
        pick = jnp.where(lane2, rows, swapped) if parity == 0 else jnp.where(lane2, swapped, rows)
        pick = pick.reshape(count, 1, LANES)
        v = jnp.zeros((count, 16, LANES), F32)
        for t in range(tables):
            part = out[:, LANES * t : LANES * (t + 1)].reshape(count, 16, LANES)
            v = jnp.where(pick == float(t), part, v)
        v_ref[0:count] = v
    ve, vo = ve_ref[0:count], vo_ref[0:count]
    x = jnp.where(lane3, ve, lane_swap(vo))
    y = jnp.where(lane3, lane_swap(ve), vo)
    return jnp.concatenate(
        [x[:, :8] - sign * y[:, 8:], x[:, 8:] + sign * y[:, :8]], axis=1
    ).astype(BF16)


INNER = (-7, 23)


def inner_kernel(units, near_ref, a1_ref, b1_ref, table_ref, out_ref, c_ref, ve_ref, vo_ref, pick_ref):
    unit = lax.div(lax.axis_index("lat"), 2)
    odd_unit = lax.rem(unit, 2) == 1
    has_l1, has_r1 = unit >= 1, unit + 1 < units
    coef_n = 18
    left = valid(has_l1, choose(odd_unit, a1_ref, b1_ref, 0, coef_n))
    right = valid(has_r1, choose(odd_unit, b1_ref, a1_ref, 0, coef_n))
    middle_coefs(c_ref, 15, near_ref, left, right, has_l1, has_r1, coef_n)
    pos = coef_n + 8
    pick_ref[0:16] = jnp.where(has_l1, choose(odd_unit, a1_ref, b1_ref, pos, pos + 1)[0], -1.0)
    pick_ref[16:32] = near_ref[pos].astype(F32)
    pick_ref[32:48] = jnp.where(has_r1, choose(odd_unit, b1_ref, a1_ref, pos, pos + 1)[0], -1.0)
    lo, hi = INNER
    out_ref[...] = band_product(
        c_ref, ((lo - 8 + 15, hi - lo),), pick_ref[lo + 16 : hi + 16], table_ref, ve_ref, vo_ref
    )


def main_kernel(
    units,
    near_ref,
    last_ref,
    a1_ref,
    b1_ref,
    a2_ref,
    b2_ref,
    table_ref,
    forward_ref,
    inverse_ref,
    inner_ref,
    keep_ref,
    send_ref,
    c_ref,
    p_ref,
    ve_ref,
    vo_ref,
    xe_ref,
    xo_ref,
    slow_ref,
    cos_ref,
    sin_ref,
    pick_ref,
    image_ref,
):
    place = lax.axis_index("lat")
    unit = lax.div(place, 2)
    second = lax.rem(place, 2)
    odd_unit = lax.rem(unit, 2) == 1
    odd_quad = lax.rem(lax.div(place, 4), 2) == 1
    has_l1, has_l2 = unit >= 1, unit >= 2
    has_r1, has_r2 = unit + 1 < units, unit + 2 < units
    pairs = 16
    coef_n = pairs + 2
    far_n = a2_ref.shape[0] - 3

    base = 26
    left = valid(has_l1, choose(odd_unit, a1_ref, b1_ref, 0, coef_n))
    right = valid(has_r1, choose(odd_unit, b1_ref, a1_ref, 0, coef_n))
    left2 = valid(has_l2, choose(odd_quad, a2_ref, b2_ref, 0, far_n))
    right2 = valid(has_r2, choose(odd_quad, b2_ref, a2_ref, 0, far_n))
    c_ref[0 : far_n - 2] = left2[: far_n - 2].astype(BF16)
    c_ref[base - 17 : base - 15] = (left2[far_n - 2 :] + jnp.concatenate(
        [valid(has_l2, left[0:1]), left[1:2]], axis=0)).astype(BF16)
    middle_coefs(c_ref, base, near_ref, left, right, has_l1, has_r1, coef_n)
    c_ref[base + 31 : base + 33] = (right2[:2] + jnp.concatenate(
        [right[coef_n - 2 : coef_n - 1], valid(has_r2, right[coef_n - 1 :])], axis=0)).astype(BF16)
    c_ref[base + 33 : base + 31 + far_n] = right2[2:].astype(BF16)

    at = coef_n
    far_rows = 48
    for step in range(2):
        lo = at + 4 * step
        for ref_rows, flag, pos in ((0, odd_unit, -32), (1, jnp.logical_not(odd_unit), 32)):
            hi_v = choose(flag, a1_ref, b1_ref, lo, lo + 2)
            lo_v = choose(flag, a1_ref, b1_ref, lo + 2, lo + 4)
            slow_ref[step, far_rows + pos : far_rows + pos + 32] = (hi_v + lo_v).reshape(32, LANES)
        slow_ref[step, far_rows : far_rows + 32] = (
            near_ref[lo : lo + 2].astype(F32) + near_ref[lo + 2 : lo + 4].astype(F32)
        ).reshape(32, LANES)
    for flag, pos in ((odd_quad, -48), (jnp.logical_not(odd_quad), 64)):
        rows = choose(flag, a2_ref, b2_ref, far_n, far_n + 1) + choose(
            flag, a2_ref, b2_ref, far_n + 1, far_n + 2
        )
        slow_ref[0, far_rows + pos : far_rows + pos + 16] = rows[0]
    slow_ref[2, far_rows : far_rows + 32] = (
        last_ref[0:2].astype(F32) + last_ref[2:4].astype(F32)
    ).reshape(32, LANES)

    for step in range(STEPS):
        pos = coef_n + 8 + step
        pick_ref[step, 32:48] = near_ref[pos].astype(F32)
        pick_ref[step, 16:32] = jnp.where(
            has_l1, choose(odd_unit, a1_ref, b1_ref, pos, pos + 1)[0], -1.0)
        pick_ref[step, 48:64] = jnp.where(
            has_r1, choose(odd_unit, b1_ref, a1_ref, pos, pos + 1)[0], -1.0)
    pick_ref[0, 0:16] = jnp.where(
        has_l2, choose(odd_quad, a2_ref, b2_ref, far_n + 2, far_n + 3)[0], -1.0)
    pick_ref[0, 64:80] = jnp.where(
        has_r2, choose(odd_quad, b2_ref, a2_ref, far_n + 2, far_n + 3)[0], -1.0)

    sign = sign_rows()
    row3 = lax.broadcasted_iota(jnp.int32, (1, 8, LANES), 1) < 4
    lane3 = low_lanes((1, 1, LANES))
    lane2 = low_lanes((1, LANES))

    plan = (
        dict(lo=-18, hi=34, base=26, first=-17),
        dict(lo=-9, hi=25, base=17, first=-9),
        dict(lo=-1, hi=17, base=9, first=0),
    )
    for step, item in enumerate(plan):
        lo, hi = item["lo"], item["hi"]
        count = hi - lo
        p_ref[0] = jnp.zeros((16, LANES), BF16)
        if step == 0:
            parts = ((lo, INNER[0] - lo), (INNER[1], hi - INNER[1]))
            p_ref[1 + INNER[0] - lo : 1 + INNER[1] - lo] = inner_ref[...]
        else:
            parts = ((lo, count),)
        rows = jnp.concatenate(
            [pick_ref[step, a + 32 : a + 32 + m] for a, m in parts], axis=0
        )
        out = band_product(
            c_ref, [(item["base"] + a - 8, m) for a, m in parts], rows, table_ref, ve_ref, vo_ref
        )
        done = 0
        for a, m in parts:
            p_ref[1 + a - lo : 1 + a - lo + m] = out[done : done + m]
            done += m
        first = item["first"]
        n = hi - first
        o = first - lo
        lhs = jnp.concatenate(
            [p_ref[o : o + n].reshape(n * 16, LANES), p_ref[o + 1 : o + 1 + n].reshape(n * 16, LANES)],
            axis=1,
        )
        back = jnp.dot(lhs, inverse_ref[...], preferred_element_type=F32)
        g0 = 2 * first + far_rows
        before = slow_ref[step, g0 - 1 : g0 - 1 + 2 * n]
        after = slow_ref[step, g0 : g0 + 2 * n]
        if step < 2:
            number = lax.broadcasted_iota(jnp.int32, (2 * n, 1), 0) + 2 * first
            def exists(block):
                inside = (block >= 0) & (block < 32)
                l1 = (block < 0) & (block >= -32) & has_l1
                r1 = (block >= 32) & (block < 64) & has_r1
                l2 = (block < -32) & has_l2
                r2 = (block >= 64) & has_r2
                return inside | l1 | r1 | l2 | r2
            ok = jnp.where(lane2, exists(number - 1).astype(jnp.int32), exists(number).astype(jnp.int32)) > 0
        theta = jnp.where(lane2, lane_swap(before), lane_swap(after))
        sin_v, cos_v = sin_cos(theta)
        if step < 2:
            sin_v = jnp.where(ok, sin_v, 0.0)
            cos_v = jnp.where(ok, cos_v, 0.0)
        cos_ref[0 : 2 * n] = cos_v
        sin_ref[0 : 2 * n] = sin_v
        images = []
        for parity, x_ref in ((0, xe_ref), (1, xo_ref)):
            b = back[:, LANES * parity : LANES * (parity + 1)].reshape(n, 16, LANES)
            c = cos_ref[pl.ds(parity, n, stride=2)].reshape(n, 1, LANES)
            s = sin_ref[pl.ds(parity, n, stride=2)].reshape(n, 1, LANES) * sign
            f0 = c * b[:, :8] - s * b[:, 8:]
            f1 = c * b[:, 8:] + s * b[:, :8]
            if step < 2:
                x_ref[0:n] = jnp.concatenate([f0, f1], axis=1).astype(BF16)
            m = 17 - parity
            f0, f1 = f0[-first : -first + m], f1[-first : -first + m]
            images.append(lane_swap(f0 * pltpu.roll(f0, 4, 1) + f1 * pltpu.roll(f1, 4, 1)))
        even, odd = images
        image_ref[step, 0] = jnp.where(lane3, even[:16], odd)
        image_ref[step, 1] = jnp.where(lane3, odd, even[1:])
        if step < 2:
            if step == 1:
                xe_ref[n] = jnp.zeros((16, LANES), BF16)
                m = n
            else:
                m = n - 1
            lhs = jnp.concatenate(
                [
                    xe_ref[0:m].reshape(m * 16, LANES),
                    xo_ref[0:m].reshape(m * 16, LANES),
                    xe_ref[1 : m + 1].reshape(m * 16, LANES),
                ],
                axis=1,
            )
            coefs = jnp.dot(lhs, forward_ref[...], preferred_element_type=F32).reshape(m, 16, LANES)
            number = lax.broadcasted_iota(jnp.int32, (m, 1, 1), 0) + first
            ok = (
                ((number >= 0) & (number < 16))
                | ((number < 0) & (number >= -16) & has_l1)
                | ((number >= 16) & (number < 32) & has_r1)
                | ((number < -16) & has_l2)
                | ((number >= 32) & has_r2)
            )
            c_ref[0:m] = jnp.where(ok, coefs, 0.0).astype(BF16)
    for ref, half in ((keep_ref, second), (send_ref, 1 - second)):
        for parity in range(2):
            span = pl.ds(8 * half, 8)
            top = jnp.where(row3, image_ref[0, parity, span], image_ref[1, parity, span])
            ref[parity] = jnp.concatenate([top, image_ref[2, parity, span]], axis=1).astype(BF16)


def final_kernel(a_ref, b_ref, out_ref):
    total = a_ref[...].astype(F32) + b_ref[...].astype(F32)
    for parity in range(2):
        for q in range(8):
            cut = slice(WINDOW * (2 * q + parity), WINDOW * (2 * q + parity + 1))
            for n in range(STEPS):
                out_ref[n, :, cut] = total[parity, q, 4 * n : 4 * n + 4]


def matching(size, by, odd):
    pairs = []
    for i in range(size):
        right = (i // by) % 2 == odd
        j = i + by if right else i - by
        pairs.append((i, j if 0 <= j < size else i))
    return pairs


def on_device(wavefield, propagator_table, table_index, slowness, frequency_scale):
    sources = wavefield.shape[2]
    points = wavefield.shape[3]
    lat = lax.axis_size("lat")
    freqs = lax.axis_size("freq")
    pairs = points // (2 * WINDOW)
    first, forward, inverse = (jnp.asarray(m, BF16) for m in pair_matrices())
    vmem = pl.BlockSpec(memory_space=pltpu.VMEM)
    hbm = pl.BlockSpec(memory_space=pltpu.HBM)
    smem = pl.BlockSpec(memory_space=pltpu.SMEM)

    def tiles(n):
        return jax.ShapeDtypeStruct((n, 16, LANES), BF16)

    info = 8
    keep, send = pl.pallas_call(
        prep_kernel,
        out_shape=(tiles(pairs + 2), tiles(pairs + 2 + info)),
        in_specs=[hbm] * 4,
        out_specs=(vmem, vmem),
        scratch_shapes=[
            pltpu.VMEM(wavefield.shape, F32),
            pltpu.VMEM(slowness.shape, F32),
            pltpu.SMEM(table_index.shape, jnp.int32),
            pltpu.VMEM(first.shape, BF16),
            pltpu.VMEM((2, pairs + 2, 16, LANES), BF16),
            pltpu.VMEM((info * 16, LANES), F32),
            pltpu.SemaphoreType.DMA((4,)),
        ],
        compiler_params=pltpu.CompilerParams(vmem_limit_bytes=8 << 20),
        cost_estimate=pl.CostEstimate(flops=10**9, bytes_accessed=10**7, transcendentals=0),
        name="prep",
    )(
        *(
            pltpu.with_memory_space_constraint(x, pltpu.HBM)
            for x in (wavefield, slowness, table_index, first)
        )
    )
    partner = [(i, i ^ 1) for i in range(lat)]
    got = lax.ppermute(send, "lat", partner)
    near_n = 2 * (pairs + 2) - 2 + 8 + STEPS
    far_n = 11 + 3
    near, far_a, far_b, last = pl.pallas_call(
        unit_kernel,
        out_shape=(tiles(near_n), tiles(far_n), tiles(far_n), tiles(4)),
        in_specs=[vmem] * 3 + [smem],
        out_specs=(vmem,) * 4,
        compiler_params=pltpu.CompilerParams(vmem_limit_bytes=4 << 20),
        name="unit",
    )(keep, send, got, frequency_scale)
    a1 = lax.ppermute(near, "lat", matching(lat, 2, 0))
    b1 = lax.ppermute(near, "lat", matching(lat, 2, 1))
    a2 = lax.ppermute(far_a, "lat", matching(lat, 4, 0))
    b2 = lax.ppermute(far_b, "lat", matching(lat, 4, 1))
    inner_n = INNER[1] - INNER[0]
    table = propagator_table[0]
    inner = pl.pallas_call(
        lambda *refs: inner_kernel(lat // 2, *refs),
        out_shape=tiles(inner_n),
        in_specs=[vmem] * 4,
        out_specs=vmem,
        scratch_shapes=[
            pltpu.VMEM((46, 16, LANES), BF16),
            pltpu.VMEM((inner_n, 16, LANES), F32),
            pltpu.VMEM((inner_n, 16, LANES), F32),
            pltpu.VMEM((48, LANES), F32),
        ],
        compiler_params=pltpu.CompilerParams(vmem_limit_bytes=24 << 20),
        cost_estimate=pl.CostEstimate(flops=2 * 10**9, bytes_accessed=10**7, transcendentals=0),
        name="inner",
    )(near, a1, b1, table)
    image = jax.ShapeDtypeStruct((2, pairs, 16, LANES), BF16)
    own, other = pl.pallas_call(
        lambda *refs: main_kernel(lat // 2, *refs),
        out_shape=(image, image),
        in_specs=[vmem] * 10,
        out_specs=(vmem, vmem),
        scratch_shapes=[
            pltpu.VMEM((68, 16, LANES), BF16),
            pltpu.VMEM((53, 16, LANES), BF16),
            pltpu.VMEM((34, 16, LANES), F32),
            pltpu.VMEM((34, 16, LANES), F32),
            pltpu.VMEM((52, 16, LANES), BF16),
            pltpu.VMEM((52, 16, LANES), BF16),
            pltpu.VMEM((STEPS, 128, LANES), F32),
            pltpu.VMEM((104, LANES), F32),
            pltpu.VMEM((104, LANES), F32),
            pltpu.VMEM((STEPS, 80, LANES), F32),
            pltpu.VMEM((STEPS, 2, 16, 8, LANES), F32),
        ],
        compiler_params=pltpu.CompilerParams(vmem_limit_bytes=32 << 20),
        name="steps",
    )(near, last, a1, b1, a2, b2, table, forward, inverse, inner)
    swapped = lax.ppermute(other, "lat", partner)
    core = lax.rem(lax.axis_index("lat"), 2)
    if freqs == 2:
        mine = core == lax.axis_index("freq")
        stay = jnp.where(mine, own, swapped)
        leave = jnp.where(mine, swapped, own)
        come = lax.ppermute(leave, "freq", [(0, 1), (1, 0)])
        return pl.pallas_call(
            final_kernel,
            out_shape=jax.ShapeDtypeStruct((STEPS, sources // 2, points), F32),
            in_specs=[vmem, vmem],
            out_specs=vmem,
            compiler_params=pltpu.CompilerParams(vmem_limit_bytes=4 << 20),
            name="total",
        )(stay, come)
    low = jnp.where(core == 0, own, swapped)
    high = jnp.where(core == 0, swapped, own)
    whole = jnp.stack([low, high])[:, :, :, : 4 * STEPS]
    whole = whole.reshape(2, 2, pairs, STEPS, 4, LANES)
    whole = jnp.transpose(whole, (3, 0, 4, 2, 1, 5)).reshape(STEPS, sources, points)
    return lax.psum_scatter(whole, "freq", scatter_dimension=1, tiled=True).astype(F32)


def solution(mesh):
    placed = (
        P(None, "freq", None, "lat"),
        P("freq", None, None, None),
        P(None, "lat"),
        P(None, "lat"),
        P("freq"),
    )
    return jax.shard_map(
        on_device, mesh=mesh, in_specs=placed, out_specs=P(None, "freq", "lat"), check_vma=False
    )
```

```python
import math

import jax
import jax.numpy as jnp
import numpy as np
from jax import lax
from jax.experimental import pallas as pl
from jax.experimental.pallas import tpu as pltpu
from jax.sharding import PartitionSpec as P


WINDOW = 128
COEFS = 64
REACH = 16
STEPS = 3
HALF = WINDOW // 2
F32 = jnp.float32
BF16 = jnp.bfloat16
LANES = 2 * COEFS


def basis_table():
    t = np.arange(2 * WINDOW, dtype=np.float32)[:, None]
    k = np.arange(COEFS, dtype=np.float32)[None, :]
    taper = np.sin(np.float32(math.pi) * (t + np.float32(0.5)) / np.float32(2 * WINDOW))
    wave = np.cos(
        np.float32(math.pi)
        * (k + np.float32(0.5))
        * (t - np.float32(HALF) + np.float32(0.5))
        / np.float32(WINDOW)
    )
    return (taper * np.float32(math.sqrt(2.0 / WINDOW)) * wave).astype(np.float32)


def pair_matrices():
    b = basis_table()
    first = np.zeros((4 * WINDOW, LANES), np.float32)
    first[HALF : HALF + 2 * WINDOW, :COEFS] = b
    first[HALF + WINDOW : HALF + 3 * WINDOW, COEFS:] = b
    forward = np.zeros((3 * WINDOW, LANES), np.float32)
    forward[: 2 * WINDOW, :COEFS] = b
    forward[WINDOW:, COEFS:] = b
    inverse = np.zeros((4 * COEFS, 2 * WINDOW), np.float32)
    inverse[COEFS : 2 * COEFS, :WINDOW] = b[WINDOW:].T
    inverse[2 * COEFS : 3 * COEFS, :WINDOW] = b[:WINDOW].T
    inverse[2 * COEFS : 3 * COEFS, WINDOW:] = b[WINDOW:].T
    inverse[3 * COEFS :, WINDOW:] = b[:WINDOW].T
    return first, forward, inverse


def sin_cos(theta):
    turns = jnp.floor(theta * np.float32(2.0 / math.pi) + np.float32(0.5))
    r = theta - turns * np.float32(1.5703125)
    r = r - turns * np.float32(4.837512969970703e-4)
    r = r - turns * np.float32(7.549789948768648e-8)
    r2 = r * r
    s = r + r * r2 * (
        np.float32(-1.6666654611e-1)
        + r2 * (np.float32(8.3321608736e-3) + r2 * np.float32(-1.9515295891e-4))
    )
    c = 1.0 - 0.5 * r2 + r2 * r2 * (
        np.float32(4.166664568298827e-2)
        + r2 * (np.float32(-1.388731625493765e-3) + r2 * np.float32(2.443315711809948e-5))
    )
    quarter = turns - 4.0 * jnp.floor(turns * 0.25)
    odd = (quarter == 1.0) | (quarter == 3.0)
    sin_v = jnp.where(odd, c, s)
    cos_v = jnp.where(odd, s, c)
    sin_v = jnp.where(quarter >= 2.0, -sin_v, sin_v)
    cos_v = jnp.where((quarter == 1.0) | (quarter == 2.0), -cos_v, cos_v)
    return sin_v, cos_v


def lane_swap(v):
    return pltpu.roll(v, LANES // 2, v.ndim - 1)


def low_lanes(shape):
    return lax.broadcasted_iota(jnp.int32, shape, len(shape) - 1) < LANES // 2


def prep_kernel(
    wave_hbm,
    slow_hbm,
    index_hbm,
    first_hbm,
    keep_ref,
    send_ref,
    wave_ref,
    slow_ref,
    index_ref,
    first_ref,
    both_ref,
    rows_ref,
    sems,
):
    copies = [
        pltpu.make_async_copy(source, target, sems.at[i])
        for i, (source, target) in enumerate(
            (
                (wave_hbm, wave_ref),
                (first_hbm, first_ref),
                (slow_hbm, slow_ref),
                (index_hbm, index_ref),
            )
        )
    ]
    for copy in copies:
        copy.start()
    core = lax.rem(lax.axis_index("lat"), 2)
    copies[2].wait()
    copies[3].wait()
    blocks = wave_ref.shape[-1] // WINDOW
    pairs = blocks // 2
    slow = slow_ref[...]
    high = slow.astype(BF16).astype(F32)
    rest = slow - high
    lanes = low_lanes((1, LANES))
    rows_ref[...] = jnp.zeros(rows_ref.shape, F32)
    for n in range(STEPS):
        for g in range(blocks):
            cut = slice(WINDOW * g, WINDOW * (g + 1))
            rows_ref[(2 * n) * blocks + g : (2 * n) * blocks + g + 1, :] = high[n : n + 1, cut]
            rows_ref[(2 * n + 1) * blocks + g : (2 * n + 1) * blocks + g + 1, :] = rest[n : n + 1, cut]
        for q in range(pairs):
            at = 2 * STEPS * blocks + n * pairs + q
            rows_ref[at : at + 1, :] = jnp.where(
                lanes,
                jnp.full((1, LANES), index_ref[n, 2 * q], jnp.int32),
                jnp.full((1, LANES), index_ref[n, 2 * q + 1], jnp.int32),
            ).astype(F32)
    send_ref[pairs + 2 :] = rows_ref[...].reshape(-1, 16, LANES).astype(BF16)
    copies[0].wait()
    copies[1].wait()
    upper = lax.broadcasted_iota(jnp.int32, (8, wave_ref.shape[-1]), 0) < 4
    for side in range(2):
        halves = []
        for low in range(2):
            near, far = wave_ref[low, 0], wave_ref[low + 2, 0]
            if side == 0:
                halves.append(jnp.where(upper, near, pltpu.roll(far, 4, 0)))
            else:
                halves.append(jnp.where(upper, pltpu.roll(near, 4, 0), far))
        samples = jnp.concatenate(halves, axis=0).astype(BF16)
        zero = jnp.zeros((16, WINDOW), BF16)
        padded = [zero] * 3
        padded += [samples[:, WINDOW * g : WINDOW * (g + 1)] for g in range(blocks)]
        padded += [zero] * 3
        parts = [
            jnp.concatenate([padded[2 * i + j] for i in range(pairs + 2)], axis=0)
            for j in range(4)
        ]
        coefs = jnp.dot(
            jnp.concatenate(parts, axis=1), first_ref[...], preferred_element_type=F32
        )
        both_ref[side] = coefs.reshape(pairs + 2, 16, LANES).astype(BF16)
    keep_ref[...] = both_ref[core]
    send_ref[0 : pairs + 2] = both_ref[1 - core]


def unit_kernel(keep_ref, sent_ref, got_ref, scale_ref, near_ref, far_a_ref, far_b_ref, last_ref):
    place = lax.axis_index("lat")
    second = lax.rem(place, 2) == 1
    n = keep_ref.shape[0]
    own_c, own_i = keep_ref[...].astype(F32), sent_ref[n:].astype(F32)
    got_c, got_i = got_ref[:n].astype(F32), got_ref[n:].astype(F32)
    b0 = jnp.where(second, got_c, own_c)
    b1 = jnp.where(second, own_c, got_c)
    i0 = jnp.where(second, got_i, own_i)
    i1 = jnp.where(second, own_i, got_i)
    unit = jnp.concatenate([b0[: n - 2], b0[n - 2 :] + b1[:2], b1[2:]], axis=0)
    near_ref[0 : 2 * n - 2] = unit.astype(BF16)
    at = 2 * n - 2
    for step in range(STEPS):
        ref, to = (near_ref, at) if step < 2 else (last_ref, 0)
        for block, info in enumerate((i0, i1)):
            theta = scale_ref[...] * (info[2 * step] + info[2 * step + 1])
            high = theta.astype(BF16)
            ref[to + block] = high
            ref[to + 2 + block] = (theta - high.astype(F32)).astype(BF16)
        if step < 2:
            at += 4
    near_ref[at] = jnp.concatenate([i0[6, :8], i1[6, :8]], axis=0).astype(BF16)
    near_ref[at + 1] = jnp.concatenate([i0[6, 8:], i1[6, 8:]], axis=0).astype(BF16)
    near_ref[at + 2] = jnp.concatenate([i0[7, :8], i1[7, :8]], axis=0).astype(BF16)
    even_quad = lax.rem(lax.div(place, 4), 2) == 0
    count = far_a_ref.shape[0] - 3
    base = 2 * n - 2
    for ref, right in ((far_a_ref, even_quad), (far_b_ref, jnp.logical_not(even_quad))):
        start = jnp.where(right, base - count, 0)
        pick = jnp.where(right, 1, 0)
        ref[0:count] = near_ref[pl.ds(start, count)]
        ref[count] = near_ref[base + pick]
        ref[count + 1] = near_ref[base + 2 + pick]
        ref[count + 2] = near_ref[base + 8]


def sign_rows():
    row = lax.broadcasted_iota(jnp.int32, (1, 8, LANES), 1)
    return jnp.where(row < 4, 1.0, -1.0).astype(F32)


def valid(flag, v):
    return jnp.where(flag, v, jnp.zeros_like(v))


def choose(flag, x_ref, y_ref, lo, hi):
    return jnp.where(flag, x_ref[lo:hi], y_ref[lo:hi]).astype(F32)


def middle_coefs(near_ref, left, right, has_l1, has_r1, coef_n):
    own = near_ref[0:coef_n].astype(F32)
    return [
        left[2 : coef_n - 2],
        left[coef_n - 2 :] + jnp.concatenate([valid(has_l1, own[0:1]), own[1:2]], axis=0),
        own[2 : coef_n - 2],
        right[:2]
        + jnp.concatenate([own[coef_n - 2 : coef_n - 1], valid(has_r1, own[coef_n - 1 :])], axis=0),
        right[2 : coef_n - 2],
    ]


def put_coefs(x_ref, coefs):
    n = coefs.shape[0]
    coefs = coefs.astype(BF16).astype(F32)
    real, imag = coefs[:, :8], coefs[:, 8:]
    source = lax.broadcasted_iota(jnp.int32, (1, 8, LANES), 1) < 4
    kinds = (real + imag, jnp.where(source, real, imag), jnp.where(source, imag, real))
    for kind, x in enumerate(kinds):
        x_ref[kind, 0, 0 : n // 2] = x.reshape(n // 2, 16, LANES).astype(BF16)
        x_ref[kind, 1, 0 : n // 2 - 1] = x[1 : n - 1].reshape(n // 2 - 1, 16, LANES).astype(BF16)


def weight_kernel(table_ref, w_ref):
    for duo in range(table_ref.shape[0] // 2):
        a, b = table_ref[2 * duo], table_ref[2 * duo + 1]
        low = low_lanes(a.shape)
        real = jnp.where(low, a, jnp.concatenate([b[:, COEFS:], b[:, :COEFS]], axis=1))
        imag = jnp.where(low, jnp.concatenate([a[:, COEFS:], a[:, :COEFS]], axis=1), b)
        w_ref[0, duo] = real
        w_ref[1, duo] = imag - real
        w_ref[2, duo] = imag + real


def band_product(x_ref, parts, rows, w_ref, k_ref):
    count = sum(n for _, n in parts)
    lane2, lane3 = low_lanes((1, LANES)), low_lanes((1, 1, LANES))
    half = jnp.floor(rows * 0.5)
    even = (rows - 2.0 * half) == 0.0
    direct = jnp.where(lane2, even.astype(F32), 1.0 - even.astype(F32)).reshape(count, 1, LANES)
    upper = half.reshape(count, 1, LANES)
    upper_swap = lane_swap(half).reshape(count, 1, LANES)
    exists = rows.reshape(count, 1, LANES) >= 0.0
    zero = jnp.zeros((COEFS, 2 * LANES), BF16)

    def band(kind, k):
        pieces = [
            x_ref[kind, (o + k) % 2, (o + k) // 2 : (o + k) // 2 + n // 2] for o, n in parts
        ]
        return jnp.concatenate(pieces, axis=0).reshape(count * 8, LANES)

    for kind in range(3):
        lhs = jnp.concatenate([band(kind, k) for k in range(REACH + 1)], axis=1)
        full = jnp.concatenate([w_ref[kind, 0], w_ref[kind, 1]], axis=1)
        rhs = jnp.concatenate(
            [jnp.concatenate([full, zero], axis=0), jnp.concatenate([zero, full], axis=0)], axis=1
        )
        out = jnp.dot(lhs, rhs, preferred_element_type=F32)
        e0, e1, o0, o1 = (
            out[:, LANES * t : LANES * (t + 1)].reshape(count, 8, LANES) for t in range(4)
        )
        u = jnp.where(upper > 0.0, jnp.where(lane3, e1, o1), jnp.where(lane3, e0, o0))
        w = jnp.where(upper_swap > 0.0, jnp.where(lane3, o1, e1), jnp.where(lane3, o0, e0))
        k_ref[kind, 0:count] = jnp.where(direct > 0.0, u, lane_swap(w))
    first, second, third = (k_ref[kind, 0:count] for kind in range(3))
    source = lax.broadcasted_iota(jnp.int32, (1, 8, LANES), 1) < 4
    real = first + jnp.where(source, -third, second)
    imag = first + jnp.where(source, second, -third)
    both = jnp.concatenate([real, imag], axis=1)
    return jnp.where(exists, both, 0.0).astype(BF16)


INNER = (-6, 22)


def inner_kernel(units, near_ref, a1_ref, b1_ref, w_ref, out_ref, x_ref, k_ref, pick_ref):
    unit = lax.div(lax.axis_index("lat"), 2)
    odd_unit = lax.rem(unit, 2) == 1
    has_l1, has_r1 = unit >= 1, unit + 1 < units
    coef_n = 18
    left = valid(has_l1, choose(odd_unit, a1_ref, b1_ref, 0, coef_n))
    right = valid(has_r1, choose(odd_unit, b1_ref, a1_ref, 0, coef_n))
    middle = middle_coefs(near_ref, left, right, has_l1, has_r1, coef_n)
    put_coefs(x_ref, jnp.concatenate(middle, axis=0))
    pos = coef_n + 8
    pick_ref[0:16] = jnp.where(has_l1, choose(odd_unit, a1_ref, b1_ref, pos, pos + 1)[0], -1.0)
    pick_ref[16:32] = near_ref[pos].astype(F32)
    pick_ref[32:48] = jnp.where(has_r1, choose(odd_unit, b1_ref, a1_ref, pos, pos + 1)[0], -1.0)
    lo, hi = INNER
    out_ref[...] = band_product(
        x_ref, ((lo - 8 + 15, hi - lo),), pick_ref[lo + 16 : hi + 16], w_ref, k_ref
    )


def main_kernel(
    units,
    near_ref,
    last_ref,
    a1_ref,
    b1_ref,
    a2_ref,
    b2_ref,
    w_ref,
    forward_ref,
    inverse_ref,
    inner_ref,
    keep_ref,
    send_ref,
    x_ref,
    p_ref,
    k_ref,
    xe_ref,
    xo_ref,
    slow_ref,
    cos_ref,
    sin_ref,
    pick_ref,
    image_ref,
):
    place = lax.axis_index("lat")
    unit = lax.div(place, 2)
    second = lax.rem(place, 2)
    odd_unit = lax.rem(unit, 2) == 1
    odd_quad = lax.rem(lax.div(place, 4), 2) == 1
    has_l1, has_l2 = unit >= 1, unit >= 2
    has_r1, has_r2 = unit + 1 < units, unit + 2 < units
    pairs = 16
    coef_n = pairs + 2
    far_n = a2_ref.shape[0] - 3

    left = valid(has_l1, choose(odd_unit, a1_ref, b1_ref, 0, coef_n))
    right = valid(has_r1, choose(odd_unit, b1_ref, a1_ref, 0, coef_n))
    left2 = valid(has_l2, choose(odd_quad, a2_ref, b2_ref, 0, far_n))
    right2 = valid(has_r2, choose(odd_quad, b2_ref, a2_ref, 0, far_n))
    near_left = jnp.concatenate([valid(has_l2, left[0:1]), left[1:2]], axis=0)
    near_right = jnp.concatenate(
        [right[coef_n - 2 : coef_n - 1], valid(has_r2, right[coef_n - 1 :])], axis=0
    )
    put_coefs(
        x_ref,
        jnp.concatenate(
            [left2[: far_n - 2], left2[far_n - 2 :] + near_left]
            + middle_coefs(near_ref, left, right, has_l1, has_r1, coef_n)
            + [right2[:2] + near_right, right2[2:]],
            axis=0,
        ),
    )

    at = coef_n
    far_rows = 48
    for step in range(2):
        lo = at + 4 * step
        for flag, pos in ((odd_unit, -32), (jnp.logical_not(odd_unit), 32)):
            hi_v = choose(flag, a1_ref, b1_ref, lo, lo + 2)
            lo_v = choose(flag, a1_ref, b1_ref, lo + 2, lo + 4)
            slow_ref[step, far_rows + pos : far_rows + pos + 32] = (hi_v + lo_v).reshape(32, LANES)
        slow_ref[step, far_rows : far_rows + 32] = (
            near_ref[lo : lo + 2].astype(F32) + near_ref[lo + 2 : lo + 4].astype(F32)
        ).reshape(32, LANES)
    for flag, pos in ((odd_quad, -48), (jnp.logical_not(odd_quad), 64)):
        rows = choose(flag, a2_ref, b2_ref, far_n, far_n + 1) + choose(
            flag, a2_ref, b2_ref, far_n + 1, far_n + 2
        )
        slow_ref[0, far_rows + pos : far_rows + pos + 16] = rows[0]
    slow_ref[2, far_rows : far_rows + 32] = (
        last_ref[0:2].astype(F32) + last_ref[2:4].astype(F32)
    ).reshape(32, LANES)

    for step in range(STEPS):
        pos = coef_n + 8 + step
        pick_ref[step, 32:48] = near_ref[pos].astype(F32)
        pick_ref[step, 16:32] = jnp.where(
            has_l1, choose(odd_unit, a1_ref, b1_ref, pos, pos + 1)[0], -1.0)
        pick_ref[step, 48:64] = jnp.where(
            has_r1, choose(odd_unit, b1_ref, a1_ref, pos, pos + 1)[0], -1.0)
    pick_ref[0, 0:16] = jnp.where(
        has_l2, choose(odd_quad, a2_ref, b2_ref, far_n + 2, far_n + 3)[0], -1.0)
    pick_ref[0, 64:80] = jnp.where(
        has_r2, choose(odd_quad, b2_ref, a2_ref, far_n + 2, far_n + 3)[0], -1.0)

    sign = sign_rows()
    row3 = lax.broadcasted_iota(jnp.int32, (1, 8, LANES), 1) < 4
    lane3 = low_lanes((1, 1, LANES))
    lane2 = low_lanes((1, LANES))

    plan = (
        dict(lo=-18, hi=34, base=26, first=-17),
        dict(lo=-9, hi=25, base=17, first=-9),
        dict(lo=-1, hi=17, base=9, first=0),
    )
    for step, item in enumerate(plan):
        lo, hi = item["lo"], item["hi"]
        count = hi - lo
        p_ref[0] = jnp.zeros((16, LANES), BF16)
        if step == 0:
            parts = ((lo, INNER[0] - lo), (INNER[1], hi - INNER[1]))
            p_ref[1 + INNER[0] - lo : 1 + INNER[1] - lo] = inner_ref[...]
        else:
            parts = ((lo, count),)
        rows = jnp.concatenate(
            [pick_ref[step, a + 32 : a + 32 + m] for a, m in parts], axis=0
        )
        out = band_product(
            x_ref, [(item["base"] + a - 8, m) for a, m in parts], rows, w_ref, k_ref
        )
        done = 0
        for a, m in parts:
            p_ref[1 + a - lo : 1 + a - lo + m] = out[done : done + m]
            done += m
        first = item["first"]
        n = hi - first
        o = first - lo
        lhs = jnp.concatenate(
            [p_ref[o : o + n].reshape(n * 16, LANES), p_ref[o + 1 : o + 1 + n].reshape(n * 16, LANES)],
            axis=1,
        )
        back = jnp.dot(lhs, inverse_ref[...], preferred_element_type=F32)
        g0 = 2 * first + far_rows
        before = slow_ref[step, g0 - 1 : g0 - 1 + 2 * n]
        after = slow_ref[step, g0 : g0 + 2 * n]
        if step < 2:
            number = lax.broadcasted_iota(jnp.int32, (2 * n, 1), 0) + 2 * first

            def exists(block):
                inside = (block >= 0) & (block < 32)
                l1 = (block < 0) & (block >= -32) & has_l1
                r1 = (block >= 32) & (block < 64) & has_r1
                l2 = (block < -32) & has_l2
                r2 = (block >= 64) & has_r2
                return inside | l1 | r1 | l2 | r2

            ok = jnp.where(lane2, exists(number - 1).astype(jnp.int32), exists(number).astype(jnp.int32)) > 0
        theta = jnp.where(lane2, lane_swap(before), lane_swap(after))
        sin_v, cos_v = sin_cos(theta)
        if step < 2:
            sin_v = jnp.where(ok, sin_v, 0.0)
            cos_v = jnp.where(ok, cos_v, 0.0)
        cos_ref[0 : 2 * n] = cos_v
        sin_ref[0 : 2 * n] = sin_v
        images = []
        for parity, sample_ref in ((0, xe_ref), (1, xo_ref)):
            b = back[:, LANES * parity : LANES * (parity + 1)].reshape(n, 16, LANES)
            c = cos_ref[pl.ds(parity, n, stride=2)].reshape(n, 1, LANES)
            s = sin_ref[pl.ds(parity, n, stride=2)].reshape(n, 1, LANES) * sign
            f0 = c * b[:, :8] - s * b[:, 8:]
            f1 = c * b[:, 8:] + s * b[:, :8]
            if step < 2:
                sample_ref[0:n] = jnp.concatenate([f0, f1], axis=1).astype(BF16)
            m = 17 - parity
            f0, f1 = f0[-first : -first + m], f1[-first : -first + m]
            images.append(lane_swap(f0 * pltpu.roll(f0, 4, 1) + f1 * pltpu.roll(f1, 4, 1)))
        even, odd = images
        image_ref[step, 0] = jnp.where(lane3, even[:16], odd)
        image_ref[step, 1] = jnp.where(lane3, odd, even[1:])
        if step < 2:
            if step == 1:
                xe_ref[n] = jnp.zeros((16, LANES), BF16)
                m = n
            else:
                m = n - 1
            lhs = jnp.concatenate(
                [
                    xe_ref[0:m].reshape(m * 16, LANES),
                    xo_ref[0:m].reshape(m * 16, LANES),
                    xe_ref[1 : m + 1].reshape(m * 16, LANES),
                ],
                axis=1,
            )
            coefs = jnp.dot(lhs, forward_ref[...], preferred_element_type=F32).reshape(m, 16, LANES)
            number = lax.broadcasted_iota(jnp.int32, (m, 1, 1), 0) + first
            ok = (
                ((number >= 0) & (number < 16))
                | ((number < 0) & (number >= -16) & has_l1)
                | ((number >= 16) & (number < 32) & has_r1)
                | ((number < -16) & has_l2)
                | ((number >= 32) & has_r2)
            )
            put_coefs(x_ref, jnp.where(ok, coefs, 0.0))
    for ref, half in ((keep_ref, second), (send_ref, 1 - second)):
        span = pl.ds(8 * half, 8)
        tops = [
            jnp.where(row3, image_ref[0, parity, span], image_ref[1, parity, span])
            for parity in range(2)
        ]
        ref[0:8] = jnp.concatenate(tops, axis=1).astype(BF16)
        last = jnp.where(row3, image_ref[2, 0, span], image_ref[2, 1, span])
        ref[8:12] = last.reshape(4, 16, LANES).astype(BF16)


def image_rows(tiles, step, block):
    q, parity = divmod(block, 2)
    if step < 2:
        row = 8 * parity + 4 * step
        return tiles[q, row : row + 4]
    row = 8 * (q % 2) + 4 * parity
    return tiles[8 + q // 2, row : row + 4]


def final_kernel(a_ref, b_ref, out_ref):
    total = a_ref[...].astype(F32) + b_ref[...].astype(F32)
    for block in range(out_ref.shape[-1] // WINDOW):
        cut = slice(WINDOW * block, WINDOW * (block + 1))
        for n in range(STEPS):
            out_ref[n, :, cut] = image_rows(total, n, block)


def matching(size, by, odd):
    pairs = []
    for i in range(size):
        right = (i // by) % 2 == odd
        j = i + by if right else i - by
        pairs.append((i, j if 0 <= j < size else i))
    return pairs


def on_device(wavefield, propagator_table, table_index, slowness, frequency_scale):
    sources = wavefield.shape[2]
    points = wavefield.shape[3]
    lat = lax.axis_size("lat")
    freqs = lax.axis_size("freq")
    pairs = points // (2 * WINDOW)
    first, forward, inverse = (jnp.asarray(m, BF16) for m in pair_matrices())
    vmem = pl.BlockSpec(memory_space=pltpu.VMEM)
    hbm = pl.BlockSpec(memory_space=pltpu.HBM)

    def tiles(n):
        return jax.ShapeDtypeStruct((n, 16, LANES), BF16)

    info = 8
    keep, send = pl.pallas_call(
        prep_kernel,
        out_shape=(tiles(pairs + 2), tiles(pairs + 2 + info)),
        in_specs=[hbm] * 4,
        out_specs=(vmem, vmem),
        scratch_shapes=[
            pltpu.VMEM(wavefield.shape, F32),
            pltpu.VMEM(slowness.shape, F32),
            pltpu.SMEM(table_index.shape, jnp.int32),
            pltpu.VMEM(first.shape, BF16),
            pltpu.VMEM((2, pairs + 2, 16, LANES), BF16),
            pltpu.VMEM((info * 16, LANES), F32),
            pltpu.SemaphoreType.DMA((4,)),
        ],
        compiler_params=pltpu.CompilerParams(vmem_limit_bytes=8 << 20),
        cost_estimate=pl.CostEstimate(flops=10**9, bytes_accessed=10**7, transcendentals=0),
        name="prep",
    )(
        *(
            pltpu.with_memory_space_constraint(x, pltpu.HBM)
            for x in (wavefield, slowness, table_index, first)
        )
    )
    partner = [(i, i ^ 1) for i in range(lat)]
    got = lax.ppermute(send, "lat", partner)
    near_n = 2 * (pairs + 2) - 2 + 8 + STEPS
    far_n = 11 + 3
    near, far_a, far_b, last = pl.pallas_call(
        unit_kernel,
        out_shape=(tiles(near_n), tiles(far_n), tiles(far_n), tiles(4)),
        in_specs=[vmem] * 4,
        out_specs=(vmem,) * 4,
        compiler_params=pltpu.CompilerParams(vmem_limit_bytes=4 << 20),
        name="unit",
    )(keep, send, got, frequency_scale[None])
    a1 = lax.ppermute(near, "lat", matching(lat, 2, 0))
    b1 = lax.ppermute(near, "lat", matching(lat, 2, 1))
    a2 = lax.ppermute(far_a, "lat", matching(lat, 4, 0))
    b2 = lax.ppermute(far_b, "lat", matching(lat, 4, 1))
    inner_n = INNER[1] - INNER[0]
    table = propagator_table[0]
    weights = pl.pallas_call(
        weight_kernel,
        out_shape=jax.ShapeDtypeStruct((3, table.shape[0] // 2) + table.shape[1:], BF16),
        in_specs=[vmem],
        out_specs=vmem,
        compiler_params=pltpu.CompilerParams(vmem_limit_bytes=16 << 20),
        cost_estimate=pl.CostEstimate(flops=10**8, bytes_accessed=10**7, transcendentals=0),
        name="weights",
    )(table)
    inner = pl.pallas_call(
        lambda *refs: inner_kernel(lat // 2, *refs),
        out_shape=tiles(inner_n),
        in_specs=[vmem] * 4,
        out_specs=vmem,
        scratch_shapes=[
            pltpu.VMEM((3, 2, 23, 16, LANES), BF16),
            pltpu.VMEM((3, inner_n, 8, LANES), F32),
            pltpu.VMEM((48, LANES), F32),
        ],
        compiler_params=pltpu.CompilerParams(vmem_limit_bytes=24 << 20),
        cost_estimate=pl.CostEstimate(flops=2 * 10**9, bytes_accessed=10**7, transcendentals=0),
        name="inner",
    )(near, a1, b1, weights)
    own, other = pl.pallas_call(
        lambda *refs: main_kernel(lat // 2, *refs),
        out_shape=(tiles(12),) * 2,
        in_specs=[vmem] * 10,
        out_specs=(vmem,) * 2,
        scratch_shapes=[
            pltpu.VMEM((3, 2, 34, 16, LANES), BF16),
            pltpu.VMEM((53, 16, LANES), BF16),
            pltpu.VMEM((3, 34, 8, LANES), F32),
            pltpu.VMEM((52, 16, LANES), BF16),
            pltpu.VMEM((52, 16, LANES), BF16),
            pltpu.VMEM((STEPS, 128, LANES), F32),
            pltpu.VMEM((104, LANES), F32),
            pltpu.VMEM((104, LANES), F32),
            pltpu.VMEM((STEPS, 80, LANES), F32),
            pltpu.VMEM((STEPS, 2, 16, 8, LANES), F32),
        ],
        compiler_params=pltpu.CompilerParams(vmem_limit_bytes=32 << 20),
        name="steps",
    )(near, last, a1, b1, a2, b2, weights, forward, inverse, inner)
    swapped = lax.ppermute(other, "lat", partner)
    core = lax.rem(lax.axis_index("lat"), 2)
    if freqs == 2:
        mine = core == lax.axis_index("freq")
        stay = jnp.where(mine, own, swapped)
        leave = jnp.where(mine, swapped, own)
        come = lax.ppermute(leave, "freq", [(0, 1), (1, 0)])
        return pl.pallas_call(
            final_kernel,
            out_shape=jax.ShapeDtypeStruct((STEPS, sources // 2, points), F32),
            in_specs=[vmem] * 2,
            out_specs=vmem,
            compiler_params=pltpu.CompilerParams(vmem_limit_bytes=4 << 20),
            name="total",
        )(stay, come)
    parts = [jnp.where(core == 0, own, swapped), jnp.where(core == 0, swapped, own)]
    rows = [
        [jnp.stack([image_rows(p, n, b) for b in range(2 * pairs)], axis=1) for p in parts]
        for n in range(STEPS)
    ]
    whole = jnp.stack([jnp.concatenate(r, axis=0) for r in rows])
    whole = whole.reshape(STEPS, sources, points)
    return lax.psum_scatter(whole, "freq", scatter_dimension=1, tiled=True).astype(F32)


def solution(mesh):
    placed = (
        P(None, "freq", None, "lat"),
        P("freq", None, None, None),
        P(None, "lat"),
        P(None, "lat"),
        P("freq"),
    )

    return jax.shard_map(
        on_device, mesh=mesh, in_specs=placed, out_specs=P(None, "freq", "lat"), check_vma=False
    )
```

```python
import math

import jax
import jax.numpy as jnp
import numpy as np
from jax import lax
from jax.experimental import pallas as pl
from jax.experimental.pallas import tpu as pltpu
from jax.sharding import PartitionSpec as P


WINDOW = 128
COEFS = 64
REACH = 16
STEPS = 3
HALF = WINDOW // 2
F32 = jnp.float32
BF16 = jnp.bfloat16
LANES = 2 * COEFS


def basis_table():
    t = np.arange(2 * WINDOW, dtype=np.float32)[:, None]
    k = np.arange(COEFS, dtype=np.float32)[None, :]
    taper = np.sin(np.float32(math.pi) * (t + np.float32(0.5)) / np.float32(2 * WINDOW))
    wave = np.cos(
        np.float32(math.pi)
        * (k + np.float32(0.5))
        * (t - np.float32(HALF) + np.float32(0.5))
        / np.float32(WINDOW)
    )
    return (taper * np.float32(math.sqrt(2.0 / WINDOW)) * wave).astype(np.float32)


def pair_matrices():
    b = basis_table()
    first = np.zeros((4 * WINDOW, LANES), np.float32)
    first[HALF : HALF + 2 * WINDOW, :COEFS] = b
    first[HALF + WINDOW : HALF + 3 * WINDOW, COEFS:] = b
    forward = np.zeros((3 * WINDOW, LANES), np.float32)
    forward[: 2 * WINDOW, :COEFS] = b
    forward[WINDOW:, COEFS:] = b
    inverse = np.zeros((4 * COEFS, 2 * WINDOW), np.float32)
    inverse[COEFS : 2 * COEFS, :WINDOW] = b[WINDOW:].T
    inverse[2 * COEFS : 3 * COEFS, :WINDOW] = b[:WINDOW].T
    inverse[2 * COEFS : 3 * COEFS, WINDOW:] = b[WINDOW:].T
    inverse[3 * COEFS :, WINDOW:] = b[:WINDOW].T
    return first, forward, inverse


def sin_cos(theta):
    turns = jnp.floor(theta * np.float32(2.0 / math.pi) + np.float32(0.5))
    r = theta - turns * np.float32(1.5703125)
    r = r - turns * np.float32(4.837512969970703e-4)
    r = r - turns * np.float32(7.549789948768648e-8)
    r2 = r * r
    s = r + r * r2 * (
        np.float32(-1.6666654611e-1)
        + r2 * (np.float32(8.3321608736e-3) + r2 * np.float32(-1.9515295891e-4))
    )
    c = 1.0 - 0.5 * r2 + r2 * r2 * (
        np.float32(4.166664568298827e-2)
        + r2 * (np.float32(-1.388731625493765e-3) + r2 * np.float32(2.443315711809948e-5))
    )
    quarter = turns - 4.0 * jnp.floor(turns * 0.25)
    odd = (quarter == 1.0) | (quarter == 3.0)
    sin_v = jnp.where(odd, c, s)
    cos_v = jnp.where(odd, s, c)
    sin_v = jnp.where(quarter >= 2.0, -sin_v, sin_v)
    cos_v = jnp.where((quarter == 1.0) | (quarter == 2.0), -cos_v, cos_v)
    return sin_v, cos_v


def lane_swap(v):
    return pltpu.roll(v, LANES // 2, v.ndim - 1)


def low_lanes(shape):
    return lax.broadcasted_iota(jnp.int32, shape, len(shape) - 1) < LANES // 2


def prep_kernel(
    wave_hbm,
    slow_hbm,
    index_hbm,
    first_hbm,
    keep_ref,
    send_ref,
    wave_ref,
    slow_ref,
    index_ref,
    first_ref,
    both_ref,
    rows_ref,
    sems,
):
    copies = [
        pltpu.make_async_copy(source, target, sems.at[i])
        for i, (source, target) in enumerate(
            (
                (wave_hbm, wave_ref),
                (first_hbm, first_ref),
                (slow_hbm, slow_ref),
                (index_hbm, index_ref),
            )
        )
    ]
    for copy in copies:
        copy.start()
    core = lax.rem(lax.axis_index("lat"), 2)
    copies[2].wait()
    copies[3].wait()
    blocks = wave_ref.shape[-1] // WINDOW
    pairs = blocks // 2
    slow = slow_ref[...]
    high = slow.astype(BF16).astype(F32)
    rest = slow - high
    lanes = low_lanes((1, LANES))
    rows_ref[...] = jnp.zeros(rows_ref.shape, F32)
    for n in range(STEPS):
        for g in range(blocks):
            cut = slice(WINDOW * g, WINDOW * (g + 1))
            rows_ref[(2 * n) * blocks + g : (2 * n) * blocks + g + 1, :] = high[n : n + 1, cut]
            rows_ref[(2 * n + 1) * blocks + g : (2 * n + 1) * blocks + g + 1, :] = rest[n : n + 1, cut]
        for q in range(pairs):
            at = 2 * STEPS * blocks + n * pairs + q
            rows_ref[at : at + 1, :] = jnp.where(
                lanes,
                jnp.full((1, LANES), index_ref[n, 2 * q], jnp.int32),
                jnp.full((1, LANES), index_ref[n, 2 * q + 1], jnp.int32),
            ).astype(F32)
    send_ref[pairs + 2 :] = rows_ref[...].reshape(-1, 16, LANES).astype(BF16)
    copies[0].wait()
    copies[1].wait()
    upper = lax.broadcasted_iota(jnp.int32, (8, wave_ref.shape[-1]), 0) < 4
    for side in range(2):
        halves = []
        for low in range(2):
            near, far = wave_ref[low, 0], wave_ref[low + 2, 0]
            if side == 0:
                halves.append(jnp.where(upper, near, pltpu.roll(far, 4, 0)))
            else:
                halves.append(jnp.where(upper, pltpu.roll(near, 4, 0), far))
        samples = jnp.concatenate(halves, axis=0).astype(BF16)
        zero = jnp.zeros((16, WINDOW), BF16)
        padded = [zero] * 3
        padded += [samples[:, WINDOW * g : WINDOW * (g + 1)] for g in range(blocks)]
        padded += [zero] * 3
        parts = [
            jnp.concatenate([padded[2 * i + j] for i in range(pairs + 2)], axis=0)
            for j in range(4)
        ]
        coefs = jnp.dot(
            jnp.concatenate(parts, axis=1), first_ref[...], preferred_element_type=F32
        )
        both_ref[side] = coefs.reshape(pairs + 2, 16, LANES).astype(BF16)
    keep_ref[...] = both_ref[core]
    send_ref[0 : pairs + 2] = both_ref[1 - core]


def unit_kernel(keep_ref, sent_ref, got_ref, scale_ref, near_ref, far_a_ref, far_b_ref, own_ref):
    place = lax.axis_index("lat")
    second = lax.rem(place, 2) == 1
    n = keep_ref.shape[0]
    own_c, own_i = keep_ref[...].astype(F32), sent_ref[n:].astype(F32)
    got_c, got_i = got_ref[:n].astype(F32), got_ref[n:].astype(F32)
    b0 = jnp.where(second, got_c, own_c)
    b1 = jnp.where(second, own_c, got_c)
    i0 = jnp.where(second, got_i, own_i)
    i1 = jnp.where(second, own_i, got_i)
    unit = jnp.concatenate([b0[: n - 2], b0[n - 2 :] + b1[:2], b1[2:]], axis=0)
    near_ref[0] = jnp.where(low_lanes((16, LANES)), unit[2 * n - 3], unit[0]).astype(BF16)
    near_ref[1 : 2 * n - 3] = unit[1 : 2 * n - 3].astype(BF16)
    at = 2 * n - 3
    phases = []
    for step in range(STEPS):
        for block, info in enumerate((i0, i1)):
            theta = scale_ref[...] * (info[2 * step] + info[2 * step + 1])
            own_ref[step, 16 * block : 16 * block + 16] = theta
            turns = jnp.floor(theta * np.float32(0.5 / math.pi) + np.float32(0.5))
            theta = theta - turns * np.float32(6.28125)
            theta = theta - turns * np.float32(2.0 * math.pi - 6.28125)
            phases.append(theta)
            if step < 2:
                near_ref[at + 2 * step + block] = theta.astype(BF16)
    at += 4
    near_ref[at] = jnp.concatenate([i0[6, :8], i1[6, :8]], axis=0).astype(BF16)
    near_ref[at + 1] = jnp.concatenate([i0[6, 8:], i1[6, 8:]], axis=0).astype(BF16)
    near_ref[at + 2] = jnp.concatenate([i0[7, :8], i1[7, :8]], axis=0).astype(BF16)
    even_quad = lax.rem(lax.div(place, 4), 2) == 0
    count = far_a_ref.shape[0] - 1
    top = jnp.concatenate([phases[1][8:], i1[6, :8]], axis=0)
    bottom = jnp.concatenate([phases[0][:8], i0[6, :8]], axis=0)
    for ref, right in ((far_a_ref, even_quad), (far_b_ref, jnp.logical_not(even_quad))):
        ref[0:count] = jnp.where(right, unit[2 * n - 2 - count :], unit[:count]).astype(BF16)
        ref[count] = jnp.where(right, top, bottom).astype(BF16)


def sign_rows():
    row = lax.broadcasted_iota(jnp.int32, (1, 8, LANES), 1)
    return jnp.where(row < 4, 1.0, -1.0).astype(F32)


def valid(flag, v):
    return jnp.where(flag, v, jnp.zeros_like(v))


def choose(flag, x_ref, y_ref, lo, hi):
    return jnp.where(flag, x_ref[lo:hi], y_ref[lo:hi]).astype(F32)


def whole_unit(tiles):
    low = low_lanes((1, 16, LANES))
    edge = tiles[0:1]
    return jnp.concatenate(
        [jnp.where(low, 0.0, edge), tiles[1:], jnp.where(low, edge, 0.0)], axis=0
    )


def middle_coefs(near_ref, left, right, has_l1, has_r1, coef_n):
    own = whole_unit(near_ref[0 : coef_n - 1].astype(F32))
    return [
        left[2 : coef_n - 2],
        left[coef_n - 2 :] + jnp.concatenate([valid(has_l1, own[0:1]), own[1:2]], axis=0),
        own[2 : coef_n - 2],
        right[:2]
        + jnp.concatenate([own[coef_n - 2 : coef_n - 1], valid(has_r1, own[coef_n - 1 :])], axis=0),
        right[2 : coef_n - 2],
    ]


def put_coefs(x_ref, coefs):
    n = coefs.shape[0]
    coefs = coefs.astype(BF16).astype(F32)
    real, imag = coefs[:, :8], coefs[:, 8:]
    source = lax.broadcasted_iota(jnp.int32, (1, 8, LANES), 1) < 4
    kinds = (real + imag, jnp.where(source, real, imag), jnp.where(source, imag, real))
    for kind, x in enumerate(kinds):
        x_ref[kind, 0, 0 : n // 2] = x.reshape(n // 2, 16, LANES).astype(BF16)
        x_ref[kind, 1, 0 : n // 2 - 1] = x[1 : n - 1].reshape(n // 2 - 1, 16, LANES).astype(BF16)


def weight_kernel(table_ref, w_ref):
    for duo in range(table_ref.shape[0] // 2):
        a, b = table_ref[2 * duo], table_ref[2 * duo + 1]
        low = low_lanes(a.shape)
        real = jnp.where(low, a, jnp.concatenate([b[:, COEFS:], b[:, :COEFS]], axis=1))
        imag = jnp.where(low, jnp.concatenate([a[:, COEFS:], a[:, :COEFS]], axis=1), b)
        w_ref[0, duo] = real
        w_ref[1, duo] = imag - real
        w_ref[2, duo] = imag + real


def band_product(x_ref, parts, rows, w_ref, k_ref):
    count = sum(n for _, n in parts)
    lane2, lane3 = low_lanes((1, LANES)), low_lanes((1, 1, LANES))
    half = jnp.floor(rows * 0.5)
    even = (rows - 2.0 * half) == 0.0
    direct = jnp.where(lane2, even.astype(F32), 1.0 - even.astype(F32)).reshape(count, 1, LANES)
    upper = half.reshape(count, 1, LANES)
    upper_swap = lane_swap(half).reshape(count, 1, LANES)
    exists = rows.reshape(count, 1, LANES) >= 0.0
    zero = jnp.zeros((COEFS, 2 * LANES), BF16)

    def band(kind, k):
        pieces = [
            x_ref[kind, (o + k) % 2, (o + k) // 2 : (o + k) // 2 + n // 2] for o, n in parts
        ]
        return jnp.concatenate(pieces, axis=0).reshape(count * 8, LANES)

    for kind in range(3):
        lhs = jnp.concatenate([band(kind, k) for k in range(REACH + 1)], axis=1)
        full = jnp.concatenate([w_ref[kind, 0], w_ref[kind, 1]], axis=1)
        rhs = jnp.concatenate(
            [jnp.concatenate([full, zero], axis=0), jnp.concatenate([zero, full], axis=0)], axis=1
        )
        out = jnp.dot(lhs, rhs, preferred_element_type=F32)
        e0, e1, o0, o1 = (
            out[:, LANES * t : LANES * (t + 1)].reshape(count, 8, LANES) for t in range(4)
        )
        u = jnp.where(upper > 0.0, jnp.where(lane3, e1, o1), jnp.where(lane3, e0, o0))
        w = jnp.where(upper_swap > 0.0, jnp.where(lane3, o1, e1), jnp.where(lane3, o0, e0))
        k_ref[kind, 0:count] = jnp.where(direct > 0.0, u, lane_swap(w))
    first, second, third = (k_ref[kind, 0:count] for kind in range(3))
    source = lax.broadcasted_iota(jnp.int32, (1, 8, LANES), 1) < 4
    real = first + jnp.where(source, -third, second)
    imag = first + jnp.where(source, second, -third)
    both = jnp.concatenate([real, imag], axis=1)
    return jnp.where(exists, both, 0.0).astype(BF16)


INNER = (-6, 22)


def inner_kernel(units, near_ref, a1_ref, b1_ref, w_ref, out_ref, x_ref, k_ref, pick_ref):
    unit = lax.div(lax.axis_index("lat"), 2)
    odd_unit = lax.rem(unit, 2) == 1
    has_l1, has_r1 = unit >= 1, unit + 1 < units
    coef_n = 18
    left = valid(has_l1, whole_unit(choose(odd_unit, a1_ref, b1_ref, 0, coef_n - 1)))
    right = valid(has_r1, whole_unit(choose(odd_unit, b1_ref, a1_ref, 0, coef_n - 1)))
    middle = middle_coefs(near_ref, left, right, has_l1, has_r1, coef_n)
    put_coefs(x_ref, jnp.concatenate(middle, axis=0))
    pos = coef_n + 3
    pick_ref[0:16] = jnp.where(has_l1, choose(odd_unit, a1_ref, b1_ref, pos, pos + 1)[0], -1.0)
    pick_ref[16:32] = near_ref[pos].astype(F32)
    pick_ref[32:48] = jnp.where(has_r1, choose(odd_unit, b1_ref, a1_ref, pos, pos + 1)[0], -1.0)
    lo, hi = INNER
    out_ref[...] = band_product(
        x_ref, ((lo - 8 + 15, hi - lo),), pick_ref[lo + 16 : hi + 16], w_ref, k_ref
    )


def main_kernel(
    units,
    near_ref,
    own_ref,
    a1_ref,
    b1_ref,
    a2_ref,
    b2_ref,
    w_ref,
    forward_ref,
    inverse_ref,
    inner_ref,
    keep_ref,
    send_ref,
    x_ref,
    p_ref,
    k_ref,
    xe_ref,
    xo_ref,
    slow_ref,
    cos_ref,
    sin_ref,
    pick_ref,
    image_ref,
):
    place = lax.axis_index("lat")
    unit = lax.div(place, 2)
    second = lax.rem(place, 2)
    odd_unit = lax.rem(unit, 2) == 1
    odd_quad = lax.rem(lax.div(place, 4), 2) == 1
    has_l1, has_l2 = unit >= 1, unit >= 2
    has_r1, has_r2 = unit + 1 < units, unit + 2 < units
    pairs = 16
    coef_n = pairs + 2
    far_n = a2_ref.shape[0] - 1

    left = valid(has_l1, whole_unit(choose(odd_unit, a1_ref, b1_ref, 0, coef_n - 1)))
    right = valid(has_r1, whole_unit(choose(odd_unit, b1_ref, a1_ref, 0, coef_n - 1)))
    left2 = valid(has_l2, choose(odd_quad, a2_ref, b2_ref, 0, far_n))
    right2 = valid(has_r2, choose(odd_quad, b2_ref, a2_ref, 0, far_n))
    near_left = jnp.concatenate([valid(has_l2, left[0:1]), left[1:2]], axis=0)
    near_right = jnp.concatenate(
        [right[coef_n - 2 : coef_n - 1], valid(has_r2, right[coef_n - 1 :])], axis=0
    )
    put_coefs(
        x_ref,
        jnp.concatenate(
            [left2[: far_n - 2], left2[far_n - 2 :] + near_left]
            + middle_coefs(near_ref, left, right, has_l1, has_r1, coef_n)
            + [right2[:2] + near_right, right2[2:]],
            axis=0,
        ),
    )

    far_rows = 48
    for step in range(STEPS):
        slow_ref[step, far_rows : far_rows + 32] = own_ref[step]
    for step in range(2):
        lo = coef_n - 1 + 2 * step
        for flag, pos in ((odd_unit, -32), (jnp.logical_not(odd_unit), 32)):
            rows = choose(flag, a1_ref, b1_ref, lo, lo + 2)
            slow_ref[step, far_rows + pos : far_rows + pos + 32] = rows.reshape(32, LANES)
    before2 = choose(odd_quad, a2_ref, b2_ref, far_n, far_n + 1)[0]
    after2 = choose(odd_quad, b2_ref, a2_ref, far_n, far_n + 1)[0]
    slow_ref[0, far_rows - 40 : far_rows - 32] = before2[:8]
    slow_ref[0, far_rows + 64 : far_rows + 72] = after2[:8]

    for step in range(STEPS):
        pos = coef_n + 3 + step
        pick_ref[step, 32:48] = near_ref[pos].astype(F32)
        pick_ref[step, 16:32] = jnp.where(
            has_l1, choose(odd_unit, a1_ref, b1_ref, pos, pos + 1)[0], -1.0)
        pick_ref[step, 48:64] = jnp.where(
            has_r1, choose(odd_unit, b1_ref, a1_ref, pos, pos + 1)[0], -1.0)
    pick_ref[0, 8:16] = jnp.where(has_l2, before2[8:], -1.0)
    pick_ref[0, 64:72] = jnp.where(has_r2, after2[8:], -1.0)

    sign = sign_rows()
    row3 = lax.broadcasted_iota(jnp.int32, (1, 8, LANES), 1) < 4
    lane3 = low_lanes((1, 1, LANES))
    lane2 = low_lanes((1, LANES))

    plan = (
        dict(lo=-18, hi=34, base=26, first=-17),
        dict(lo=-9, hi=25, base=17, first=-9),
        dict(lo=-1, hi=17, base=9, first=0),
    )
    for step, item in enumerate(plan):
        lo, hi = item["lo"], item["hi"]
        count = hi - lo
        p_ref[0] = jnp.zeros((16, LANES), BF16)
        if step == 0:
            parts = ((lo, INNER[0] - lo), (INNER[1], hi - INNER[1]))
            p_ref[1 + INNER[0] - lo : 1 + INNER[1] - lo] = inner_ref[...]
        else:
            parts = ((lo, count),)
        rows = jnp.concatenate(
            [pick_ref[step, a + 32 : a + 32 + m] for a, m in parts], axis=0
        )
        out = band_product(
            x_ref, [(item["base"] + a - 8, m) for a, m in parts], rows, w_ref, k_ref
        )
        done = 0
        for a, m in parts:
            p_ref[1 + a - lo : 1 + a - lo + m] = out[done : done + m]
            done += m
        first = item["first"]
        n = hi - first
        o = first - lo
        lhs = jnp.concatenate(
            [p_ref[o : o + n].reshape(n * 16, LANES), p_ref[o + 1 : o + 1 + n].reshape(n * 16, LANES)],
            axis=1,
        )
        back = jnp.dot(lhs, inverse_ref[...], preferred_element_type=F32)
        g0 = 2 * first + far_rows
        before = slow_ref[step, g0 - 1 : g0 - 1 + 2 * n]
        after = slow_ref[step, g0 : g0 + 2 * n]
        if step < 2:
            number = lax.broadcasted_iota(jnp.int32, (2 * n, 1), 0) + 2 * first

            def exists(block):
                inside = (block >= 0) & (block < 32)
                l1 = (block < 0) & (block >= -32) & has_l1
                r1 = (block >= 32) & (block < 64) & has_r1
                l2 = (block < -32) & has_l2
                r2 = (block >= 64) & has_r2
                return inside | l1 | r1 | l2 | r2

            ok = jnp.where(lane2, exists(number - 1).astype(jnp.int32), exists(number).astype(jnp.int32)) > 0
        theta = jnp.where(lane2, lane_swap(before), lane_swap(after))
        sin_v, cos_v = sin_cos(theta)
        if step < 2:
            sin_v = jnp.where(ok, sin_v, 0.0)
            cos_v = jnp.where(ok, cos_v, 0.0)
        cos_ref[0 : 2 * n] = cos_v
        sin_ref[0 : 2 * n] = sin_v
        images = []
        for parity, sample_ref in ((0, xe_ref), (1, xo_ref)):
            b = back[:, LANES * parity : LANES * (parity + 1)].reshape(n, 16, LANES)
            c = cos_ref[pl.ds(parity, n, stride=2)].reshape(n, 1, LANES)
            s = sin_ref[pl.ds(parity, n, stride=2)].reshape(n, 1, LANES) * sign
            f0 = c * b[:, :8] - s * b[:, 8:]
            f1 = c * b[:, 8:] + s * b[:, :8]
            if step < 2:
                sample_ref[0:n] = jnp.concatenate([f0, f1], axis=1).astype(BF16)
            m = 17 - parity
            f0, f1 = f0[-first : -first + m], f1[-first : -first + m]
            images.append(lane_swap(f0 * pltpu.roll(f0, 4, 1) + f1 * pltpu.roll(f1, 4, 1)))
        even, odd = images
        image_ref[step, 0] = jnp.where(lane3, even[:16], odd)
        image_ref[step, 1] = jnp.where(lane3, odd, even[1:])
        if step < 2:
            if step == 1:
                xe_ref[n] = jnp.zeros((16, LANES), BF16)
                m = n
            else:
                m = n - 1
            lhs = jnp.concatenate(
                [
                    xe_ref[0:m].reshape(m * 16, LANES),
                    xo_ref[0:m].reshape(m * 16, LANES),
                    xe_ref[1 : m + 1].reshape(m * 16, LANES),
                ],
                axis=1,
            )
            coefs = jnp.dot(lhs, forward_ref[...], preferred_element_type=F32).reshape(m, 16, LANES)
            number = lax.broadcasted_iota(jnp.int32, (m, 1, 1), 0) + first
            ok = (
                ((number >= 0) & (number < 16))
                | ((number < 0) & (number >= -16) & has_l1)
                | ((number >= 16) & (number < 32) & has_r1)
                | ((number < -16) & has_l2)
                | ((number >= 32) & has_r2)
            )
            put_coefs(x_ref, jnp.where(ok, coefs, 0.0))
    for ref, half in ((keep_ref, second), (send_ref, 1 - second)):
        span = pl.ds(8 * half, 8)
        tops = [
            jnp.where(row3, image_ref[0, parity, span], image_ref[1, parity, span])
            for parity in range(2)
        ]
        ref[0:8] = jnp.concatenate(tops, axis=1).astype(BF16)
        last = jnp.where(row3, image_ref[2, 0, span], image_ref[2, 1, span])
        ref[8:12] = last.reshape(4, 16, LANES).astype(BF16)


def image_rows(tiles, step, block):
    q, parity = divmod(block, 2)
    if step < 2:
        row = 8 * parity + 4 * step
        return tiles[q, row : row + 4]
    row = 8 * (q % 2) + 4 * parity
    return tiles[8 + q // 2, row : row + 4]


def final_kernel(a_ref, b_ref, out_ref):
    total = a_ref[...].astype(F32) + b_ref[...].astype(F32)
    for block in range(out_ref.shape[-1] // WINDOW):
        cut = slice(WINDOW * block, WINDOW * (block + 1))
        for n in range(STEPS):
            out_ref[n, :, cut] = image_rows(total, n, block)


def matching(size, by, odd):
    pairs = []
    for i in range(size):
        right = (i // by) % 2 == odd
        j = i + by if right else i - by
        pairs.append((i, j if 0 <= j < size else i ^ 1))
    return pairs


def on_device(wavefield, propagator_table, table_index, slowness, frequency_scale):
    sources = wavefield.shape[2]
    points = wavefield.shape[3]
    lat = lax.axis_size("lat")
    freqs = lax.axis_size("freq")
    pairs = points // (2 * WINDOW)
    first, forward, inverse = (jnp.asarray(m, BF16) for m in pair_matrices())
    vmem = pl.BlockSpec(memory_space=pltpu.VMEM)
    hbm = pl.BlockSpec(memory_space=pltpu.HBM)

    def tiles(n):
        return jax.ShapeDtypeStruct((n, 16, LANES), BF16)

    info = 8
    keep, send = pl.pallas_call(
        prep_kernel,
        out_shape=(tiles(pairs + 2), tiles(pairs + 2 + info)),
        in_specs=[hbm] * 4,
        out_specs=(vmem, vmem),
        scratch_shapes=[
            pltpu.VMEM(wavefield.shape, F32),
            pltpu.VMEM(slowness.shape, F32),
            pltpu.SMEM(table_index.shape, jnp.int32),
            pltpu.VMEM(first.shape, BF16),
            pltpu.VMEM((2, pairs + 2, 16, LANES), BF16),
            pltpu.VMEM((info * 16, LANES), F32),
            pltpu.SemaphoreType.DMA((4,)),
        ],
        compiler_params=pltpu.CompilerParams(vmem_limit_bytes=8 << 20),
        cost_estimate=pl.CostEstimate(flops=10**9, bytes_accessed=10**7, transcendentals=0),
        name="prep",
    )(
        *(
            pltpu.with_memory_space_constraint(x, pltpu.HBM)
            for x in (wavefield, slowness, table_index, first)
        )
    )
    partner = [(i, i ^ 1) for i in range(lat)]
    got = lax.ppermute(send, "lat", partner)
    near_n = 2 * (pairs + 2) - 3 + 4 + STEPS
    far_n = 11 + 1
    near, far_a, far_b, phases = pl.pallas_call(
        unit_kernel,
        out_shape=(
            tiles(near_n),
            tiles(far_n),
            tiles(far_n),
            jax.ShapeDtypeStruct((STEPS, 4 * pairs, LANES), F32),
        ),
        in_specs=[vmem] * 4,
        out_specs=(vmem,) * 4,
        compiler_params=pltpu.CompilerParams(vmem_limit_bytes=4 << 20),
        name="unit",
    )(keep, send, got, frequency_scale[None])
    a1 = lax.ppermute(near, "lat", matching(lat, 2, 0))
    b1 = lax.ppermute(near, "lat", matching(lat, 2, 1))
    a2 = lax.ppermute(far_a, "lat", matching(lat, 4, 0))
    b2 = lax.ppermute(far_b, "lat", matching(lat, 4, 1))
    inner_n = INNER[1] - INNER[0]
    table = propagator_table[0]
    weights = pl.pallas_call(
        weight_kernel,
        out_shape=jax.ShapeDtypeStruct((3, table.shape[0] // 2) + table.shape[1:], BF16),
        in_specs=[vmem],
        out_specs=vmem,
        compiler_params=pltpu.CompilerParams(vmem_limit_bytes=16 << 20),
        cost_estimate=pl.CostEstimate(flops=10**8, bytes_accessed=10**7, transcendentals=0),
        name="weights",
    )(table)
    inner = pl.pallas_call(
        lambda *refs: inner_kernel(lat // 2, *refs),
        out_shape=tiles(inner_n),
        in_specs=[vmem] * 4,
        out_specs=vmem,
        scratch_shapes=[
            pltpu.VMEM((3, 2, 23, 16, LANES), BF16),
            pltpu.VMEM((3, inner_n, 8, LANES), F32),
            pltpu.VMEM((48, LANES), F32),
        ],
        compiler_params=pltpu.CompilerParams(vmem_limit_bytes=24 << 20),
        cost_estimate=pl.CostEstimate(flops=2 * 10**9, bytes_accessed=10**7, transcendentals=0),
        name="inner",
    )(near, a1, b1, weights)
    own, other = pl.pallas_call(
        lambda *refs: main_kernel(lat // 2, *refs),
        out_shape=(tiles(12),) * 2,
        in_specs=[vmem] * 10,
        out_specs=(vmem,) * 2,
        scratch_shapes=[
            pltpu.VMEM((3, 2, 34, 16, LANES), BF16),
            pltpu.VMEM((53, 16, LANES), BF16),
            pltpu.VMEM((3, 34, 8, LANES), F32),
            pltpu.VMEM((52, 16, LANES), BF16),
            pltpu.VMEM((52, 16, LANES), BF16),
            pltpu.VMEM((STEPS, 128, LANES), F32),
            pltpu.VMEM((104, LANES), F32),
            pltpu.VMEM((104, LANES), F32),
            pltpu.VMEM((STEPS, 80, LANES), F32),
            pltpu.VMEM((STEPS, 2, 16, 8, LANES), F32),
        ],
        compiler_params=pltpu.CompilerParams(vmem_limit_bytes=32 << 20),
        name="steps",
    )(near, phases, a1, b1, a2, b2, weights, forward, inverse, inner)
    swapped = lax.ppermute(other, "lat", partner)
    core = lax.rem(lax.axis_index("lat"), 2)
    if freqs == 2:
        mine = core == lax.axis_index("freq")
        stay = jnp.where(mine, own, swapped)
        leave = jnp.where(mine, swapped, own)
        come = lax.ppermute(leave, "freq", [(0, 1), (1, 0)])
        return pl.pallas_call(
            final_kernel,
            out_shape=jax.ShapeDtypeStruct((STEPS, sources // 2, points), F32),
            in_specs=[vmem] * 2,
            out_specs=vmem,
            compiler_params=pltpu.CompilerParams(vmem_limit_bytes=4 << 20),
            name="total",
        )(stay, come)
    parts = [jnp.where(core == 0, own, swapped), jnp.where(core == 0, swapped, own)]
    rows = [
        [jnp.stack([image_rows(p, n, b) for b in range(2 * pairs)], axis=1) for p in parts]
        for n in range(STEPS)
    ]
    whole = jnp.stack([jnp.concatenate(r, axis=0) for r in rows])
    whole = whole.reshape(STEPS, sources, points)
    return lax.psum_scatter(whole, "freq", scatter_dimension=1, tiled=True).astype(F32)


def solution(mesh):
    placed = (
        P(None, "freq", None, "lat"),
        P("freq", None, None, None),
        P(None, "lat"),
        P(None, "lat"),
        P("freq"),
    )

    return jax.shard_map(
        on_device, mesh=mesh, in_specs=placed, out_specs=P(None, "freq", "lat"), check_vma=False
    )
```

```python
import math

import jax
import jax.numpy as jnp
import numpy as np
from jax import lax
from jax.experimental import pallas as pl
from jax.experimental.pallas import tpu as pltpu
from jax.sharding import PartitionSpec as P


WINDOW = 128
COEFS = 64
REACH = 16
STEPS = 3
HALF = WINDOW // 2
F32 = jnp.float32
BF16 = jnp.bfloat16
LANES = 2 * COEFS


def basis_table():
    t = np.arange(2 * WINDOW, dtype=np.float32)[:, None]
    k = np.arange(COEFS, dtype=np.float32)[None, :]
    taper = np.sin(np.float32(math.pi) * (t + np.float32(0.5)) / np.float32(2 * WINDOW))
    wave = np.cos(
        np.float32(math.pi)
        * (k + np.float32(0.5))
        * (t - np.float32(HALF) + np.float32(0.5))
        / np.float32(WINDOW)
    )
    return (taper * np.float32(math.sqrt(2.0 / WINDOW)) * wave).astype(np.float32)


def pair_matrices():
    b = basis_table()
    first = np.zeros((4 * WINDOW, LANES), np.float32)
    first[HALF : HALF + 2 * WINDOW, :COEFS] = b
    first[HALF + WINDOW : HALF + 3 * WINDOW, COEFS:] = b
    forward = np.zeros((3 * WINDOW, LANES), np.float32)
    forward[: 2 * WINDOW, :COEFS] = b
    forward[WINDOW:, COEFS:] = b
    inverse = np.zeros((4 * COEFS, 2 * WINDOW), np.float32)
    inverse[COEFS : 2 * COEFS, :WINDOW] = b[WINDOW:].T
    inverse[2 * COEFS : 3 * COEFS, :WINDOW] = b[:WINDOW].T
    inverse[2 * COEFS : 3 * COEFS, WINDOW:] = b[WINDOW:].T
    inverse[3 * COEFS :, WINDOW:] = b[:WINDOW].T
    return first, forward, inverse


def sin_cos(theta):
    turns = jnp.floor(theta * np.float32(2.0 / math.pi) + np.float32(0.5))
    r = theta - turns * np.float32(1.5703125)
    r = r - turns * np.float32(4.837512969970703e-4)
    r = r - turns * np.float32(7.549789948768648e-8)
    r2 = r * r
    s = r + r * r2 * (
        np.float32(-1.6666654611e-1)
        + r2 * (np.float32(8.3321608736e-3) + r2 * np.float32(-1.9515295891e-4))
    )
    c = 1.0 - 0.5 * r2 + r2 * r2 * (
        np.float32(4.166664568298827e-2)
        + r2 * (np.float32(-1.388731625493765e-3) + r2 * np.float32(2.443315711809948e-5))
    )
    quarter = turns - 4.0 * jnp.floor(turns * 0.25)
    odd = (quarter == 1.0) | (quarter == 3.0)
    sin_v = jnp.where(odd, c, s)
    cos_v = jnp.where(odd, s, c)
    sin_v = jnp.where(quarter >= 2.0, -sin_v, sin_v)
    cos_v = jnp.where((quarter == 1.0) | (quarter == 2.0), -cos_v, cos_v)
    return sin_v, cos_v


def lane_swap(v):
    return pltpu.roll(v, LANES // 2, v.ndim - 1)


def low_lanes(shape):
    return lax.broadcasted_iota(jnp.int32, shape, len(shape) - 1) < LANES // 2


def prep_kernel(
    wave_hbm,
    slow_hbm,
    index_hbm,
    first_hbm,
    keep_ref,
    send_ref,
    wave_ref,
    slow_ref,
    index_ref,
    first_ref,
    both_ref,
    rows_ref,
    sems,
):
    copies = [
        pltpu.make_async_copy(source, target, sems.at[i])
        for i, (source, target) in enumerate(
            (
                (wave_hbm, wave_ref),
                (first_hbm, first_ref),
                (slow_hbm, slow_ref),
                (index_hbm, index_ref),
            )
        )
    ]
    for copy in copies:
        copy.start()
    core = lax.rem(lax.axis_index("lat"), 2)
    copies[2].wait()
    copies[3].wait()
    blocks = wave_ref.shape[-1] // WINDOW
    pairs = blocks // 2
    slow = slow_ref[...]
    high = slow.astype(BF16).astype(F32)
    rest = slow - high
    lanes = low_lanes((1, LANES))
    rows_ref[...] = jnp.zeros(rows_ref.shape, F32)
    for n in range(STEPS):
        for g in range(blocks):
            cut = slice(WINDOW * g, WINDOW * (g + 1))
            rows_ref[(2 * n) * blocks + g : (2 * n) * blocks + g + 1, :] = high[n : n + 1, cut]
            rows_ref[(2 * n + 1) * blocks + g : (2 * n + 1) * blocks + g + 1, :] = rest[n : n + 1, cut]
        for q in range(pairs):
            at = 2 * STEPS * blocks + n * pairs + q
            rows_ref[at : at + 1, :] = jnp.where(
                lanes,
                jnp.full((1, LANES), index_ref[n, 2 * q], jnp.int32),
                jnp.full((1, LANES), index_ref[n, 2 * q + 1], jnp.int32),
            ).astype(F32)
    send_ref[pairs + 2 :] = rows_ref[...].reshape(-1, 16, LANES).astype(BF16)
    copies[0].wait()
    copies[1].wait()
    upper = lax.broadcasted_iota(jnp.int32, (8, wave_ref.shape[-1]), 0) < 4
    for side in range(2):
        halves = []
        for low in range(2):
            near, far = wave_ref[low, 0], wave_ref[low + 2, 0]
            if side == 0:
                halves.append(jnp.where(upper, near, pltpu.roll(far, 4, 0)))
            else:
                halves.append(jnp.where(upper, pltpu.roll(near, 4, 0), far))
        samples = jnp.concatenate(halves, axis=0).astype(BF16)
        zero = jnp.zeros((16, WINDOW), BF16)
        padded = [zero] * 3
        padded += [samples[:, WINDOW * g : WINDOW * (g + 1)] for g in range(blocks)]
        padded += [zero] * 3
        parts = [
            jnp.concatenate([padded[2 * i + j] for i in range(pairs + 2)], axis=0)
            for j in range(4)
        ]
        coefs = jnp.dot(
            jnp.concatenate(parts, axis=1), first_ref[...], preferred_element_type=F32
        )
        both_ref[side] = coefs.reshape(pairs + 2, 16, LANES).astype(BF16)
    keep_ref[...] = both_ref[core]
    send_ref[0 : pairs + 2] = both_ref[1 - core]


def unit_kernel(keep_ref, sent_ref, got_ref, scale_ref, near_ref, far_a_ref, far_b_ref, own_ref):
    place = lax.axis_index("lat")
    second = lax.rem(place, 2) == 1
    n = keep_ref.shape[0]
    own_c, own_i = keep_ref[...].astype(F32), sent_ref[n:].astype(F32)
    got_c, got_i = got_ref[:n].astype(F32), got_ref[n:].astype(F32)
    b0 = jnp.where(second, got_c, own_c)
    b1 = jnp.where(second, own_c, got_c)
    i0 = jnp.where(second, got_i, own_i)
    i1 = jnp.where(second, own_i, got_i)
    unit = jnp.concatenate([b0[: n - 2], b0[n - 2 :] + b1[:2], b1[2:]], axis=0)
    near_ref[0] = jnp.where(low_lanes((16, LANES)), unit[2 * n - 3], unit[0]).astype(BF16)
    near_ref[1 : 2 * n - 3] = unit[1 : 2 * n - 3].astype(BF16)
    at = 2 * n - 3
    phases = []
    for step in range(STEPS):
        for block, info in enumerate((i0, i1)):
            theta = scale_ref[...] * (info[2 * step] + info[2 * step + 1])
            own_ref[step, 16 * block : 16 * block + 16] = theta
            turns = jnp.floor(theta * np.float32(0.5 / math.pi) + np.float32(0.5))
            theta = theta - turns * np.float32(6.28125)
            theta = theta - turns * np.float32(2.0 * math.pi - 6.28125)
            phases.append(theta)
            if step < 2:
                near_ref[at + 2 * step + block] = theta.astype(BF16)
    at += 4
    near_ref[at] = jnp.concatenate([i0[6, :8], i1[6, :8]], axis=0).astype(BF16)
    near_ref[at + 1] = jnp.concatenate([i0[6, 8:], i1[6, 8:]], axis=0).astype(BF16)
    near_ref[at + 2] = jnp.concatenate([i0[7, :8], i1[7, :8]], axis=0).astype(BF16)
    even_quad = lax.rem(lax.div(place, 4), 2) == 0
    count = far_a_ref.shape[0] - 1
    top = jnp.concatenate([phases[1][8:], i1[6, :8]], axis=0)
    bottom = jnp.concatenate([phases[0][:8], i0[6, :8]], axis=0)
    for ref, right in ((far_a_ref, even_quad), (far_b_ref, jnp.logical_not(even_quad))):
        ref[0:count] = jnp.where(right, unit[2 * n - 2 - count :], unit[:count]).astype(BF16)
        ref[count] = jnp.where(right, top, bottom).astype(BF16)


def sign_rows():
    row = lax.broadcasted_iota(jnp.int32, (1, 8, LANES), 1)
    return jnp.where(row < 4, 1.0, -1.0).astype(F32)


def valid(flag, v):
    return jnp.where(flag, v, jnp.zeros_like(v))


def choose(flag, x_ref, y_ref, lo, hi):
    return jnp.where(flag, x_ref[lo:hi], y_ref[lo:hi]).astype(F32)


def whole_unit(tiles):
    low = low_lanes((1, 16, LANES))
    edge = tiles[0:1]
    return jnp.concatenate(
        [jnp.where(low, 0.0, edge), tiles[1:], jnp.where(low, edge, 0.0)], axis=0
    )


def middle_coefs(near_ref, left, right, has_l1, has_r1, coef_n):
    own = whole_unit(near_ref[0 : coef_n - 1].astype(F32))
    return [
        left[2 : coef_n - 2],
        left[coef_n - 2 :] + jnp.concatenate([valid(has_l1, own[0:1]), own[1:2]], axis=0),
        own[2 : coef_n - 2],
        right[:2]
        + jnp.concatenate([own[coef_n - 2 : coef_n - 1], valid(has_r1, own[coef_n - 1 :])], axis=0),
        right[2 : coef_n - 2],
    ]


def put_coefs(x_ref, coefs):
    n = coefs.shape[0]
    coefs = coefs.astype(BF16).astype(F32)
    real, imag = coefs[:, :8], coefs[:, 8:]
    source = lax.broadcasted_iota(jnp.int32, (1, 8, LANES), 1) < 4
    kinds = (real + imag, jnp.where(source, real, imag), jnp.where(source, imag, real))
    for kind, x in enumerate(kinds):
        x_ref[kind, 0, 0 : n // 2] = x.reshape(n // 2, 16, LANES).astype(BF16)
        x_ref[kind, 1, 0 : n // 2 - 1] = x[1 : n - 1].reshape(n // 2 - 1, 16, LANES).astype(BF16)


def weight_kernel(table_ref, w_ref):
    for duo in range(table_ref.shape[0] // 2):
        a, b = table_ref[2 * duo], table_ref[2 * duo + 1]
        low = low_lanes(a.shape)
        real = jnp.where(low, a, jnp.concatenate([b[:, COEFS:], b[:, :COEFS]], axis=1))
        imag = jnp.where(low, jnp.concatenate([a[:, COEFS:], a[:, :COEFS]], axis=1), b)
        w_ref[0, duo] = real
        w_ref[1, duo] = imag - real
        w_ref[2, duo] = imag + real


def band_product(x_ref, parts, rows, w_ref, k_ref):
    count = sum(n for _, n in parts)
    lane2, lane3 = low_lanes((1, LANES)), low_lanes((1, 1, LANES))
    half = jnp.floor(rows * 0.5)
    even = (rows - 2.0 * half) == 0.0
    direct = jnp.where(lane2, even.astype(F32), 1.0 - even.astype(F32)).reshape(count, 1, LANES)
    upper = half.reshape(count, 1, LANES)
    upper_swap = lane_swap(half).reshape(count, 1, LANES)
    exists = rows.reshape(count, 1, LANES) >= 0.0
    zero = jnp.zeros((COEFS, 2 * LANES), BF16)

    def band(kind, k):
        pieces = [
            x_ref[kind, (o + k) % 2, (o + k) // 2 : (o + k) // 2 + n // 2] for o, n in parts
        ]
        return jnp.concatenate(pieces, axis=0).reshape(count * 8, LANES)

    for kind in range(3):
        lhs = jnp.concatenate([band(kind, k) for k in range(REACH + 1)], axis=1)
        full = jnp.concatenate([w_ref[kind, 0], w_ref[kind, 1]], axis=1)
        rhs = jnp.concatenate(
            [jnp.concatenate([full, zero], axis=0), jnp.concatenate([zero, full], axis=0)], axis=1
        )
        out = jnp.dot(lhs, rhs, preferred_element_type=F32)
        e0, e1, o0, o1 = (
            out[:, LANES * t : LANES * (t + 1)].reshape(count, 8, LANES) for t in range(4)
        )
        u = jnp.where(upper > 0.0, jnp.where(lane3, e1, o1), jnp.where(lane3, e0, o0))
        w = jnp.where(upper_swap > 0.0, jnp.where(lane3, o1, e1), jnp.where(lane3, o0, e0))
        k_ref[kind, 0:count] = jnp.where(direct > 0.0, u, lane_swap(w))
    first, second, third = (k_ref[kind, 0:count] for kind in range(3))
    source = lax.broadcasted_iota(jnp.int32, (1, 8, LANES), 1) < 4
    real = first + jnp.where(source, -third, second)
    imag = first + jnp.where(source, second, -third)
    both = jnp.concatenate([real, imag], axis=1)
    return jnp.where(exists, both, 0.0).astype(BF16)


INNER = (-6, 22)


def inner_kernel(units, near_ref, a1_ref, b1_ref, w_ref, out_ref, x_ref, k_ref, pick_ref):
    unit = lax.div(lax.axis_index("lat"), 2)
    odd_unit = lax.rem(unit, 2) == 1
    has_l1, has_r1 = unit >= 1, unit + 1 < units
    coef_n = 18
    left = valid(has_l1, whole_unit(choose(odd_unit, a1_ref, b1_ref, 0, coef_n - 1)))
    right = valid(has_r1, whole_unit(choose(odd_unit, b1_ref, a1_ref, 0, coef_n - 1)))
    middle = middle_coefs(near_ref, left, right, has_l1, has_r1, coef_n)
    put_coefs(x_ref, jnp.concatenate(middle, axis=0))
    pos = coef_n + 3
    pick_ref[0:16] = jnp.where(has_l1, choose(odd_unit, a1_ref, b1_ref, pos, pos + 1)[0], -1.0)
    pick_ref[16:32] = near_ref[pos].astype(F32)
    pick_ref[32:48] = jnp.where(has_r1, choose(odd_unit, b1_ref, a1_ref, pos, pos + 1)[0], -1.0)
    lo, hi = INNER
    out_ref[...] = band_product(
        x_ref, ((lo - 8 + 15, hi - lo),), pick_ref[lo + 16 : hi + 16], w_ref, k_ref
    )


def main_kernel(
    units,
    near_ref,
    own_ref,
    a1_ref,
    b1_ref,
    a2_ref,
    b2_ref,
    w_ref,
    forward_ref,
    inverse_ref,
    inner_ref,
    keep_ref,
    first_ref,
    send_ref,
    x_ref,
    p_ref,
    k_ref,
    xe_ref,
    xo_ref,
    slow_ref,
    cos_ref,
    sin_ref,
    pick_ref,
    image_ref,
):
    place = lax.axis_index("lat")
    unit = lax.div(place, 2)
    second = lax.rem(place, 2)
    odd_unit = lax.rem(unit, 2) == 1
    odd_quad = lax.rem(lax.div(place, 4), 2) == 1
    has_l1, has_l2 = unit >= 1, unit >= 2
    has_r1, has_r2 = unit + 1 < units, unit + 2 < units
    pairs = 16
    coef_n = pairs + 2
    far_n = a2_ref.shape[0] - 1

    left = valid(has_l1, whole_unit(choose(odd_unit, a1_ref, b1_ref, 0, coef_n - 1)))
    right = valid(has_r1, whole_unit(choose(odd_unit, b1_ref, a1_ref, 0, coef_n - 1)))
    left2 = valid(has_l2, choose(odd_quad, a2_ref, b2_ref, 0, far_n))
    right2 = valid(has_r2, choose(odd_quad, b2_ref, a2_ref, 0, far_n))
    near_left = jnp.concatenate([valid(has_l2, left[0:1]), left[1:2]], axis=0)
    near_right = jnp.concatenate(
        [right[coef_n - 2 : coef_n - 1], valid(has_r2, right[coef_n - 1 :])], axis=0
    )
    put_coefs(
        x_ref,
        jnp.concatenate(
            [left2[: far_n - 2], left2[far_n - 2 :] + near_left]
            + middle_coefs(near_ref, left, right, has_l1, has_r1, coef_n)
            + [right2[:2] + near_right, right2[2:]],
            axis=0,
        ),
    )

    far_rows = 48
    for step in range(STEPS):
        slow_ref[step, far_rows : far_rows + 32] = own_ref[step]
    for step in range(2):
        lo = coef_n - 1 + 2 * step
        for flag, pos in ((odd_unit, -32), (jnp.logical_not(odd_unit), 32)):
            rows = choose(flag, a1_ref, b1_ref, lo, lo + 2)
            slow_ref[step, far_rows + pos : far_rows + pos + 32] = rows.reshape(32, LANES)
    before2 = choose(odd_quad, a2_ref, b2_ref, far_n, far_n + 1)[0]
    after2 = choose(odd_quad, b2_ref, a2_ref, far_n, far_n + 1)[0]
    slow_ref[0, far_rows - 40 : far_rows - 32] = before2[:8]
    slow_ref[0, far_rows + 64 : far_rows + 72] = after2[:8]

    for step in range(STEPS):
        pos = coef_n + 3 + step
        pick_ref[step, 32:48] = near_ref[pos].astype(F32)
        pick_ref[step, 16:32] = jnp.where(
            has_l1, choose(odd_unit, a1_ref, b1_ref, pos, pos + 1)[0], -1.0)
        pick_ref[step, 48:64] = jnp.where(
            has_r1, choose(odd_unit, b1_ref, a1_ref, pos, pos + 1)[0], -1.0)
    pick_ref[0, 8:16] = jnp.where(has_l2, before2[8:], -1.0)
    pick_ref[0, 64:72] = jnp.where(has_r2, after2[8:], -1.0)

    sign = sign_rows()
    row3 = lax.broadcasted_iota(jnp.int32, (1, 8, LANES), 1) < 4
    lane3 = low_lanes((1, 1, LANES))
    lane2 = low_lanes((1, LANES))

    plan = (
        dict(lo=-18, hi=34, base=26, first=-17),
        dict(lo=-9, hi=25, base=17, first=-9),
        dict(lo=-1, hi=17, base=9, first=0),
    )
    for step, item in enumerate(plan):
        lo, hi = item["lo"], item["hi"]
        count = hi - lo
        p_ref[0] = jnp.zeros((16, LANES), BF16)
        if step == 0:
            parts = ((lo, INNER[0] - lo), (INNER[1], hi - INNER[1]))
            p_ref[1 + INNER[0] - lo : 1 + INNER[1] - lo] = inner_ref[...]
        else:
            parts = ((lo, count),)
        rows = jnp.concatenate(
            [pick_ref[step, a + 32 : a + 32 + m] for a, m in parts], axis=0
        )
        out = band_product(
            x_ref, [(item["base"] + a - 8, m) for a, m in parts], rows, w_ref, k_ref
        )
        done = 0
        for a, m in parts:
            p_ref[1 + a - lo : 1 + a - lo + m] = out[done : done + m]
            done += m
        first = item["first"]
        n = hi - first
        o = first - lo
        lhs = jnp.concatenate(
            [p_ref[o : o + n].reshape(n * 16, LANES), p_ref[o + 1 : o + 1 + n].reshape(n * 16, LANES)],
            axis=1,
        )
        back = jnp.dot(lhs, inverse_ref[...], preferred_element_type=F32)
        g0 = 2 * first + far_rows
        before = slow_ref[step, g0 - 1 : g0 - 1 + 2 * n]
        after = slow_ref[step, g0 : g0 + 2 * n]
        if step < 2:
            number = lax.broadcasted_iota(jnp.int32, (2 * n, 1), 0) + 2 * first

            def exists(block):
                inside = (block >= 0) & (block < 32)
                l1 = (block < 0) & (block >= -32) & has_l1
                r1 = (block >= 32) & (block < 64) & has_r1
                l2 = (block < -32) & has_l2
                r2 = (block >= 64) & has_r2
                return inside | l1 | r1 | l2 | r2

            ok = jnp.where(lane2, exists(number - 1).astype(jnp.int32), exists(number).astype(jnp.int32)) > 0
        theta = jnp.where(lane2, lane_swap(before), lane_swap(after))
        sin_v, cos_v = sin_cos(theta)
        if step < 2:
            sin_v = jnp.where(ok, sin_v, 0.0)
            cos_v = jnp.where(ok, cos_v, 0.0)
        cos_ref[0 : 2 * n] = cos_v
        sin_ref[0 : 2 * n] = sin_v
        images = []
        for parity, sample_ref in ((0, xe_ref), (1, xo_ref)):
            b = back[:, LANES * parity : LANES * (parity + 1)].reshape(n, 16, LANES)
            c = cos_ref[pl.ds(parity, n, stride=2)].reshape(n, 1, LANES)
            s = sin_ref[pl.ds(parity, n, stride=2)].reshape(n, 1, LANES) * sign
            f0 = c * b[:, :8] - s * b[:, 8:]
            f1 = c * b[:, 8:] + s * b[:, :8]
            if step < 2:
                sample_ref[0:n] = jnp.concatenate([f0, f1], axis=1).astype(BF16)
            m = 17 - parity
            f0, f1 = f0[-first : -first + m], f1[-first : -first + m]
            images.append(lane_swap(f0 * pltpu.roll(f0, 4, 1) + f1 * pltpu.roll(f1, 4, 1)))
        even, odd = images
        image_ref[step, 0] = jnp.where(lane3, even[:16], odd)
        image_ref[step, 1] = jnp.where(lane3, odd, even[1:])
        if step < 2:
            if step == 1:
                xe_ref[n] = jnp.zeros((16, LANES), BF16)
                m = n
            else:
                m = n - 1
            lhs = jnp.concatenate(
                [
                    xe_ref[0:m].reshape(m * 16, LANES),
                    xo_ref[0:m].reshape(m * 16, LANES),
                    xe_ref[1 : m + 1].reshape(m * 16, LANES),
                ],
                axis=1,
            )
            coefs = jnp.dot(lhs, forward_ref[...], preferred_element_type=F32).reshape(m, 16, LANES)
            number = lax.broadcasted_iota(jnp.int32, (m, 1, 1), 0) + first
            ok = (
                ((number >= 0) & (number < 16))
                | ((number < 0) & (number >= -16) & has_l1)
                | ((number >= 16) & (number < 32) & has_r1)
                | ((number < -16) & has_l2)
                | ((number >= 32) & has_r2)
            )
            put_coefs(x_ref, jnp.where(ok, coefs, 0.0))
    swap_first = lax.axis_index("freq") == second
    for ref, half in (
        (keep_ref, second),
        (first_ref, jnp.where(swap_first, 1 - second, second)),
        (send_ref, 1 - second),
    ):
        span = pl.ds(8 * half, 8)
        tops = [
            jnp.where(row3, image_ref[0, parity, span], image_ref[1, parity, span])
            for parity in range(2)
        ]
        ref[0:8] = jnp.concatenate(tops, axis=1).astype(BF16)
        last = jnp.where(row3, image_ref[2, 0, span], image_ref[2, 1, span])
        ref[8:12] = last.reshape(4, 16, LANES).astype(BF16)


def image_rows(tiles, step, block):
    q, parity = divmod(block, 2)
    if step < 2:
        row = 8 * parity + 4 * step
        return tiles[q, row : row + 4]
    row = 8 * (q % 2) + 4 * parity
    return tiles[8 + q // 2, row : row + 4]


def final_kernel(own_ref, a_ref, b_ref, out_ref):
    straight = lax.rem(lax.axis_index("lat"), 2) == lax.axis_index("freq")
    first = jnp.where(straight, own_ref[...], b_ref[...]).astype(F32)
    total = first + a_ref[...].astype(F32)
    for block in range(out_ref.shape[-1] // WINDOW):
        cut = slice(WINDOW * block, WINDOW * (block + 1))
        for n in range(STEPS):
            out_ref[n, :, cut] = image_rows(total, n, block)


def matching(size, by, odd):
    pairs = []
    for i in range(size):
        right = (i // by) % 2 == odd
        j = i + by if right else i - by
        pairs.append((i, j if 0 <= j < size else i ^ 1))
    return pairs


def on_device(wavefield, propagator_table, table_index, slowness, frequency_scale):
    sources = wavefield.shape[2]
    points = wavefield.shape[3]
    lat = lax.axis_size("lat")
    freqs = lax.axis_size("freq")
    pairs = points // (2 * WINDOW)
    first, forward, inverse = (jnp.asarray(m, BF16) for m in pair_matrices())
    vmem = pl.BlockSpec(memory_space=pltpu.VMEM)
    hbm = pl.BlockSpec(memory_space=pltpu.HBM)

    def tiles(n):
        return jax.ShapeDtypeStruct((n, 16, LANES), BF16)

    info = 8
    keep, send = pl.pallas_call(
        prep_kernel,
        out_shape=(tiles(pairs + 2), tiles(pairs + 2 + info)),
        in_specs=[hbm] * 4,
        out_specs=(vmem, vmem),
        scratch_shapes=[
            pltpu.VMEM(wavefield.shape, F32),
            pltpu.VMEM(slowness.shape, F32),
            pltpu.SMEM(table_index.shape, jnp.int32),
            pltpu.VMEM(first.shape, BF16),
            pltpu.VMEM((2, pairs + 2, 16, LANES), BF16),
            pltpu.VMEM((info * 16, LANES), F32),
            pltpu.SemaphoreType.DMA((4,)),
        ],
        compiler_params=pltpu.CompilerParams(vmem_limit_bytes=8 << 20),
        cost_estimate=pl.CostEstimate(flops=10**9, bytes_accessed=10**7, transcendentals=0),
        name="prep",
    )(
        *(
            pltpu.with_memory_space_constraint(x, pltpu.HBM)
            for x in (wavefield, slowness, table_index, first)
        )
    )
    partner = [(i, i ^ 1) for i in range(lat)]
    got = lax.ppermute(send, "lat", partner)
    near_n = 2 * (pairs + 2) - 3 + 4 + STEPS
    far_n = 11 + 1
    near, far_a, far_b, phases = pl.pallas_call(
        unit_kernel,
        out_shape=(
            tiles(near_n),
            tiles(far_n),
            tiles(far_n),
            jax.ShapeDtypeStruct((STEPS, 4 * pairs, LANES), F32),
        ),
        in_specs=[vmem] * 4,
        out_specs=(vmem,) * 4,
        compiler_params=pltpu.CompilerParams(vmem_limit_bytes=4 << 20),
        name="unit",
    )(keep, send, got, frequency_scale[None])
    a1 = lax.ppermute(near, "lat", matching(lat, 2, 0))
    b1 = lax.ppermute(near, "lat", matching(lat, 2, 1))
    a2 = lax.ppermute(far_a, "lat", matching(lat, 4, 0))
    b2 = lax.ppermute(far_b, "lat", matching(lat, 4, 1))
    inner_n = INNER[1] - INNER[0]
    table = propagator_table[0]
    weights = pl.pallas_call(
        weight_kernel,
        out_shape=jax.ShapeDtypeStruct((3, table.shape[0] // 2) + table.shape[1:], BF16),
        in_specs=[vmem],
        out_specs=vmem,
        compiler_params=pltpu.CompilerParams(vmem_limit_bytes=16 << 20),
        cost_estimate=pl.CostEstimate(flops=10**8, bytes_accessed=10**7, transcendentals=0),
        name="weights",
    )(table)
    inner = pl.pallas_call(
        lambda *refs: inner_kernel(lat // 2, *refs),
        out_shape=tiles(inner_n),
        in_specs=[vmem] * 4,
        out_specs=vmem,
        scratch_shapes=[
            pltpu.VMEM((3, 2, 23, 16, LANES), BF16),
            pltpu.VMEM((3, inner_n, 8, LANES), F32),
            pltpu.VMEM((48, LANES), F32),
        ],
        compiler_params=pltpu.CompilerParams(vmem_limit_bytes=24 << 20),
        cost_estimate=pl.CostEstimate(flops=2 * 10**9, bytes_accessed=10**7, transcendentals=0),
        name="inner",
    )(near, a1, b1, weights)
    own, leave, other = pl.pallas_call(
        lambda *refs: main_kernel(lat // 2, *refs),
        out_shape=(tiles(12),) * 3,
        in_specs=[vmem] * 10,
        out_specs=(vmem,) * 3,
        scratch_shapes=[
            pltpu.VMEM((3, 2, 34, 16, LANES), BF16),
            pltpu.VMEM((53, 16, LANES), BF16),
            pltpu.VMEM((3, 34, 8, LANES), F32),
            pltpu.VMEM((52, 16, LANES), BF16),
            pltpu.VMEM((52, 16, LANES), BF16),
            pltpu.VMEM((STEPS, 128, LANES), F32),
            pltpu.VMEM((104, LANES), F32),
            pltpu.VMEM((104, LANES), F32),
            pltpu.VMEM((STEPS, 80, LANES), F32),
            pltpu.VMEM((STEPS, 2, 16, 8, LANES), F32),
        ],
        compiler_params=pltpu.CompilerParams(vmem_limit_bytes=32 << 20),
        name="steps",
    )(near, phases, a1, b1, a2, b2, weights, forward, inverse, inner)
    if freqs == 2:
        ring, cross = [], []
        for place in range(lat):
            for freq in range(2):
                here, across = 2 * place + freq, 2 * (place ^ 1)
                ring.append((here, across + freq if freq == place % 2 else 2 * place + 1 - freq))
                cross.append((here, across + 1 - freq))
        come = lax.ppermute(leave, ("lat", "freq"), ring)
        over = lax.ppermute(other, ("lat", "freq"), cross)
        return pl.pallas_call(
            final_kernel,
            out_shape=jax.ShapeDtypeStruct((STEPS, sources // 2, points), F32),
            in_specs=[vmem] * 3,
            out_specs=vmem,
            compiler_params=pltpu.CompilerParams(vmem_limit_bytes=4 << 20),
            name="total",
        )(own, come, over)
    swapped = lax.ppermute(other, "lat", partner)
    core = lax.rem(lax.axis_index("lat"), 2)
    parts = [jnp.where(core == 0, own, swapped), jnp.where(core == 0, swapped, own)]
    rows = [
        [jnp.stack([image_rows(p, n, b) for b in range(2 * pairs)], axis=1) for p in parts]
        for n in range(STEPS)
    ]
    whole = jnp.stack([jnp.concatenate(r, axis=0) for r in rows])
    whole = whole.reshape(STEPS, sources, points)
    return lax.psum_scatter(whole, "freq", scatter_dimension=1, tiled=True).astype(F32)


def solution(mesh):
    placed = (
        P(None, "freq", None, "lat"),
        P("freq", None, None, None),
        P(None, "lat"),
        P(None, "lat"),
        P("freq"),
    )

    return jax.shard_map(
        on_device, mesh=mesh, in_specs=placed, out_specs=P(None, "freq", "lat"), check_vma=False
    )
```
